32 devices in a mesh: img: 4 (over x, core), patch: 8 (over z, y).
Axes of the slice: x: 2, y: 2, z: 4, core: 2. Of those that a mesh axis runs over, the one named last changes fastest.
Arguments:
- hidden: bfloat16 [8, 8, 128, 640], P('img', 'patch'), may hold values from -100 to 100
- stale_attn_in: bfloat16 [8, 8, 128, 640], P('img', 'patch'), may hold values from -100 to 100
- stale_conv_in: bfloat16 [8, 8, 128, 640], P('img', 'patch'), may hold values from -6 to 6
- ln_gain: float32 [640], replicated, may hold values from 0.25 to 1.75
- ln_bias: float32 [640], replicated, may hold values from -2 to 2
- w_qkv: bfloat16 [640, 1920], replicated, may hold values from -3 to 3
- w_out: bfloat16 [640, 640], replicated, may hold values from -0.25 to 0.25
- gn_gain: float32 [640], replicated, may hold values from 0.25 to 1.75
- gn_bias: float32 [640], replicated, may hold values from -1.5 to 1.5
- conv_weight: bfloat16 [3, 3, 640, 640], replicated, may hold values from -0.078125 to 0.078125
- conv_bias: float32 [640], replicated, may hold values from -1.5 to 1.5
- time_shift: float32 [8, 640], P('img'), may hold values from -6 to 6
Outputs:
- block_out: bfloat16 [8, 8, 128, 640], P('img', 'patch')
The draws below stay inside these ranges and needn't reach their ends.
All inputs are finite; a program needn't handle non-finite values.
Results may differ from the reference program's by a relative error of at most 0.0075.
The reference program's roundings to bfloat16 on the way count: a program that leaves them out, or rounds other values in their place, can miss the bound.
Values may be sent and summed in bfloat16 or wider, within the bound.
A program may use at most 128 MiB of HBM per device.

```python
import math
import jax
import jax.numpy as jnp
from jax import lax

C = 640
GROUPS = 32
HEAD_DIM = 64
ROWS_DEV = 1
COLS = 128
SAMPLES = 8
ROWS = 8
N_PATCH = 8


def paired_inputs(key):
    base_key = jax.random.fold_in(key, 101)
    subkeys = jax.random.split(base_key, 7)
    full_shape = (SAMPLES, ROWS, COLS, C)
    noise_current = jax.random.truncated_normal(subkeys[0], -4.0, 4.0, full_shape, jnp.float32)
    noise_stale = jax.random.truncated_normal(subkeys[1], -4.0, 4.0, full_shape, jnp.float32)
    pattern = 1.5 * jax.random.truncated_normal(subkeys[6], -4.0, 4.0, (SAMPLES, ROWS, 1, C), jnp.float32)
    row_frac = (jnp.arange(ROWS, dtype=jnp.float32) + 0.5) / ROWS - 0.5
    row_scale = 10.0 ** (row_frac[None, :] + 0.5 * jax.random.uniform(subkeys[2], (SAMPLES, ROWS), jnp.float32) - 0.25)
    col_scale = 2.0 ** (2.0 * jax.random.uniform(subkeys[3], (SAMPLES, COLS), jnp.float32) - 1.0)
    chan_scale = 2.0 ** (2.0 * jax.random.uniform(subkeys[4], (C,), jnp.float32) - 1.0)
    full_scale = row_scale[:, :, None, None] * col_scale[:, None, :, None] * chan_scale
    current = (noise_current + pattern) * full_scale
    stale = (noise_stale + pattern) * full_scale
    current = jnp.clip(current, -96.0, 96.0) * 0.03
    stale = jnp.clip(stale, -96.0, 96.0)
    return (current, stale)


def draw_hidden(key, part):
    return paired_inputs(key)[0].astype(jnp.bfloat16)


def draw_stale_attn_in(key, part):
    return paired_inputs(key)[1].astype(jnp.bfloat16)


def draw_ln_bias(key, part):
    bias_scale = 0.3
    return bias_scale * jax.random.truncated_normal(jax.random.fold_in(key, 303), -4.0, 4.0, (C,), jnp.float32)


def draw_w_qkv(key, part):
    subkeys = jax.random.split(jax.random.fold_in(key, 202), 4)
    query_cols = jax.random.truncated_normal(subkeys[0], -4.0, 4.0, (C, C), jnp.float32) / math.sqrt(C)
    value_cols = jax.random.truncated_normal(subkeys[1], -4.0, 4.0, (C, C), jnp.float32) / math.sqrt(C)
    query_cols = 2.5 * query_cols
    key_cols = jax.random.truncated_normal(subkeys[3], -4.0, 4.0, (C, C), jnp.float32) / math.sqrt(C)
    return jnp.concatenate([query_cols, key_cols, value_cols], 1).astype(jnp.bfloat16)


def block_scale(own_key, extent, pieces, smallest, high):
    factor_of, own = 1.0, jax.random.fold_in(own_key, 6)
    for axis_at, blocks in pieces:
        steps = jnp.exp(jax.random.uniform(jax.random.fold_in(own, axis_at), (blocks,), jnp.float32, smallest / len(pieces), high / len(pieces)))
        factor_of = factor_of * jnp.repeat(steps, extent[axis_at] // blocks).reshape([-1 if axis == axis_at else 1 for axis in range(len(extent))])
    return factor_of


def noise(own_key, shape, scale, reach, cuts=(), kind=jnp.bfloat16):
    drawn = jax.random.normal(own_key, shape, jnp.float32) * scale
    if len(cuts) > 0:
        drawn = block_scale(own_key, shape, cuts, -0.22, 0.18) * drawn
    return jnp.clip(drawn, min=-reach, max=reach).astype(kind)


def setup_inputs(seed: int = 0) -> dict:
    seeds = jax.random.split(jax.random.key(seed), 13)
    return {
        "hidden": draw_hidden(jax.random.fold_in(seeds[12], 71), 0),
        "stale_attn_in": draw_stale_attn_in(jax.random.fold_in(seeds[12], 71), 0),
        "stale_conv_in": noise(seeds[2], (SAMPLES, ROWS, COLS, C), 1.0, 6.0, ((0, 4), (1, 8))),
        "ln_gain": jnp.clip(1.0 + 0.15 * jax.random.normal(seeds[3], (C,), jnp.float32), 0.25, 1.75),
        "ln_bias": draw_ln_bias(jax.random.fold_in(seeds[12], 71), 0),
        "w_qkv": draw_w_qkv(jax.random.fold_in(seeds[12], 71), 0),
        "w_out": noise(seeds[6], (C, C), C ** -0.5, 0.25),
        "gn_gain": jnp.clip(1.0 + 0.15 * jax.random.normal(seeds[7], (C,), jnp.float32), 0.25, 1.75),
        "gn_bias": noise(seeds[8], (C,), 0.3, 1.5, (), jnp.float32),
        "conv_weight": noise(seeds[9], (3, 3, C, C), (9 * C) ** -0.5, 0.078125),
        "conv_bias": noise(seeds[10], (C,), 0.3, 1.5, (), jnp.float32),
        "time_shift": noise(seeds[11], (SAMPLES, C), 1.0, 6.0, ((0, 4),), jnp.float32),
    }


EPSILON = 1e-05

def to_half(values):
    return lax.optimization_barrier(values.astype(jnp.bfloat16))

def layer_norm(values, gain, bias):
    values = values.astype(jnp.float32)
    centre = lax.optimization_barrier(jnp.mean(values, -1, keepdims=True))
    centred = values - centre
    spread = lax.optimization_barrier(jnp.mean(centred * centred, -1, keepdims=True))
    return to_half(centred * lax.rsqrt(spread + EPSILON) * gain + bias)

def reference(hidden, stale_attn_in, stale_conv_in, ln_gain, ln_bias, w_qkv, w_out, gn_gain, gn_bias, conv_weight, conv_bias, time_shift):
    head_count = C // HEAD_DIM
    tokens = ROWS * COLS
    patches = N_PATCH
    per_patch = ROWS_DEV * COLS
    score_scale = HEAD_DIM ** (-0.5)
    fresh_in = layer_norm(hidden, ln_gain, ln_bias).reshape(SAMPLES, tokens, C)
    stale_in = layer_norm(stale_attn_in, ln_gain, ln_bias).reshape(SAMPLES, tokens, C)

    def split_heads(values):
        return values.reshape(patches, per_patch, head_count, HEAD_DIM).transpose(2, 0, 1, 3)

    def one_head(head_parts):
        queries, fresh_keys, fresh_values, stale_keys, stale_values = head_parts
        queries = queries.astype(jnp.float32)
        remote = jnp.einsum('pqd,rkd->pqrk', queries, stale_keys.astype(jnp.float32)) * score_scale
        local_scores = jnp.einsum('pqd,pkd->pqk', queries, fresh_keys.astype(jnp.float32)) * score_scale
        same_patch = jnp.eye(patches, dtype=bool)[:, None, :, None]
        remote = jnp.where(same_patch, -jnp.inf, remote)
        row_max = jnp.maximum(lax.optimization_barrier(jnp.max(remote, axis=(2, 3))), lax.optimization_barrier(jnp.max(local_scores, -1)))
        remote_weights = jnp.exp(remote - row_max[:, :, None, None])
        local_weights = jnp.exp(local_scores - row_max[:, :, None])
        weight_sum = lax.optimization_barrier(jnp.sum(remote_weights, axis=(2, 3))) + lax.optimization_barrier(jnp.sum(local_weights, -1))
        gathered = jnp.einsum('pqrk,rkd->pqd', to_half(remote_weights).astype(jnp.float32), stale_values.astype(jnp.float32))
        gathered = gathered + jnp.einsum('pqk,pkd->pqd', to_half(local_weights).astype(jnp.float32), fresh_values.astype(jnp.float32))
        return gathered / weight_sum[:, :, None]

    def attend_sample(operands):
        fresh_rows, stale_rows = operands
        projected = to_half(jnp.dot(fresh_rows, w_qkv, preferred_element_type=jnp.float32))
        stale_pairs = to_half(jnp.dot(stale_rows, w_qkv[:, C:], preferred_element_type=jnp.float32))
        head_parts = (split_heads(projected[:, :C]), split_heads(projected[:, C:2 * C]), split_heads(projected[:, 2 * C:]), split_heads(stale_pairs[:, :C]), split_heads(stale_pairs[:, C:]))
        per_head = lax.map(one_head, head_parts)
        attended = to_half(per_head.transpose(1, 2, 0, 3).reshape(tokens, C))
        return jnp.dot(attended, w_out, preferred_element_type=jnp.float32)
    attention_out = lax.map(attend_sample, (fresh_in, stale_in))
    residual = to_half(hidden.reshape(SAMPLES, tokens, C).astype(jnp.float32) + attention_out)
    grouped = residual.astype(jnp.float32).reshape(SAMPLES, tokens, GROUPS, C // GROUPS)
    group_mean = lax.optimization_barrier(jnp.mean(grouped, axis=(1, 3), keepdims=True))
    centred = grouped - group_mean
    group_var = lax.optimization_barrier(jnp.mean(centred * centred, axis=(1, 3), keepdims=True))
    normalized = (centred * lax.rsqrt(group_var + EPSILON)).reshape(SAMPLES, tokens, C)
    activated = to_half(jax.nn.silu(normalized * gn_gain + gn_bias)).reshape(SAMPLES, ROWS, COLS, C)

    def convolve(operands):
        fresh_rows, stale_rows = operands
        fresh_patch = fresh_rows.reshape(patches, ROWS_DEV, COLS, C)
        stale_patch = stale_rows.reshape(patches, ROWS_DEV, COLS, C)
        zero_rim = jnp.zeros((1, 1, COLS, C), jnp.bfloat16)
        rim_above = jnp.concatenate([zero_rim, stale_patch[:-1, ROWS_DEV - 1:]], 0)
        rim_below = jnp.concatenate([stale_patch[1:, :1], zero_rim], 0)
        framed = jnp.concatenate([rim_above, fresh_patch, rim_below], 1)
        framed = jnp.pad(framed, ((0, 0), (0, 0), (1, 1), (0, 0)))
        summed = jnp.zeros((patches * ROWS_DEV * COLS, C), jnp.float32)
        for tap_row in range(3):
            for tap_col in range(3):
                window = framed[:, tap_row:tap_row + ROWS_DEV, tap_col:tap_col + COLS, :].reshape(-1, C)
                summed = summed + jnp.dot(window, conv_weight[tap_row, tap_col], preferred_element_type=jnp.float32)
        return summed.reshape(ROWS, COLS, C)
    convolved = lax.map(convolve, (activated, stale_conv_in))
    summed_out = convolved + conv_bias + time_shift[:, None, None, :] + residual.astype(jnp.float32).reshape(SAMPLES, ROWS, COLS, C)
    return summed_out.astype(jnp.bfloat16)
```

```python
import functools
import heapq
import itertools

import jax
import jax.numpy as jnp
from jax import lax
from jax.experimental import pallas as pl
from jax.experimental.pallas import tpu as pltpu
from jax.sharding import PartitionSpec as P

GROUPS = 32
HEAD_DIM = 64
EPSILON = 1e-05
MESH = pl.DeviceIdType.MESH
F32 = jnp.float32
BF16 = jnp.bfloat16

DOWN, UP, ACROSS = 0, 1, 2
MOVED = True
TUNED = {
    4: [
        (
            [6, 22, 770, 786, 612, 38, 88, 140, 122, 152, 54, 580, 74, 188, 248, 316, 200, 216, 300, 682, 628, 232, 666, 596, 106, 168, 360, 376, 444, 698, 428, 650, 488, 984, 504, 968],
            35,
            36,
            [(0, 0, 0), (0, 1, 0), (1, 0, 0), (1, 1, 0), (1, 2, 0), (1, 3, 0)],
            [13, 18, 25, 26, 28, 35],
        ),
        (
            [135, 151, 167, 596, 183, 580, 10, 219, 313, 30, 200, 280, 235, 297, 840, 42, 268, 328, 88, 120, 412, 58, 360, 650, 628, 72, 396, 456, 445, 472, 856, 250, 429, 744, 344, 698, 728, 612, 104, 488, 376, 666, 682, 760, 504, 712],
            45,
            45,
            [(0, 1, 0), (0, 0, 0), (0, 3, 3), (0, 2, 5), (1, 1, 0), (1, 0, 0), (1, 2, 0), (1, 3, 0)],
            [11, 26, 31, 35, 35, 39, 41, 45],
        ),
        (
            [263, 279, 311, 295, 140, 363, 393, 170, 413, 666, 580, 186, 328, 425, 12, 456, 650, 28, 441, 472, 216, 347, 488, 628, 152, 200, 840, 46, 88, 856, 596, 232, 377, 612, 62, 698, 72, 712, 104, 248, 120, 760, 682, 504, 728, 744],
            44,
            44,
            [(0, 3, 0), (0, 2, 0), (0, 1, 3), (0, 0, 5), (1, 2, 0), (1, 1, 0), (1, 0, 0), (1, 3, 0)],
            [20, 22, 30, 37, 37, 40, 41, 44],
        ),
        (
            [389, 405, 769, 785, 437, 421, 316, 457, 268, 680, 612, 296, 489, 596, 328, 360, 472, 728, 172, 648, 188, 248, 628, 376, 712, 580, 232, 344, 280, 696, 44, 664, 505, 60, 120, 760, 104, 968, 984, 744],
            37,
            39,
            [(0, 3, 0), (0, 2, 0), (1, 2, 0), (1, 1, 0), (1, 3, 0), (1, 0, 0)],
            [17, 29, 29, 29, 33, 37],
        ),
    ]
}


def special_parts(length):
    return tuple(8 * length + 4 * k for k in range(1, 8))


def mirrored_part(length, y, part):
    return part if y == 0 or part >= 8 * length else 4 * (2 * length - 1 - part // 4) + part % 4


def transfers(length):
    own_edge, cross, handed, q_own, q_far, o_own, o_far = special_parts(length)
    ends = (0, length - 1)

    def turned(zd, sz, half):
        return abs(sz - zd) == 1 and (half == 1 or (zd not in ends and sz in ends))

    result = {}
    for z, y in itertools.product(range(length), range(2)):
        sends = {}
        sides = [(k, zd) for k, zd in ((DOWN, z - 1), (UP, z + 1)) if 0 <= zd < length]
        for sz, sy, sp in itertools.product(range(length), range(2), range(4)):
            part = (2 * sz + sy) * 4 + sp
            sends[part] = [
                (k, part)
                for k, zd in sides
                if needs(length, zd, sz, sp // 2)
                and ((sz <= z if k == UP else sz >= z) if sy == y else sz == z and turned(zd, sz, sp % 2))
            ]
            if sy == y and needs(length, z, sz, sp // 2) and not turned(z, sz, sp % 2):
                sends[part].append((ACROSS, part))
        on = UP if y == 0 else DOWN
        for k in range(4):
            sends[own_edge + k] = [(ACROSS, cross + k)]
            sends[cross + k] = [(on, handed + k)] if on in dict(sides) else []
        for k in range(2):
            sends[q_own + k] = [(UP if z == 0 else DOWN, q_far + k)] if z in ends else []
            sends[o_own + k] = [(DOWN if z == 1 else UP, o_far + k)] if z in (1, length - 2) else []
        result[z, y] = sends
    return result


def needs(length, z, sz, sample):
    return not (sample == 0 and z in (0, length - 1) and abs(sz - z) > 1)


def programs_by_time(length):
    own_edge, cross, handed, q_own, q_far, o_own, o_far = special_parts(length)
    ends = (0, length - 1)
    sends = transfers(length)
    queues, busy, events, count = {}, {}, [], itertools.count()
    landed = {d: {} for d in sends}
    left, answered = {}, set()
    rank = {own_edge: 5, cross: 4, handed: 4, q_own: 0, q_far: 0, o_own: -1, o_far: -1}

    def push(t, kind, *rest):
        heapq.heappush(events, (t, next(count), kind, rest))

    def offer(t, d, part):
        for k, there in sends[d].get(part, []):
            push(t, "queue", d, k, part, there)

    def launch(t, d, k):
        busy[d, k] = bool(queues[d, k])
        if busy[d, k]:
            _, there, part = heapq.heappop(queues[d, k])
            left.setdefault((d, part), t)
            push(t + 1.76, "sent", d, k, there)

    for d in sends:
        for k in range(4):
            offer(0.0, d, (2 * d[0] + d[1]) * 4 + k)
            offer(0.0, d, own_edge + k)
        for k in range(2):
            if d[0] in ends:
                offer(2.0, d, q_own + k)
    while events:
        t, _, kind, (d, *rest) = heapq.heappop(events)
        z, y = d
        if kind == "queue":
            k, part, there = rest
            u = z if y == 0 else length - 1 - z
            c = mirrored_part(length, y, part)
            if c < 8 * length:
                order = c % 4 // 2 - abs(c // 8 - u) * (0.5 if k == ACROSS else 1.0)
            else:
                order = rank[c // 4 * 4]
            heapq.heappush(queues.setdefault((d, k), []), ((order, c), there, part))
            if not busy.get((d, k)):
                busy[d, k] = True
                push(t, "launch", d, k)
        elif kind == "launch":
            launch(t, d, rest[0])
        elif kind == "sent":
            k, there = rest
            push(t + 1.75, "landed", ((z - 1, y), (z + 1, y), (z, 1 - y))[k], there)
            launch(t, d, k)
        else:
            landed[d][rest[0]] = t
            offer(t + 0.3, d, rest[0])
            if z in (1, length - 2) and d not in answered:
                far = [
                    (2 * sz + sy) * 4 + sp
                    for sz, sy, sp in itertools.product(range(length), range(2), range(2))
                    if not needs(length, 0 if z == 1 else length - 1, sz, 0) and sz != z
                ]
                if all(p in landed[d] for p in (q_far, q_far + 1, *far)):
                    answered.add(d)
                    for k in range(2):
                        offer(t + 2.5, d, o_own + k)
    programs = []
    for z in range(length):
        d = (z, 0)
        timed = [(t, 1, p) for p, t in landed[d].items()]
        timed += [(-2.0, 0, 8 * z + k) for k in range(2)]
        if z in ends:
            timed += [(-1.0, 0, q_own + k) for k in range(2)]
        for p in (8 * z + 2, 8 * z + 3, *range(own_edge, own_edge + 4)):
            timed.append((max(0.0, left[d, p] - 1.0), 0, p))
        timed.sort()
        codes = [p * 16 + 8 * waits + sum(2**k for k, _ in sends[d].get(p, [])) for _, waits, p in timed]
        in_loop = 1 + max(i for i, (_, _, p) in enumerate(timed) if p < 8 * length)
        results = [i + 1 for i, (_, _, p) in enumerate(timed) if p >= o_far]
        complete, queries = {}, 0
        for i, (_, _, p) in enumerate(timed):
            if p < 8 * length and needs(length, z, p // 8, p % 4 // 2):
                complete[p % 4 // 2, p // 8] = i + 1
            if q_far <= p < q_far + 2:
                queries = i + 1
        steps, bounds, top, helped = [], [], 0, False
        chosen = sorted(complete, key=lambda k: (k[0], complete[k]))
        for i, (sample, sz) in enumerate(chosen):
            top = max(top, complete[sample, sz])
            flags = 0
            if z in (1, length - 2) and sample == 0:
                if not needs(length, 0 if z == 1 else length - 1, sz, 0):
                    flags, helped, top = 1 if helped else 3, True, max(top, queries)
                if i == length - 1:
                    flags += 4
            steps.append((sample, sz, flags))
            bounds.append(top)
        programs.append((codes, in_loop, max([in_loop, *results]), steps, bounds))
    return programs


def device_plan(length):
    n = 2 * length
    programs = TUNED.get(length) or programs_by_time(length)
    plan = {name: [] for name in ("ops", "bounds", "steps", "n_steps", "in_loop", "to_merge", "n_ops")}
    plan["sent"] = [[0] * n for _ in range(3)]
    for d in range(n):
        z, y = divmod(d, 2)
        codes, in_loop, to_merge, steps, bounds = programs[z if y == 0 else length - 1 - z]
        ops = []
        for code in codes:
            where = code % 8
            if y == 1:
                where = where // 4 * 4 + where // 2 % 2 + where % 2 * 2
            ops.append(mirrored_part(length, y, code // 16) * 16 + code // 8 % 2 * 8 + where)
            for k in range(3):
                plan["sent"][k][d] += where // 2**k % 2
        plan["ops"].append(ops)
        plan["bounds"].append([*bounds, in_loop])
        plan["steps"].append(
            [s + 2 * (sz if y == 0 else length - 1 - sz) + 512 * flags for s, sz, flags in steps]
        )
        for name, value in zip(("n_steps", "in_loop", "to_merge", "n_ops"), (len(steps), in_loop, to_merge, len(ops))):
            plan[name].append(value)
    for name in ("ops", "bounds", "steps"):
        width = max(len(row) for row in plan[name])
        plan[name] = [row + [0] * (width - len(row)) for row in plan[name]]
    return plan


def layer_norm(values, gain, bias):
    values = values.astype(F32)
    centre = jnp.mean(values, -1, keepdims=True)
    centred = values - centre
    spread = jnp.mean(centred * centred, -1, keepdims=True)
    return (centred * lax.rsqrt(spread + EPSILON) * gain + bias).astype(BF16)


def dot(a, b):
    return jnp.dot(a, b, preferred_element_type=F32)


def split_dot(a, b):
    high = a.astype(BF16)
    rest = a - high.astype(F32)
    mid = rest.astype(BF16)
    low = (rest - mid.astype(F32)).astype(BF16)
    return dot(high, b) + dot(mid, b) + dot(low, b)


def kernel(
    n,
    plan,
    hidden_hbm,
    stale_attn_hbm,
    stale_conv_hbm,
    ln_gain_hbm,
    ln_bias_hbm,
    w_qkv_hbm,
    w_out_hbm,
    gn_gain_hbm,
    gn_bias_hbm,
    conv_w_hbm,
    conv_bias_hbm,
    time_shift_hbm,
    out,
    hidden,
    stale_attn,
    ln_gain,
    ln_bias,
    gn_gain,
    gn_bias,
    conv_bias,
    time_shift,
    w_qkv,
    w_out,
    conv_w,
    blocks,
    keys,
    values,
    q_diag,
    soft,
    soft_far,
    accum,
    same_group,
    conv_acc,
    stats,
    load_sem,
    vector_sem,
    send_sem,
    recv_sem,
    soft_sem,
    stat_sem,
):
    samples, _, cols, channels = out.shape
    tokens = samples * cols
    pairs = channels // (2 * HEAD_DIM)
    group_size = channels // GROUPS
    length = n // 2
    own_edge, cross, handed, q_own, q_far, o_own, o_far = special_parts(length)
    fresh_part = 4 * n
    me = lax.axis_index("patch")
    z = me // 2
    y = me % 2
    above_exists = z > 0
    below_exists = z < length - 1
    neighbours = ((above_exists, me - 2), (below_exists, me + 2), (True, z * 2 + 1 - y))

    barrier = pltpu.get_barrier_semaphore()
    for there, device in neighbours:
        def announce(device=device):
            pl.semaphore_signal(barrier, inc=1, device_id={"patch": device}, device_id_type=MESH)
        if there is True:
            announce()
        else:
            pl.when(there)(announce)

    load_stale = pltpu.make_async_copy(stale_attn_hbm, stale_attn, load_sem.at[0])
    load_hidden = pltpu.make_async_copy(hidden_hbm, hidden, load_sem.at[1])
    load_qkv = pltpu.make_async_copy(w_qkv_hbm, w_qkv, load_sem.at[2])
    load_edge = pltpu.make_async_copy(stale_conv_hbm, blocks.at[pl.ds(own_edge, 4)], load_sem.at[3])
    load_out = pltpu.make_async_copy(w_out_hbm, w_out, load_sem.at[4])
    load_conv = pltpu.make_async_copy(conv_w_hbm, conv_w, load_sem.at[5])
    load_shift = pltpu.make_async_copy(time_shift_hbm, time_shift, load_sem.at[6])
    vectors = [
        pltpu.make_async_copy(source, target, vector_sem.at[i])
        for i, (source, target) in enumerate(
            (
                (ln_gain_hbm, ln_gain),
                (ln_bias_hbm, ln_bias),
                (gn_gain_hbm, gn_gain),
                (gn_bias_hbm, gn_bias),
                (conv_bias_hbm, conv_bias),
            )
        )
    ]
    load_stale.start()
    for load in vectors[:2]:
        load.start()
    load_hidden.start()
    load_qkv.start()
    load_edge.start()
    for load in vectors[2:]:
        load.start()
    load_shift.start()
    load_out.start()
    load_conv.start()

    def pick(choices):
        if len(set(choices)) == 1:
            return jnp.int32(choices[0])
        value = jnp.int32(choices[0])
        for k in range(1, n):
            value = jnp.where(me == k, jnp.int32(choices[k]), value)
        return value

    def table(name):
        rows = plan[name]
        bits = max(v for row in rows for v in row).bit_length()
        per = 31 // bits
        words = [
            pick([sum(v << (bits * k) for k, v in enumerate(row[at : at + per])) for row in rows])
            for at in range(0, len(rows[0]), per)
        ]

        def look(i):
            word = words[0]
            for k in range(1, len(words)):
                word = jnp.where(i // per == k, words[k], word)
            return lax.shift_right_logical(word, i % per * bits) & (2**bits - 1)

        return look

    ops, bounds, steps = table("ops"), table("bounds"), table("steps")
    n_steps = pick(plan["n_steps"])
    in_loop = pick(plan["in_loop"])
    to_merge = pick(plan["to_merge"])
    n_ops = pick(plan["n_ops"])
    soft[...] = jnp.zeros_like(soft)
    for slot in range(samples + 1):
        soft[slot, 0] = jnp.full(soft.shape[2:], -jnp.inf, F32)
    accum[...] = jnp.zeros_like(accum)
    q_diag[...] = jnp.zeros_like(q_diag)

    @pl.when(jnp.where(y == 0, z == 0, z == length - 1))
    def _():
        blocks[handed : handed + 4] = jnp.zeros_like(blocks[handed : handed + 4])

    mine = me * 4
    per_sample = 2
    for load in vectors[:2]:
        load.wait()
    load_stale.wait()

    def pump(i, carry):
        op = ops(i)
        part = op // 16
        landed = jnp.where(part < 4 * n, part, part - 8)

        @pl.when(op // 8 % 2 == 1)
        def _():
            pltpu.make_async_remote_copy(
                src_ref=blocks.at[part],
                dst_ref=blocks.at[part],
                send_sem=send_sem.at[0],
                recv_sem=recv_sem.at[landed],
                device_id={"patch": z * 2 + 1 - y},
                device_id_type=MESH,
            ).wait_recv()

        there = jnp.where(part < 4 * n, part, part + 4)
        landing = jnp.where(part < 4 * n, part, part - 4)
        for k, (_, device) in enumerate(neighbours):

            @pl.when(op // 2**k % 2 == 1)
            def _(k=k, device=device):
                pltpu.make_async_remote_copy(
                    src_ref=blocks.at[part],
                    dst_ref=blocks.at[there],
                    send_sem=send_sem.at[k],
                    recv_sem=recv_sem.at[landing],
                    device_id={"patch": device},
                    device_id_type=MESH,
                ).start()

        return carry

    def pumps(first, last):
        lax.fori_loop(first, last, pump, 0)

    def norm_stale(s):
        part = layer_norm(stale_attn[2 * s : 2 * s + 2], ln_gain[...], ln_bias[...])
        blocks[pl.ds(mine + 2 * s, 2)] = part

    norm_stale(0)
    pl.semaphore_wait(barrier, 1 + above_exists.astype(jnp.int32) + below_exists.astype(jnp.int32))
    pumps(0, 2)
    for s in range(1, samples):
        norm_stale(s)

    load_hidden.wait()
    fresh = layer_norm(hidden[...], ln_gain[...], ln_bias[...])
    blocks[fresh_part : fresh_part + 4] = fresh.reshape(4, tokens // 4, channels)
    load_qkv.wait()
    queries = dot(fresh, w_qkv[:, :channels]).astype(BF16).astype(F32) * HEAD_DIM ** (-0.5)
    if MOVED:
        blocks[q_own : q_own + 2] = queries[:cols].astype(BF16).reshape(2, cols // 2, channels)

    def spread_queries(slot, q_t):
        for pair in range(pairs):
            for half in range(2):
                row = (2 * pair + half) * HEAD_DIM
                q_diag[
                    slot, pair, half * HEAD_DIM : (half + 1) * HEAD_DIM, half * cols : (half + 1) * cols
                ] = q_t[row : row + HEAD_DIM]

    q_t = queries.T.astype(BF16)
    for s in range(samples):
        spread_queries(s, q_t[:, s * cols : (s + 1) * cols])
    load_edge.wait()
    pumps(2, bounds(0))
    channel_row = lax.broadcasted_iota(jnp.int32, (channels, channels), 0) // group_size
    channel_col = lax.broadcasted_iota(jnp.int32, (channels, channels), 1) // group_size
    same_group[...] = jnp.where(channel_row == channel_col, 1.0, 0.0).astype(BF16)

    def attend(slot):
        lanes = [slice(pair * 2 * HEAD_DIM, (pair + 1) * 2 * HEAD_DIM) for pair in range(pairs)]
        old_max, old_sum = soft[slot, 0], soft[slot, 1]
        scores = [dot(keys[:, lanes[pair]], q_diag[slot, pair]) for pair in range(pairs)]
        new_max = [
            jnp.maximum(old_max[pair : pair + 1], jnp.max(scores[pair], 0, keepdims=True))
            for pair in range(pairs)
        ]
        weights = [jnp.exp(scores[pair] - new_max[pair]) for pair in range(pairs)]
        both = [lax.dot_general(
                values[:, lanes[pair]],
                weights[pair].astype(BF16),
                (((0,), (0,)), ((), ())),
                preferred_element_type=F32,
            )
            for pair in range(pairs)]
        rescale = [jnp.exp(old_max[pair : pair + 1] - new_max[pair]) for pair in range(pairs)]
        soft[slot, 0] = jnp.concatenate(new_max, 0)
        soft[slot, 1] = jnp.concatenate(
            [
                jnp.sum(weights[pair], 0, keepdims=True) + old_sum[pair : pair + 1] * rescale[pair]
                for pair in range(pairs)
            ],
            0,
        )
        for pair in range(pairs):
            for half in range(2):
                row = (2 * pair + half) * HEAD_DIM
                own = slice(half * cols, (half + 1) * cols)
                accum[slot, row : row + HEAD_DIM] = (
                    both[pair][half * HEAD_DIM : (half + 1) * HEAD_DIM, own]
                    + accum[slot, row : row + HEAD_DIM] * rescale[pair][:, own]
                )

    def normalised(slot):
        for head in range(2 * pairs):
            row = head * HEAD_DIM
            total = soft[slot, 1, head // 2 : head // 2 + 1, (head % 2) * cols : (head % 2 + 1) * cols]
            accum[slot, row : row + HEAD_DIM] = accum[slot, row : row + HEAD_DIM] / total
        return accum[slot].T

    def soft_copy(device):
        return pltpu.make_async_remote_copy(
            src_ref=soft.at[samples],
            dst_ref=soft_far,
            send_sem=soft_sem.at[0],
            recv_sem=soft_sem.at[1],
            device_id={"patch": device},
            device_id_type=MESH,
        )

    at_end = (z == 0) | (z == length - 1)
    helps = (z == 1) | (z == length - 2)
    outward = jnp.where(z == 1, me - 2, me + 2)

    def step(i, carry):
        code = steps(i)
        s = code % 2
        sz = code // 2 % 256
        first_slot = jnp.where(sz == z, n, 2 * sz + y)
        second_slot = 2 * sz + 1 - y
        low = bounds(i)
        span = bounds(i + 1) - low
        marks = [low + span * k // 2 for k in range(3)]
        rows = jnp.concatenate(
            [
                blocks[pl.ds(slot * 4 + 2 * s, 2)].reshape(cols, channels)
                for slot in (first_slot, second_slot)
            ],
            0,
        )
        both_kv = dot(rows, w_qkv[:, channels:]).astype(BF16)
        keys[...] = both_kv[:, :channels]
        values[...] = both_kv[:, channels:]
        pumps(marks[0], marks[1])
        attend(s)
        pumps(marks[1], marks[2])
        if MOVED:
            flag = code // 512

            @pl.when(flag % 2 == 1)
            def _():
                @pl.when(flag // 2 % 2 == 1)
                def _():
                    far = blocks[q_far : q_far + 2].reshape(cols, channels)
                    spread_queries(samples, far.astype(F32).T.astype(BF16))

                attend(samples)

            @pl.when(flag // 4 % 2 == 1)
            def _():
                part = normalised(samples).astype(BF16)
                blocks[o_own : o_own + 2] = part.reshape(2, cols // 2, channels)
                soft_copy(outward).start()
                for k in range(2):
                    pltpu.make_async_remote_copy(
                        src_ref=blocks.at[o_own + k],
                        dst_ref=blocks.at[o_far + k],
                        send_sem=soft_sem.at[2 + k],
                        recv_sem=recv_sem.at[o_far + k - 8],
                        device_id={"patch": outward},
                        device_id_type=MESH,
                    ).start()

        return carry

    lax.fori_loop(0, n_steps, step, 0)
    if MOVED:
        pumps(in_loop, to_merge)

        @pl.when(at_end)
        def _():
            soft_copy(z * 2 + 1 - y).wait_recv()
            far = blocks[o_far : o_far + 2].reshape(cols, channels).astype(F32).T
            for head in range(2 * pairs):
                row = head * HEAD_DIM
                at = (slice(head // 2, head // 2 + 1), slice((head % 2) * cols, (head % 2 + 1) * cols))
                near_max, far_max = soft[(0, 0, *at)], soft_far[(0, *at)]
                top = jnp.maximum(near_max, far_max)
                near_scale = jnp.exp(near_max - top)
                far_sum = soft_far[(1, *at)] * jnp.exp(far_max - top)
                accum[0, row : row + HEAD_DIM] = (
                    accum[0, row : row + HEAD_DIM] * near_scale + far[row : row + HEAD_DIM] * far_sum
                )
                soft[(0, 1, *at)] = soft[(0, 1, *at)] * near_scale + far_sum

    attended = jnp.concatenate([normalised(s) for s in range(samples)], 0).astype(BF16)
    load_out.wait()
    residual = hidden[...].astype(F32) + dot(attended, w_out[...])
    residual = residual.astype(BF16).astype(F32).reshape(samples, cols, channels)

    sum_rows = jnp.concatenate([jnp.sum(residual[s], 0, keepdims=True) for s in range(samples)], 0)
    cells = cols * group_size
    local_mean = split_dot(sum_rows, same_group[...]) / cells
    centred = residual - local_mean[:, None, :]
    square_rows = jnp.concatenate(
        [jnp.sum(centred[s] * centred[s], 0, keepdims=True) for s in range(samples)], 0
    )
    local_square = split_dot(square_rows, same_group[...])
    stats[me, :samples] = local_mean
    stats[me, samples:] = local_square

    def stat_copy(distance):
        return pltpu.make_async_remote_copy(
            src_ref=stats.at[me],
            dst_ref=stats.at[me],
            send_sem=stat_sem.at[0],
            recv_sem=stat_sem.at[1],
            device_id={"patch": lax.rem(me + distance, n)},
            device_id_type=MESH,
        )

    for distance in range(1, n):
        stat_copy(distance).start()

    pumps(to_merge, n_ops)
    load_conv.wait()
    above = blocks[pl.ds(jnp.where(y == 0, handed, cross), 4)].reshape(tokens, channels)
    below = blocks[pl.ds(jnp.where(y == 0, cross, handed), 4)].reshape(tokens, channels)
    for tap in range(3):
        conv_acc[tap] = dot(above, conv_w[0, tap]) + dot(below, conv_w[2, tap])
    for load in vectors[2:]:
        load.wait()
    load_shift.wait()

    others = stats.at[pl.ds(0, n - 1)]
    pltpu.make_async_remote_copy(
        src_ref=others,
        dst_ref=others,
        send_sem=stat_sem.at[0],
        recv_sem=stat_sem.at[1],
        device_id={"patch": z * 2 + 1 - y},
        device_id_type=MESH,
    ).wait_recv()
    every = stats[...]
    group_mean = jnp.mean(every[:, :samples], 0)
    shift = every[:, :samples] - group_mean[None]
    group_var = (jnp.sum(every[:, samples:], 0) + cells * jnp.sum(shift * shift, 0)) / (cells * n)
    scale = lax.rsqrt(group_var + EPSILON)
    pre = (residual - group_mean[:, None, :]) * scale[:, None, :] * gn_gain[...] + gn_bias[...]
    activated = (pre / (1.0 + jnp.exp(-pre))).astype(BF16).reshape(tokens, channels)

    column = lax.broadcasted_iota(jnp.int32, (tokens, 1), 0) % cols
    total = conv_acc[1] + dot(activated, conv_w[1, 1])
    left = pltpu.roll(conv_acc[0] + dot(activated, conv_w[1, 0]), 1, 0)
    total = total + jnp.where(column == 0, 0.0, left)
    right = pltpu.roll(conv_acc[2] + dot(activated, conv_w[1, 2]), tokens - 1, 0)
    total = total + jnp.where(column == cols - 1, 0.0, right)
    total = total.reshape(samples, cols, channels) + conv_bias[...]
    for sample in range(samples):
        out[sample, 0] = (
            total[sample] + time_shift[sample : sample + 1] + residual[sample]
        ).astype(BF16)

    def sent(source, semaphore):
        pltpu.make_async_remote_copy(
            src_ref=source,
            dst_ref=source,
            send_sem=semaphore,
            recv_sem=stat_sem.at[1],
            device_id={"patch": z * 2 + 1 - y},
            device_id_type=MESH,
        ).wait_send()

    sent(others, stat_sem.at[0])
    for k in range(3):
        for count in sorted(set(plan["sent"][k]) - {0}):
            those = [d for d in range(n) if plan["sent"][k][d] == count]
            match = functools.reduce(jnp.logical_or, [me == d for d in those])
            pl.when(match)(lambda: sent(blocks.at[pl.ds(0, count)], send_sem.at[k]))
    if MOVED:

        @pl.when(helps)
        def _():
            sent(soft.at[samples], soft_sem.at[0])
            for k in range(2):
                sent(blocks.at[o_own + k], soft_sem.at[2 + k])


def shards(n, *arrays):
    (hidden, stale_attn, stale_conv, ln_gain, ln_bias, w_qkv, w_out) = arrays[:7]
    (gn_gain, gn_bias, conv_w, conv_bias, time_shift) = arrays[7:]
    samples, rows_dev, cols, channels = hidden.shape
    assert rows_dev == 1 and samples == 2 and n % 2 == 0 and n >= 8, "unsupported split"
    tokens = samples * cols
    pairs = channels // (2 * HEAD_DIM)
    hbm = pl.BlockSpec(memory_space=pl.ANY)
    vmem = pl.BlockSpec(memory_space=pltpu.VMEM)
    dma = pltpu.SemaphoreType.DMA
    plan = device_plan(n // 2)
    parts = 4 * (n + 8)
    slots = samples + 1 if MOVED else samples
    return pl.pallas_call(
        functools.partial(kernel, n, plan),
        out_shape=pltpu.VMEM(hidden.shape, BF16),
        in_specs=[hbm] * 12,
        out_specs=vmem,
        scratch_shapes=[
            pltpu.VMEM((tokens, channels), BF16),
            pltpu.VMEM((4, tokens // 4, channels), BF16),
        ]
        + [pltpu.VMEM((channels,), F32)] * 5
        + [
            pltpu.VMEM(time_shift.shape, F32),
            pltpu.VMEM(w_qkv.shape, BF16),
            pltpu.VMEM(w_out.shape, BF16),
            pltpu.VMEM(conv_w.shape, BF16),
            pltpu.VMEM((parts, tokens // 4, channels), BF16),
            pltpu.VMEM((2 * cols, channels), BF16),
            pltpu.VMEM((2 * cols, channels), BF16),
            pltpu.VMEM((samples + 1, pairs, 2 * HEAD_DIM, 2 * cols), BF16),
            pltpu.VMEM((samples + 1, 2, pairs, 2 * cols), F32),
            pltpu.VMEM((2, pairs, 2 * cols), F32),
            pltpu.VMEM((samples + 1, channels, cols), F32),
            pltpu.VMEM((channels, channels), BF16),
            pltpu.VMEM((3, tokens, channels), F32),
            pltpu.VMEM((n, 2 * samples, channels), F32),
            dma((7,)),
            dma((5,)),
            dma((3,)),
            dma((4 * n + (22 if MOVED else 8),)),
            dma((4,)),
            dma((2,)),
        ],
        compiler_params=pltpu.CompilerParams(
            collective_id=0, has_side_effects=True, vmem_limit_bytes=56 * 2**20
        ),
        name="section",
    )(
        hidden.reshape(tokens, channels),
        stale_attn.reshape(4, tokens // 4, channels),
        stale_conv.reshape(4, tokens // 4, channels),
        ln_gain,
        ln_bias,
        w_qkv,
        w_out,
        gn_gain,
        gn_bias,
        conv_w,
        conv_bias,
        time_shift,
    )


def solution(mesh):
    wide = P("img", "patch", None, None)
    in_specs = (wide, wide, wide) + (P(),) * 8 + (P("img", None),)
    body = functools.partial(shards, mesh.shape["patch"])
    return jax.shard_map(body, mesh=mesh, in_specs=in_specs, out_specs=wide, check_vma=False)
```

```python
import functools
import heapq
import itertools

import jax
import jax.numpy as jnp
from jax import lax
from jax.experimental import pallas as pl
from jax.experimental.pallas import tpu as pltpu
from jax.sharding import PartitionSpec as P

GROUPS = 32
HEAD_DIM = 64
EPSILON = 1e-05
MESH = pl.DeviceIdType.MESH
F32 = jnp.float32
BF16 = jnp.bfloat16

DOWN, UP, ACROSS = 0, 1, 2
MOVED = True
TUNED = {
    4: [
        (
            [6, 22, 54, 38, 612, 770, 786, 136, 90, 628, 122, 74, 172, 152, 650, 188, 248, 316, 106, 300, 698, 232, 428, 200, 444, 376, 360, 580, 596, 216, 488, 504, 968, 682, 984, 666],
            32,
            35,
            [(0, 0, 0), (1, 0, 0), (1, 1, 0), (1, 2, 0), (0, 1, 0), (1, 3, 0)],
            [12, 19, 22, 27, 30, 32],
        ),
        (
            [135, 151, 167, 10, 268, 284, 26, 201, 183, 42, 313, 396, 58, 217, 328, 234, 250, 840, 412, 297, 580, 856, 628, 429, 344, 596, 88, 445, 472, 456, 72, 120, 360, 104, 666, 612, 376, 650, 712, 488, 682, 504, 698, 760, 744, 728],
            42,
            42,
            [(0, 1, 0), (1, 1, 0), (0, 2, 3), (0, 3, 5), (0, 0, 0), (1, 0, 0), (1, 2, 0), (1, 3, 0)],
            [14, 17, 25, 30, 31, 34, 37, 42],
        ),
        (
            [263, 279, 311, 140, 393, 409, 346, 330, 295, 156, 12, 425, 170, 216, 28, 441, 580, 186, 596, 377, 361, 840, 612, 46, 200, 856, 504, 72, 62, 88, 650, 488, 456, 628, 248, 232, 104, 472, 666, 698, 120, 682, 712, 728, 744, 760],
            41,
            41,
            [(0, 2, 0), (1, 2, 0), (0, 1, 3), (0, 0, 5), (1, 3, 0), (1, 1, 0), (0, 3, 0), (1, 0, 0)],
            [8, 21, 26, 30, 32, 36, 38, 41],
        ),
        (
            [389, 405, 580, 437, 785, 280, 421, 769, 628, 505, 344, 316, 300, 172, 489, 457, 360, 188, 376, 44, 696, 473, 60, 612, 264, 232, 248, 596, 328, 104, 968, 120, 712, 984, 664, 760, 648, 728, 680, 744],
            32,
            34,
            [(1, 3, 0), (1, 2, 0), (0, 3, 0), (1, 1, 0), (0, 2, 0), (1, 0, 0)],
            [15, 19, 22, 27, 29, 32],
        ),
    ]
}


def special_parts(length):
    return tuple(8 * length + 4 * k for k in range(1, 8))


def mirrored_part(length, y, part):
    return part if y == 0 or part >= 8 * length else 4 * (2 * length - 1 - part // 4) + part % 4


def transfers(length):
    own_edge, cross, handed, q_own, q_far, o_own, o_far = special_parts(length)
    ends = (0, length - 1)

    def turned(zd, sz, half):
        return abs(sz - zd) == 1 and (half == 1 or (zd not in ends and sz in ends))

    result = {}
    for z, y in itertools.product(range(length), range(2)):
        sends = {}
        sides = [(k, zd) for k, zd in ((DOWN, z - 1), (UP, z + 1)) if 0 <= zd < length]
        for sz, sy, sp in itertools.product(range(length), range(2), range(4)):
            part = (2 * sz + sy) * 4 + sp
            sends[part] = [
                (k, part)
                for k, zd in sides
                if needs(length, zd, sz, sp // 2)
                and ((sz <= z if k == UP else sz >= z) if sy == y else sz == z and turned(zd, sz, sp % 2))
            ]
            if sy == y and needs(length, z, sz, sp // 2) and not turned(z, sz, sp % 2):
                sends[part].append((ACROSS, part))
        on = UP if y == 0 else DOWN
        for k in range(4):
            sends[own_edge + k] = [(ACROSS, cross + k)]
            sends[cross + k] = [(on, handed + k)] if on in dict(sides) else []
        for k in range(2):
            sends[q_own + k] = [(UP if z == 0 else DOWN, q_far + k)] if z in ends else []
            sends[o_own + k] = [(DOWN if z == 1 else UP, o_far + k)] if z in (1, length - 2) else []
        result[z, y] = sends
    return result


def needs(length, z, sz, sample):
    return not (sample == 0 and z in (0, length - 1) and abs(sz - z) > 1)


def programs_by_time(length):
    own_edge, cross, handed, q_own, q_far, o_own, o_far = special_parts(length)
    ends = (0, length - 1)
    sends = transfers(length)
    queues, busy, events, count = {}, {}, [], itertools.count()
    landed = {d: {} for d in sends}
    left, answered = {}, set()
    rank = {own_edge: 5, cross: 4, handed: 4, q_own: 0, q_far: 0, o_own: -1, o_far: -1}

    def push(t, kind, *rest):
        heapq.heappush(events, (t, next(count), kind, rest))

    def offer(t, d, part):
        for k, there in sends[d].get(part, []):
            push(t, "queue", d, k, part, there)

    def launch(t, d, k):
        busy[d, k] = bool(queues[d, k])
        if busy[d, k]:
            _, there, part = heapq.heappop(queues[d, k])
            left.setdefault((d, part), t)
            push(t + 1.76, "sent", d, k, there)

    for d in sends:
        for k in range(4):
            offer(0.0, d, (2 * d[0] + d[1]) * 4 + k)
            offer(0.0, d, own_edge + k)
        for k in range(2):
            if d[0] in ends:
                offer(2.0, d, q_own + k)
    while events:
        t, _, kind, (d, *rest) = heapq.heappop(events)
        z, y = d
        if kind == "queue":
            k, part, there = rest
            u = z if y == 0 else length - 1 - z
            c = mirrored_part(length, y, part)
            if c < 8 * length:
                order = c % 4 // 2 - abs(c // 8 - u) * (0.5 if k == ACROSS else 1.0)
            else:
                order = rank[c // 4 * 4]
            heapq.heappush(queues.setdefault((d, k), []), ((order, c), there, part))
            if not busy.get((d, k)):
                busy[d, k] = True
                push(t, "launch", d, k)
        elif kind == "launch":
            launch(t, d, rest[0])
        elif kind == "sent":
            k, there = rest
            push(t + 1.75, "landed", ((z - 1, y), (z + 1, y), (z, 1 - y))[k], there)
            launch(t, d, k)
        else:
            landed[d][rest[0]] = t
            offer(t + 0.3, d, rest[0])
            if z in (1, length - 2) and d not in answered:
                far = [
                    (2 * sz + sy) * 4 + sp
                    for sz, sy, sp in itertools.product(range(length), range(2), range(2))
                    if not needs(length, 0 if z == 1 else length - 1, sz, 0) and sz != z
                ]
                if all(p in landed[d] for p in (q_far, q_far + 1, *far)):
                    answered.add(d)
                    for k in range(2):
                        offer(t + 2.5, d, o_own + k)
    programs = []
    for z in range(length):
        d = (z, 0)
        timed = [(t, 1, p) for p, t in landed[d].items()]
        timed += [(-2.0, 0, 8 * z + k) for k in range(2)]
        if z in ends:
            timed += [(-1.0, 0, q_own + k) for k in range(2)]
        for p in (8 * z + 2, 8 * z + 3, *range(own_edge, own_edge + 4)):
            timed.append((max(0.0, left[d, p] - 1.0), 0, p))
        timed.sort()
        codes = [p * 16 + 8 * waits + sum(2**k for k, _ in sends[d].get(p, [])) for _, waits, p in timed]
        in_loop = 1 + max(i for i, (_, _, p) in enumerate(timed) if p < 8 * length)
        results = [i + 1 for i, (_, _, p) in enumerate(timed) if p >= o_far]
        complete, queries = {}, 0
        for i, (_, _, p) in enumerate(timed):
            if p < 8 * length and needs(length, z, p // 8, p % 4 // 2):
                complete[p % 4 // 2, p // 8] = i + 1
            if q_far <= p < q_far + 2:
                queries = i + 1
        steps, bounds, top, helped = [], [], 0, False
        chosen = sorted(complete, key=lambda k: (complete[k], k))
        for i, (sample, sz) in enumerate(chosen):
            top = max(top, complete[sample, sz])
            flags = 0
            if z in (1, length - 2) and sample == 0:
                if not needs(length, 0 if z == 1 else length - 1, sz, 0):
                    flags, helped, top = 1 if helped else 3, True, max(top, queries)
                    last_far = i
            steps.append([sample, sz, flags])
            bounds.append(top)
        if z in (1, length - 2):
            steps[last_far][2] += 4
        programs.append((codes, in_loop, max([in_loop, *results]), steps, bounds))
    return programs


def device_plan(length):
    n = 2 * length
    cross = special_parts(length)[1]
    programs = TUNED.get(length) or programs_by_time(length)
    plan = {name: [] for name in ("ops", "bounds", "steps", "n_steps", "in_loop", "to_merge", "crossed", "n_ops")}
    plan["sent"] = [[0] * n for _ in range(3)]
    for d in range(n):
        z, y = divmod(d, 2)
        codes, in_loop, to_merge, steps, bounds = programs[z if y == 0 else length - 1 - z]
        ops = []
        for code in codes:
            where = code % 8
            if y == 1:
                where = where // 4 * 4 + where // 2 % 2 + where % 2 * 2
            ops.append(mirrored_part(length, y, code // 16) * 16 + code // 8 % 2 * 8 + where)
            for k in range(3):
                plan["sent"][k][d] += where // 2**k % 2
        plan["ops"].append(ops)
        plan["bounds"].append([*bounds, in_loop])
        plan["steps"].append(
            [s + 2 * (sz if y == 0 else length - 1 - sz) + 512 * flags for s, sz, flags in steps]
        )
        across = [i + 1 for i, code in enumerate(codes) if cross <= code // 16 < cross + 4]
        plan["n_steps"].append(len(steps))
        plan["in_loop"].append(in_loop)
        plan["to_merge"].append(to_merge)
        plan["crossed"].append(max(to_merge, *across))
        plan["n_ops"].append(len(ops))
    for name in ("ops", "bounds", "steps"):
        width = max(len(row) for row in plan[name])
        plan[name] = [row + [0] * (width - len(row)) for row in plan[name]]
    return plan


def layer_norm(values, gain, bias):
    values = values.astype(F32)
    centre = jnp.mean(values, -1, keepdims=True)
    centred = values - centre
    spread = jnp.mean(centred * centred, -1, keepdims=True)
    return (centred * lax.rsqrt(spread + EPSILON) * gain + bias).astype(BF16)


def dot(a, b):
    return jnp.dot(a, b, preferred_element_type=F32)


def balanced_dot(a, b):
    wide = b.shape[1] // 512 * 512
    half = a.shape[0] // 2
    rest = b[:, wide:]
    tail = jnp.concatenate([dot(a[:half], rest), dot(a[half:], rest)], 0)
    return jnp.concatenate([dot(a, b[:, :wide]), tail], 1)


def split_dot(a, b):
    high = a.astype(BF16)
    rest = a - high.astype(F32)
    mid = rest.astype(BF16)
    low = (rest - mid.astype(F32)).astype(BF16)
    rows = a.shape[0]
    thirds = dot(jnp.concatenate([high, mid, low], 0), b)
    return thirds[:rows] + thirds[rows : 2 * rows] + thirds[2 * rows :]


def kernel(
    n,
    plan,
    hidden_hbm,
    stale_attn_hbm,
    stale_conv_hbm,
    ln_gain_hbm,
    ln_bias_hbm,
    w_qkv_hbm,
    w_out_hbm,
    gn_gain_hbm,
    gn_bias_hbm,
    conv_w_hbm,
    conv_bias_hbm,
    time_shift_hbm,
    out,
    hidden,
    stale_attn,
    ln_gain,
    ln_bias,
    gn_gain,
    gn_bias,
    conv_bias,
    time_shift,
    w_qkv,
    w_out,
    conv_w,
    blocks,
    keys,
    values,
    q_diag,
    soft,
    soft_far,
    accum,
    same_group,
    conv_acc,
    stats,
    load_sem,
    vector_sem,
    send_sem,
    recv_sem,
    soft_sem,
    stat_sem,
):
    samples, _, cols, channels = out.shape
    tokens = samples * cols
    pairs = channels // (2 * HEAD_DIM)
    group_size = channels // GROUPS
    length = n // 2
    own_edge, cross, handed, q_own, q_far, o_own, o_far = special_parts(length)
    fresh_part = 4 * n
    me = lax.axis_index("patch")
    z = me // 2
    y = me % 2
    above_exists = z > 0
    below_exists = z < length - 1
    neighbours = ((above_exists, me - 2), (below_exists, me + 2), (True, z * 2 + 1 - y))

    barrier = pltpu.get_barrier_semaphore()
    for there, device in neighbours:
        def announce(device=device):
            pl.semaphore_signal(barrier, inc=1, device_id={"patch": device}, device_id_type=MESH)
        if there is True:
            announce()
        else:
            pl.when(there)(announce)

    load_stale = pltpu.make_async_copy(stale_attn_hbm, stale_attn, load_sem.at[0])
    load_hidden = pltpu.make_async_copy(hidden_hbm, hidden, load_sem.at[1])
    load_qkv = pltpu.make_async_copy(w_qkv_hbm, w_qkv, load_sem.at[2])
    load_edge = pltpu.make_async_copy(stale_conv_hbm, blocks.at[pl.ds(own_edge, 4)], load_sem.at[3])
    load_out = pltpu.make_async_copy(w_out_hbm, w_out, load_sem.at[4])
    load_conv = [
        pltpu.make_async_copy(
            conv_w_hbm.at[row, tap],
            conv_w.at[row, :, pl.ds(tap * channels, channels)],
            load_sem.at[5],
        )
        for row in range(3)
        for tap in range(3)
    ]
    load_shift = pltpu.make_async_copy(time_shift_hbm, time_shift, load_sem.at[6])
    vectors = [
        pltpu.make_async_copy(source, target, vector_sem.at[i])
        for i, (source, target) in enumerate(
            (
                (ln_gain_hbm, ln_gain),
                (ln_bias_hbm, ln_bias),
                (gn_gain_hbm, gn_gain),
                (gn_bias_hbm, gn_bias),
                (conv_bias_hbm, conv_bias),
            )
        )
    ]
    load_stale.start()
    for load in vectors[:2]:
        load.start()
    load_hidden.start()

    def pick(choices):
        if len(set(choices)) == 1:
            return jnp.int32(choices[0])
        value = jnp.int32(choices[0])
        for k in range(1, n):
            value = jnp.where(me == k, jnp.int32(choices[k]), value)
        return value

    def table(name):
        rows = plan[name]
        bits = max(v for row in rows for v in row).bit_length()
        per = 31 // bits
        words = [
            pick([sum(v << (bits * k) for k, v in enumerate(row[at : at + per])) for row in rows])
            for at in range(0, len(rows[0]), per)
        ]

        def look(i):
            word = words[0]
            for k in range(1, len(words)):
                word = jnp.where(i // per == k, words[k], word)
            return lax.shift_right_logical(word, i % per * bits) & (2**bits - 1)

        return look

    ops, bounds, steps = table("ops"), table("bounds"), table("steps")
    n_steps = pick(plan["n_steps"])
    in_loop = pick(plan["in_loop"])
    to_merge = pick(plan["to_merge"])
    crossed = pick(plan["crossed"])
    n_ops = pick(plan["n_ops"])
    soft[...] = jnp.zeros_like(soft)
    for slot in range(samples + 1):
        soft[slot, 0] = jnp.full(soft.shape[2:], -jnp.inf, F32)
    accum[...] = jnp.zeros_like(accum)
    q_diag[...] = jnp.zeros_like(q_diag)

    @pl.when(jnp.where(y == 0, z == 0, z == length - 1))
    def _():
        blocks[handed : handed + 4] = jnp.zeros_like(blocks[handed : handed + 4])

    mine = me * 4
    per_sample = 2
    for load in vectors[:2]:
        load.wait()
    load_stale.wait()
    load_qkv.start()
    load_edge.start()
    for load in vectors[2:]:
        load.start()
    load_shift.start()
    load_out.start()
    for load in load_conv:
        load.start()

    def pump(i, carry):
        op = ops(i)
        part = op // 16
        landed = jnp.where(part < 4 * n, part, part - 8)

        @pl.when(op // 8 % 2 == 1)
        def _():
            pltpu.make_async_remote_copy(
                src_ref=blocks.at[part],
                dst_ref=blocks.at[part],
                send_sem=send_sem.at[0],
                recv_sem=recv_sem.at[landed],
                device_id={"patch": z * 2 + 1 - y},
                device_id_type=MESH,
            ).wait_recv()

        there = jnp.where(part < 4 * n, part, part + 4)
        landing = jnp.where(part < 4 * n, part, part - 4)
        for k, (_, device) in enumerate(neighbours):

            @pl.when(op // 2**k % 2 == 1)
            def _(k=k, device=device):
                pltpu.make_async_remote_copy(
                    src_ref=blocks.at[part],
                    dst_ref=blocks.at[there],
                    send_sem=send_sem.at[k],
                    recv_sem=recv_sem.at[landing],
                    device_id={"patch": device},
                    device_id_type=MESH,
                ).start()

        return carry

    def pumps(first, last):
        lax.fori_loop(first, last, pump, 0)

    def norm_stale(s):
        part = layer_norm(stale_attn[2 * s : 2 * s + 2], ln_gain[...], ln_bias[...])
        blocks[pl.ds(mine + 2 * s, 2)] = part

    norm_stale(0)
    pl.semaphore_wait(barrier, 1 + above_exists.astype(jnp.int32) + below_exists.astype(jnp.int32))
    pumps(0, 2)
    for s in range(1, samples):
        norm_stale(s)

    load_hidden.wait()
    fresh = layer_norm(hidden[...], ln_gain[...], ln_bias[...])
    blocks[fresh_part : fresh_part + 4] = fresh.reshape(4, tokens // 4, channels)
    load_qkv.wait()
    queries = dot(fresh, w_qkv[:, :channels]).astype(BF16).astype(F32) * HEAD_DIM ** (-0.5)
    if MOVED:
        blocks[q_own : q_own + 2] = queries[:cols].astype(BF16).reshape(2, cols // 2, channels)

    def spread_queries(slot, q_t):
        for pair in range(pairs):
            for half in range(2):
                row = (2 * pair + half) * HEAD_DIM
                q_diag[
                    slot, pair, half * HEAD_DIM : (half + 1) * HEAD_DIM, half * cols : (half + 1) * cols
                ] = q_t[row : row + HEAD_DIM]

    q_t = queries.T.astype(BF16)
    for s in range(samples):
        spread_queries(s, q_t[:, s * cols : (s + 1) * cols])
    load_edge.wait()
    pumps(2, bounds(0))
    channel_row = lax.broadcasted_iota(jnp.int32, (channels, channels), 0) // group_size
    channel_col = lax.broadcasted_iota(jnp.int32, (channels, channels), 1) // group_size
    same_group[...] = jnp.where(channel_row == channel_col, 1.0, 0.0).astype(BF16)

    def attend(slot):
        lanes = [slice(pair * 2 * HEAD_DIM, (pair + 1) * 2 * HEAD_DIM) for pair in range(pairs)]
        old_max, old_sum = soft[slot, 0], soft[slot, 1]
        scores = [dot(keys[:, lanes[pair]], q_diag[slot, pair]) for pair in range(pairs)]
        new_max = [
            jnp.maximum(old_max[pair : pair + 1], jnp.max(scores[pair], 0, keepdims=True))
            for pair in range(pairs)
        ]
        weights = [jnp.exp(scores[pair] - new_max[pair]) for pair in range(pairs)]
        both = [lax.dot_general(
                values[:, lanes[pair]],
                weights[pair].astype(BF16),
                (((0,), (0,)), ((), ())),
                preferred_element_type=F32,
            )
            for pair in range(pairs)]
        rescale = [jnp.exp(old_max[pair : pair + 1] - new_max[pair]) for pair in range(pairs)]
        soft[slot, 0] = jnp.concatenate(new_max, 0)
        soft[slot, 1] = jnp.concatenate(
            [
                jnp.sum(weights[pair], 0, keepdims=True) + old_sum[pair : pair + 1] * rescale[pair]
                for pair in range(pairs)
            ],
            0,
        )
        for pair in range(pairs):
            for half in range(2):
                row = (2 * pair + half) * HEAD_DIM
                own = slice(half * cols, (half + 1) * cols)
                accum[slot, row : row + HEAD_DIM] = (
                    both[pair][half * HEAD_DIM : (half + 1) * HEAD_DIM, own]
                    + accum[slot, row : row + HEAD_DIM] * rescale[pair][:, own]
                )

    def normalised(slot):
        for head in range(2 * pairs):
            row = head * HEAD_DIM
            total = soft[slot, 1, head // 2 : head // 2 + 1, (head % 2) * cols : (head % 2 + 1) * cols]
            accum[slot, row : row + HEAD_DIM] = accum[slot, row : row + HEAD_DIM] * (1.0 / total)
        return accum[slot].T

    def soft_copy(device):
        return pltpu.make_async_remote_copy(
            src_ref=soft.at[samples],
            dst_ref=soft_far,
            send_sem=soft_sem.at[0],
            recv_sem=soft_sem.at[1],
            device_id={"patch": device},
            device_id_type=MESH,
        )

    at_end = (z == 0) | (z == length - 1)
    helps = (z == 1) | (z == length - 2)
    outward = jnp.where(z == 1, me - 2, me + 2)

    def step(i, carry):
        code = steps(i)
        s = code % 2
        sz = code // 2 % 256
        first_slot = jnp.where(sz == z, n, 2 * sz + y)
        second_slot = 2 * sz + 1 - y
        low = bounds(i)
        span = bounds(i + 1) - low
        marks = [low + span * k // 2 for k in range(3)]
        rows = jnp.concatenate(
            [
                blocks[pl.ds(slot * 4 + 2 * s, 2)].reshape(cols, channels)
                for slot in (first_slot, second_slot)
            ],
            0,
        )
        both_kv = balanced_dot(rows, w_qkv[:, channels:]).astype(BF16)
        keys[...] = both_kv[:, :channels]
        values[...] = both_kv[:, channels:]
        pumps(marks[0], marks[1])
        attend(s)
        pumps(marks[1], marks[2])
        if MOVED:
            flag = code // 512

            @pl.when(flag % 2 == 1)
            def _():
                @pl.when(flag // 2 % 2 == 1)
                def _():
                    far = blocks[q_far : q_far + 2].reshape(cols, channels)
                    spread_queries(samples, far.astype(F32).T.astype(BF16))

                attend(samples)

            @pl.when(flag // 4 % 2 == 1)
            def _():
                part = normalised(samples).astype(BF16)
                blocks[o_own : o_own + 2] = part.reshape(2, cols // 2, channels)
                soft_copy(outward).start()
                for k in range(2):
                    pltpu.make_async_remote_copy(
                        src_ref=blocks.at[o_own + k],
                        dst_ref=blocks.at[o_far + k],
                        send_sem=soft_sem.at[2 + k],
                        recv_sem=recv_sem.at[o_far + k - 8],
                        device_id={"patch": outward},
                        device_id_type=MESH,
                    ).start()

        return carry

    lax.fori_loop(0, n_steps, step, 0)
    if MOVED:
        pumps(in_loop, to_merge)

        @pl.when(at_end)
        def _():
            soft_copy(z * 2 + 1 - y).wait_recv()
            far = blocks[o_far : o_far + 2].reshape(cols, channels).astype(F32).T
            for head in range(2 * pairs):
                row = head * HEAD_DIM
                at = (slice(head // 2, head // 2 + 1), slice((head % 2) * cols, (head % 2 + 1) * cols))
                near_max, far_max = soft[(0, 0, *at)], soft_far[(0, *at)]
                top = jnp.maximum(near_max, far_max)
                near_scale = jnp.exp(near_max - top)
                far_sum = soft_far[(1, *at)] * jnp.exp(far_max - top)
                accum[0, row : row + HEAD_DIM] = (
                    accum[0, row : row + HEAD_DIM] * near_scale + far[row : row + HEAD_DIM] * far_sum
                )
                soft[(0, 1, *at)] = soft[(0, 1, *at)] * near_scale + far_sum

    attended = jnp.concatenate([normalised(s) for s in range(samples)], 0).astype(BF16)
    load_out.wait()
    residual = hidden[...].astype(F32) + balanced_dot(attended, w_out[...])
    residual = residual.astype(BF16).astype(F32).reshape(samples, cols, channels)

    sum_rows = jnp.concatenate([jnp.sum(residual[s], 0, keepdims=True) for s in range(samples)], 0)
    cells = cols * group_size
    local_mean = split_dot(sum_rows, same_group[...]) / cells
    centred = residual - local_mean[:, None, :]
    square_rows = jnp.concatenate(
        [jnp.sum(centred[s] * centred[s], 0, keepdims=True) for s in range(samples)], 0
    )
    local_square = split_dot(square_rows, same_group[...])
    stats[me, :samples] = local_mean
    stats[me, samples:] = local_square

    def stat_copy(distance):
        return pltpu.make_async_remote_copy(
            src_ref=stats.at[me],
            dst_ref=stats.at[me],
            send_sem=stat_sem.at[0],
            recv_sem=stat_sem.at[1],
            device_id={"patch": lax.rem(me + distance, n)},
            device_id_type=MESH,
        )

    for distance in range(1, n):
        stat_copy(distance).start()

    pumps(to_merge, crossed)
    pltpu.make_async_copy(conv_w, conv_w, load_sem.at[5]).wait()
    cross_row = jnp.where(y == 0, 2, 0)
    conv_acc[...] = dot(blocks[cross : cross + 4].reshape(tokens, channels), conv_w[cross_row])
    pumps(crossed, n_ops)
    conv_acc[...] += dot(blocks[handed : handed + 4].reshape(tokens, channels), conv_w[2 - cross_row])
    for load in vectors[2:]:
        load.wait()
    load_shift.wait()

    others = stats.at[pl.ds(0, n - 1)]
    pltpu.make_async_remote_copy(
        src_ref=others,
        dst_ref=others,
        send_sem=stat_sem.at[0],
        recv_sem=stat_sem.at[1],
        device_id={"patch": z * 2 + 1 - y},
        device_id_type=MESH,
    ).wait_recv()
    every = stats[...]
    group_mean = jnp.mean(every[:, :samples], 0)
    shift = every[:, :samples] - group_mean[None]
    group_var = (jnp.sum(every[:, samples:], 0) + cells * jnp.sum(shift * shift, 0)) / (cells * n)
    scale = lax.rsqrt(group_var + EPSILON)
    pre = (residual - group_mean[:, None, :]) * scale[:, None, :] * gn_gain[...] + gn_bias[...]
    activated = (pre / (1.0 + jnp.exp(-pre))).astype(BF16).reshape(tokens, channels)

    column = lax.broadcasted_iota(jnp.int32, (tokens, 1), 0) % cols
    taps = conv_acc[...] + dot(activated, conv_w[1])
    left, total, right = (taps[:, tap * channels : (tap + 1) * channels] for tap in range(3))
    total = total + jnp.where(column == 0, 0.0, pltpu.roll(left, 1, 0))
    total = total + jnp.where(column == cols - 1, 0.0, pltpu.roll(right, tokens - 1, 0))
    total = total.reshape(samples, cols, channels) + conv_bias[...]
    for sample in range(samples):
        out[sample, 0] = (
            total[sample] + time_shift[sample : sample + 1] + residual[sample]
        ).astype(BF16)

    def sent(source, semaphore):
        pltpu.make_async_remote_copy(
            src_ref=source,
            dst_ref=source,
            send_sem=semaphore,
            recv_sem=stat_sem.at[1],
            device_id={"patch": z * 2 + 1 - y},
            device_id_type=MESH,
        ).wait_send()

    sent(others, stat_sem.at[0])
    for k in range(3):
        for count in sorted(set(plan["sent"][k]) - {0}):
            those = [d for d in range(n) if plan["sent"][k][d] == count]
            match = functools.reduce(jnp.logical_or, [me == d for d in those])
            pl.when(match)(lambda: sent(blocks.at[pl.ds(0, count)], send_sem.at[k]))
    if MOVED:

        @pl.when(helps)
        def _():
            sent(soft.at[samples], soft_sem.at[0])
            for k in range(2):
                sent(blocks.at[o_own + k], soft_sem.at[2 + k])


def shards(n, *arrays):
    (hidden, stale_attn, stale_conv, ln_gain, ln_bias, w_qkv, w_out) = arrays[:7]
    (gn_gain, gn_bias, conv_w, conv_bias, time_shift) = arrays[7:]
    samples, rows_dev, cols, channels = hidden.shape
    assert rows_dev == 1 and samples == 2 and n % 2 == 0 and n >= 8, "unsupported split"
    tokens = samples * cols
    pairs = channels // (2 * HEAD_DIM)
    hbm = pl.BlockSpec(memory_space=pl.ANY)
    vmem = pl.BlockSpec(memory_space=pltpu.VMEM)
    dma = pltpu.SemaphoreType.DMA
    plan = device_plan(n // 2)
    parts = 4 * (n + 8)
    slots = samples + 1 if MOVED else samples
    return pl.pallas_call(
        functools.partial(kernel, n, plan),
        out_shape=pltpu.VMEM(hidden.shape, BF16),
        in_specs=[hbm] * 12,
        out_specs=vmem,
        scratch_shapes=[
            pltpu.VMEM((tokens, channels), BF16),
            pltpu.VMEM((4, tokens // 4, channels), BF16),
        ]
        + [pltpu.VMEM((channels,), F32)] * 5
        + [
            pltpu.VMEM(time_shift.shape, F32),
            pltpu.VMEM(w_qkv.shape, BF16),
            pltpu.VMEM(w_out.shape, BF16),
            pltpu.VMEM((3, channels, 3 * channels), BF16),
            pltpu.VMEM((parts, tokens // 4, channels), BF16),
            pltpu.VMEM((2 * cols, channels), BF16),
            pltpu.VMEM((2 * cols, channels), BF16),
            pltpu.VMEM((samples + 1, pairs, 2 * HEAD_DIM, 2 * cols), BF16),
            pltpu.VMEM((samples + 1, 2, pairs, 2 * cols), F32),
            pltpu.VMEM((2, pairs, 2 * cols), F32),
            pltpu.VMEM((samples + 1, channels, cols), F32),
            pltpu.VMEM((channels, channels), BF16),
            pltpu.VMEM((tokens, 3 * channels), F32),
            pltpu.VMEM((n, 2 * samples, channels), F32),
            dma((7,)),
            dma((5,)),
            dma((3,)),
            dma((4 * n + (22 if MOVED else 8),)),
            dma((4,)),
            dma((2,)),
        ],
        compiler_params=pltpu.CompilerParams(
            collective_id=0, has_side_effects=True, vmem_limit_bytes=56 * 2**20
        ),
        name="section",
    )(
        hidden.reshape(tokens, channels),
        stale_attn.reshape(4, tokens // 4, channels),
        stale_conv.reshape(4, tokens // 4, channels),
        ln_gain,
        ln_bias,
        w_qkv,
        w_out,
        gn_gain,
        gn_bias,
        conv_w,
        conv_bias,
        time_shift,
    )


def solution(mesh):
    wide = P("img", "patch", None, None)
    in_specs = (wide, wide, wide) + (P(),) * 8 + (P("img", None),)
    body = functools.partial(shards, mesh.shape["patch"])
    return jax.shard_map(body, mesh=mesh, in_specs=in_specs, out_specs=wide, check_vma=False)
```

```python
import functools
import heapq
import itertools

import jax
import jax.numpy as jnp
from jax import lax
from jax.experimental import pallas as pl
from jax.experimental.pallas import tpu as pltpu
from jax.sharding import PartitionSpec as P

GROUPS = 32
HEAD_DIM = 64
LANES = 128
EPSILON = 1e-05
MESH = pl.DeviceIdType.MESH
F32 = jnp.float32
BF16 = jnp.bfloat16

DOWN, UP, ACROSS = 0, 1, 2
MOVED = True
TUNED = {
    4: [
        (
            [6, 22, 54, 38, 612, 770, 786, 136, 90, 628, 122, 74, 172, 152, 650, 188, 248, 316, 106, 300, 698, 232, 428, 200, 444, 376, 360, 580, 596, 216, 488, 504, 968, 682, 984, 666],
            32,
            35,
            [(0, 0, 0), (1, 0, 0), (1, 1, 0), (1, 2, 0), (0, 1, 0), (1, 3, 0)],
            [12, 19, 22, 27, 30, 32],
        ),
        (
            [135, 151, 167, 10, 268, 284, 26, 201, 183, 42, 313, 396, 58, 217, 328, 234, 250, 840, 412, 297, 580, 856, 628, 429, 344, 596, 88, 445, 472, 456, 72, 120, 360, 104, 666, 612, 376, 650, 712, 488, 682, 504, 698, 760, 744, 728],
            42,
            42,
            [(0, 1, 0), (1, 1, 0), (0, 2, 3), (0, 3, 5), (0, 0, 0), (1, 0, 0), (1, 2, 0), (1, 3, 0)],
            [14, 17, 25, 30, 31, 34, 37, 42],
        ),
        (
            [263, 279, 311, 140, 393, 409, 346, 330, 295, 156, 12, 425, 170, 216, 28, 441, 580, 186, 596, 377, 361, 840, 612, 46, 200, 856, 504, 72, 62, 88, 650, 488, 456, 628, 248, 232, 104, 472, 666, 698, 120, 682, 712, 728, 744, 760],
            41,
            41,
            [(0, 2, 0), (1, 2, 0), (0, 1, 3), (0, 0, 5), (1, 3, 0), (1, 1, 0), (0, 3, 0), (1, 0, 0)],
            [8, 21, 26, 30, 32, 36, 38, 41],
        ),
        (
            [389, 405, 580, 437, 785, 280, 421, 769, 628, 505, 344, 316, 300, 172, 489, 457, 360, 188, 376, 44, 696, 473, 60, 612, 264, 232, 248, 596, 328, 104, 968, 120, 712, 984, 664, 760, 648, 728, 680, 744],
            32,
            34,
            [(1, 3, 0), (1, 2, 0), (0, 3, 0), (1, 1, 0), (0, 2, 0), (1, 0, 0)],
            [15, 19, 22, 27, 29, 32],
        ),
    ]
}


def special_parts(length):
    return tuple(8 * length + 4 * k for k in range(1, 8))


def mirrored_part(length, y, part):
    return part if y == 0 or part >= 8 * length else 4 * (2 * length - 1 - part // 4) + part % 4


def transfers(length):
    own_edge, cross, handed, q_own, q_far, o_own, o_far = special_parts(length)
    ends = (0, length - 1)

    def turned(zd, sz, half):
        return abs(sz - zd) == 1 and (half == 1 or (zd not in ends and sz in ends))

    result = {}
    for z, y in itertools.product(range(length), range(2)):
        sends = {}
        sides = [(k, zd) for k, zd in ((DOWN, z - 1), (UP, z + 1)) if 0 <= zd < length]
        for sz, sy, sp in itertools.product(range(length), range(2), range(4)):
            part = (2 * sz + sy) * 4 + sp
            sends[part] = [
                (k, part)
                for k, zd in sides
                if needs(length, zd, sz, sp // 2)
                and ((sz <= z if k == UP else sz >= z) if sy == y else sz == z and turned(zd, sz, sp % 2))
            ]
            if sy == y and needs(length, z, sz, sp // 2) and not turned(z, sz, sp % 2):
                sends[part].append((ACROSS, part))
        on = UP if y == 0 else DOWN
        for k in range(4):
            sends[own_edge + k] = [(ACROSS, cross + k)]
            sends[cross + k] = [(on, handed + k)] if on in dict(sides) else []
        for k in range(2):
            sends[q_own + k] = [(UP if z == 0 else DOWN, q_far + k)] if z in ends else []
            sends[o_own + k] = [(DOWN if z == 1 else UP, o_far + k)] if z in (1, length - 2) else []
        result[z, y] = sends
    return result


def needs(length, z, sz, sample):
    return not (sample == 0 and z in (0, length - 1) and abs(sz - z) > 1)


def programs_by_time(length):
    own_edge, cross, handed, q_own, q_far, o_own, o_far = special_parts(length)
    ends = (0, length - 1)
    sends = transfers(length)
    queues, busy, events, count = {}, {}, [], itertools.count()
    landed = {d: {} for d in sends}
    left, answered = {}, set()
    rank = {own_edge: 5, cross: 4, handed: 4, q_own: 0, q_far: 0, o_own: -1, o_far: -1}

    def push(t, kind, *rest):
        heapq.heappush(events, (t, next(count), kind, rest))

    def offer(t, d, part):
        for k, there in sends[d].get(part, []):
            push(t, "queue", d, k, part, there)

    def launch(t, d, k):
        busy[d, k] = bool(queues[d, k])
        if busy[d, k]:
            _, there, part = heapq.heappop(queues[d, k])
            left.setdefault((d, part), t)
            push(t + 1.76, "sent", d, k, there)

    for d in sends:
        for k in range(4):
            offer(0.0, d, (2 * d[0] + d[1]) * 4 + k)
            offer(0.0, d, own_edge + k)
        for k in range(2):
            if d[0] in ends:
                offer(2.0, d, q_own + k)
    while events:
        t, _, kind, (d, *rest) = heapq.heappop(events)
        z, y = d
        if kind == "queue":
            k, part, there = rest
            u = z if y == 0 else length - 1 - z
            c = mirrored_part(length, y, part)
            if c < 8 * length:
                order = c % 4 // 2 - abs(c // 8 - u) * (0.5 if k == ACROSS else 1.0)
            else:
                order = rank[c // 4 * 4]
            heapq.heappush(queues.setdefault((d, k), []), ((order, c), there, part))
            if not busy.get((d, k)):
                busy[d, k] = True
                push(t, "launch", d, k)
        elif kind == "launch":
            launch(t, d, rest[0])
        elif kind == "sent":
            k, there = rest
            push(t + 1.75, "landed", ((z - 1, y), (z + 1, y), (z, 1 - y))[k], there)
            launch(t, d, k)
        else:
            landed[d][rest[0]] = t
            offer(t + 0.3, d, rest[0])
            if z in (1, length - 2) and d not in answered:
                far = [
                    (2 * sz + sy) * 4 + sp
                    for sz, sy, sp in itertools.product(range(length), range(2), range(2))
                    if not needs(length, 0 if z == 1 else length - 1, sz, 0) and sz != z
                ]
                if all(p in landed[d] for p in (q_far, q_far + 1, *far)):
                    answered.add(d)
                    for k in range(2):
                        offer(t + 2.5, d, o_own + k)
    programs = []
    for z in range(length):
        d = (z, 0)
        timed = [(t, 1, p) for p, t in landed[d].items()]
        timed += [(-2.0, 0, 8 * z + k) for k in range(2)]
        if z in ends:
            timed += [(-1.0, 0, q_own + k) for k in range(2)]
        for p in (8 * z + 2, 8 * z + 3, *range(own_edge, own_edge + 4)):
            timed.append((max(0.0, left[d, p] - 1.0), 0, p))
        timed.sort()
        codes = [p * 16 + 8 * waits + sum(2**k for k, _ in sends[d].get(p, [])) for _, waits, p in timed]
        in_loop = 1 + max(i for i, (_, _, p) in enumerate(timed) if p < 8 * length)
        results = [i + 1 for i, (_, _, p) in enumerate(timed) if p >= o_far]
        complete, queries = {}, 0
        for i, (_, _, p) in enumerate(timed):
            if p < 8 * length and needs(length, z, p // 8, p % 4 // 2):
                complete[p % 4 // 2, p // 8] = i + 1
            if q_far <= p < q_far + 2:
                queries = i + 1
        steps, bounds, top, helped = [], [], 0, False
        chosen = sorted(complete, key=lambda k: (complete[k], k))
        for i, (sample, sz) in enumerate(chosen):
            top = max(top, complete[sample, sz])
            flags = 0
            if z in (1, length - 2) and sample == 0:
                if not needs(length, 0 if z == 1 else length - 1, sz, 0):
                    flags, helped, top = 1 if helped else 3, True, max(top, queries)
                    last_far = i
            steps.append([sample, sz, flags])
            bounds.append(top)
        if z in (1, length - 2):
            steps[last_far][2] += 4
        programs.append((codes, in_loop, max([in_loop, *results]), steps, bounds))
    return programs


def device_plan(length):
    n = 2 * length
    cross = special_parts(length)[1]
    programs = TUNED.get(length) or programs_by_time(length)
    plan = {name: [] for name in ("ops", "bounds", "steps", "n_steps", "in_loop", "to_merge", "crossed", "n_ops")}
    plan["sent"] = [[0] * n for _ in range(3)]
    for d in range(n):
        z, y = divmod(d, 2)
        codes, in_loop, to_merge, steps, bounds = programs[z if y == 0 else length - 1 - z]
        ops = []
        for code in codes:
            where = code % 8
            if y == 1:
                where = where // 4 * 4 + where // 2 % 2 + where % 2 * 2
            ops.append(mirrored_part(length, y, code // 16) * 16 + code // 8 % 2 * 8 + where)
            for k in range(3):
                plan["sent"][k][d] += where // 2**k % 2
        plan["ops"].append(ops)
        plan["bounds"].append([*bounds, in_loop])
        plan["steps"].append(
            [s + 2 * (sz if y == 0 else length - 1 - sz) + 512 * flags for s, sz, flags in steps]
        )
        across = [i + 1 for i, code in enumerate(codes) if cross <= code // 16 < cross + 4]
        plan["n_steps"].append(len(steps))
        plan["in_loop"].append(in_loop)
        plan["to_merge"].append(to_merge)
        plan["crossed"].append(max(to_merge, *across))
        plan["n_ops"].append(len(ops))
    for name in ("ops", "bounds", "steps"):
        width = max(len(row) for row in plan[name])
        plan[name] = [row + [0] * (width - len(row)) for row in plan[name]]
    return plan


def layer_norm(values, gain, bias):
    values = values.astype(F32)
    centre = jnp.mean(values, -1, keepdims=True)
    centred = values - centre
    spread = jnp.mean(centred * centred, -1, keepdims=True)
    return (centred * lax.rsqrt(spread + EPSILON) * gain + bias).astype(BF16)


def dot(a, b):
    return jnp.dot(a, b, preferred_element_type=F32)


def balanced_dot(a, b):
    wide = b.shape[1] // 512 * 512
    half = a.shape[0] // 2
    rest = b[:, wide:]
    tail = jnp.concatenate([dot(a[:half], rest), dot(a[half:], rest)], 0)
    return jnp.concatenate([dot(a, b[:, :wide]), tail], 1)


def split_dot(a, b):
    high = a.astype(BF16)
    rest = a - high.astype(F32)
    mid = rest.astype(BF16)
    low = (rest - mid.astype(F32)).astype(BF16)
    rows = a.shape[0]
    thirds = dot(jnp.concatenate([high, mid, low], 0), b)
    return thirds[:rows] + thirds[rows : 2 * rows] + thirds[2 * rows :]


def kernel(
    n,
    plan,
    hidden_hbm,
    stale_attn_hbm,
    stale_conv_hbm,
    ln_gain_hbm,
    ln_bias_hbm,
    w_qkv_hbm,
    w_out_hbm,
    gn_gain_hbm,
    gn_bias_hbm,
    conv_w_hbm,
    conv_bias_hbm,
    time_shift_hbm,
    out,
    hidden,
    stale_attn,
    ln_gain,
    ln_bias,
    gn_gain,
    gn_bias,
    conv_bias,
    time_shift,
    w_qkv,
    w_out,
    conv_w,
    blocks,
    keys,
    values,
    q_diag,
    soft,
    soft_far,
    accum,
    same_group,
    to_group,
    from_group,
    conv_acc,
    stats,
    load_sem,
    vector_sem,
    send_sem,
    recv_sem,
    soft_sem,
    stat_sem,
):
    samples, _, cols, channels = out.shape
    tokens = samples * cols
    pairs = channels // (2 * HEAD_DIM)
    group_size = channels // GROUPS
    length = n // 2
    own_edge, cross, handed, q_own, q_far, o_own, o_far = special_parts(length)
    fresh_part = 4 * n
    me = lax.axis_index("patch")
    z = me // 2
    y = me % 2
    above_exists = z > 0
    below_exists = z < length - 1
    neighbours = ((above_exists, me - 2), (below_exists, me + 2), (True, z * 2 + 1 - y))

    barrier = pltpu.get_barrier_semaphore()
    for there, device in neighbours:
        def announce(device=device):
            pl.semaphore_signal(barrier, inc=1, device_id={"patch": device}, device_id_type=MESH)
        if there is True:
            announce()
        else:
            pl.when(there)(announce)

    load_stale = pltpu.make_async_copy(stale_attn_hbm, stale_attn, load_sem.at[0])
    load_hidden = pltpu.make_async_copy(hidden_hbm, hidden, load_sem.at[1])
    load_qkv = pltpu.make_async_copy(w_qkv_hbm, w_qkv, load_sem.at[2])
    load_edge = pltpu.make_async_copy(stale_conv_hbm, blocks.at[pl.ds(own_edge, 4)], load_sem.at[3])
    load_out = pltpu.make_async_copy(w_out_hbm, w_out, load_sem.at[4])
    load_conv = [
        pltpu.make_async_copy(
            conv_w_hbm.at[row, tap],
            conv_w.at[row, :, pl.ds(tap * channels, channels)],
            load_sem.at[5],
        )
        for row in range(3)
        for tap in range(3)
    ]
    load_shift = pltpu.make_async_copy(time_shift_hbm, time_shift, load_sem.at[6])
    vectors = [
        pltpu.make_async_copy(source, target, vector_sem.at[i])
        for i, (source, target) in enumerate(
            (
                (ln_gain_hbm, ln_gain),
                (ln_bias_hbm, ln_bias),
                (gn_gain_hbm, gn_gain),
                (gn_bias_hbm, gn_bias),
                (conv_bias_hbm, conv_bias),
            )
        )
    ]
    load_stale.start()
    for load in vectors[:2]:
        load.start()
    load_hidden.start()

    def pick(choices):
        if len(set(choices)) == 1:
            return jnp.int32(choices[0])
        value = jnp.int32(choices[0])
        for k in range(1, n):
            value = jnp.where(me == k, jnp.int32(choices[k]), value)
        return value

    def table(name):
        rows = plan[name]
        bits = max(v for row in rows for v in row).bit_length()
        per = 31 // bits
        words = [
            pick([sum(v << (bits * k) for k, v in enumerate(row[at : at + per])) for row in rows])
            for at in range(0, len(rows[0]), per)
        ]

        scale = 2**16 // per + 1
        assert all(i * scale >> 16 == i // per for i in range(len(rows[0])))

        def look(i):
            at = lax.shift_right_logical(i * scale, 16)
            level, bit = words, 1
            while len(level) > 1:
                odd = (at & bit) != 0
                pairs_of = [level[k : k + 2] for k in range(0, len(level), 2)]
                level = [jnp.where(odd, p[1], p[0]) if len(p) == 2 else p[0] for p in pairs_of]
                bit *= 2
            return lax.shift_right_logical(level[0], (i - at * per) * bits) & (2**bits - 1)

        return look

    ops, bounds, steps = table("ops"), table("bounds"), table("steps")
    n_steps = pick(plan["n_steps"])
    in_loop = pick(plan["in_loop"])
    to_merge = pick(plan["to_merge"])
    crossed = pick(plan["crossed"])
    n_ops = pick(plan["n_ops"])
    soft[...] = jnp.zeros_like(soft)
    for slot in range(samples + 1):
        soft[slot, 0] = jnp.full(soft.shape[2:], -jnp.inf, F32)
    accum[...] = jnp.zeros_like(accum)
    q_diag[...] = jnp.zeros_like(q_diag)

    @pl.when(jnp.where(y == 0, z == 0, z == length - 1))
    def _():
        blocks[handed : handed + 4] = jnp.zeros_like(blocks[handed : handed + 4])

    mine = me * 4
    per_sample = 2
    for load in vectors[:2]:
        load.wait()
    load_stale.wait()
    load_qkv.start()
    load_edge.start()
    for load in vectors[2:]:
        load.start()
    load_shift.start()
    load_out.start()
    for load in load_conv:
        load.start()

    def landing_of(part):
        late = jnp.where(part < q_far, part - 8, jnp.where(part < o_far, part - 12, part - 18))
        return jnp.where(part < 4 * n, part, late)

    def pump(i, carry):
        op = ops(i)
        part = lax.shift_right_logical(op, 4)
        stale = part < 4 * n
        landed = landing_of(part)

        @pl.when((op & 8) != 0)
        def _():
            pltpu.make_async_remote_copy(
                src_ref=blocks.at[part],
                dst_ref=blocks.at[part],
                send_sem=send_sem.at[0],
                recv_sem=recv_sem.at[landed],
                device_id={"patch": z * 2 + 1 - y},
                device_id_type=MESH,
            ).wait_recv()

        there = jnp.where(stale, part, part + 4)
        landing = landing_of(there)
        for k, (_, device) in enumerate(neighbours):

            @pl.when((op & 2**k) != 0)
            def _(k=k, device=device):
                pltpu.make_async_remote_copy(
                    src_ref=blocks.at[part],
                    dst_ref=blocks.at[there],
                    send_sem=send_sem.at[k],
                    recv_sem=recv_sem.at[landing],
                    device_id={"patch": device},
                    device_id_type=MESH,
                ).start()

        return carry

    def pumps(first, last):
        lax.fori_loop(first, last, pump, 0)

    def norm_stale(s):
        part = layer_norm(stale_attn[2 * s : 2 * s + 2], ln_gain[...], ln_bias[...])
        blocks[pl.ds(mine + 2 * s, 2)] = part

    norm_stale(0)
    pl.semaphore_wait(barrier, 1 + above_exists.astype(jnp.int32) + below_exists.astype(jnp.int32))
    pumps(0, 2)
    for s in range(1, samples):
        norm_stale(s)

    load_hidden.wait()
    fresh = layer_norm(hidden[...], ln_gain[...], ln_bias[...])
    blocks[fresh_part : fresh_part + 4] = fresh.reshape(4, tokens // 4, channels)
    load_qkv.wait()
    queries = dot(fresh, w_qkv[:, :channels]).astype(BF16).astype(F32) * HEAD_DIM ** (-0.5)
    if MOVED:
        blocks[q_own : q_own + 2] = queries[:cols].astype(BF16).reshape(2, cols // 2, channels)

    def spread_queries(slot, q_t):
        for pair in range(pairs):
            for half in range(2):
                row = (2 * pair + half) * HEAD_DIM
                q_diag[
                    slot, pair, half * HEAD_DIM : (half + 1) * HEAD_DIM, half * cols : (half + 1) * cols
                ] = q_t[row : row + HEAD_DIM]

    q_t = queries.T.astype(BF16)
    for s in range(samples):
        spread_queries(s, q_t[:, s * cols : (s + 1) * cols])
    load_edge.wait()
    pumps(2, bounds(0))
    channel_row = lax.broadcasted_iota(jnp.int32, (channels, channels), 0) // group_size
    channel_col = lax.broadcasted_iota(jnp.int32, (channels, channels), 1) // group_size
    same_group[...] = jnp.where(channel_row == channel_col, 1.0, 0.0).astype(BF16)
    narrow = to_group.shape[1]
    channel = lax.broadcasted_iota(jnp.int32, (channels, narrow), 0) // group_size
    group = lax.broadcasted_iota(jnp.int32, (channels, narrow), 1)
    to_group[...] = jnp.where(channel == group, 1.0, 0.0).astype(BF16)
    channel = lax.broadcasted_iota(jnp.int32, (narrow, channels), 1) // group_size
    group = lax.broadcasted_iota(jnp.int32, (narrow, channels), 0)
    from_group[...] = jnp.where(channel == group, 1.0, 0.0).astype(BF16)

    def attend(slot):
        lanes = [slice(pair * 2 * HEAD_DIM, (pair + 1) * 2 * HEAD_DIM) for pair in range(pairs)]
        old_max, old_sum = soft[slot, 0], soft[slot, 1]
        scores = [dot(keys[:, lanes[pair]], q_diag[slot, pair]) for pair in range(pairs)]
        new_max = [
            jnp.maximum(old_max[pair : pair + 1], jnp.max(scores[pair], 0, keepdims=True))
            for pair in range(pairs)
        ]
        weights = [jnp.exp(scores[pair] - new_max[pair]) for pair in range(pairs)]
        both = [lax.dot_general(
                values[:, lanes[pair]],
                weights[pair].astype(BF16),
                (((0,), (0,)), ((), ())),
                preferred_element_type=F32,
            )
            for pair in range(pairs)]
        rescale = [jnp.exp(old_max[pair : pair + 1] - new_max[pair]) for pair in range(pairs)]
        soft[slot, 0] = jnp.concatenate(new_max, 0)
        soft[slot, 1] = jnp.concatenate(
            [
                jnp.sum(weights[pair], 0, keepdims=True) + old_sum[pair : pair + 1] * rescale[pair]
                for pair in range(pairs)
            ],
            0,
        )
        for pair in range(pairs):
            for half in range(2):
                row = (2 * pair + half) * HEAD_DIM
                own = slice(half * cols, (half + 1) * cols)
                accum[slot, row : row + HEAD_DIM] = (
                    both[pair][half * HEAD_DIM : (half + 1) * HEAD_DIM, own]
                    + accum[slot, row : row + HEAD_DIM] * rescale[pair][:, own]
                )

    def normalised(slot):
        for head in range(2 * pairs):
            row = head * HEAD_DIM
            total = soft[slot, 1, head // 2 : head // 2 + 1, (head % 2) * cols : (head % 2 + 1) * cols]
            accum[slot, row : row + HEAD_DIM] = accum[slot, row : row + HEAD_DIM] * (1.0 / total)
        return accum[slot].T

    def soft_copy(device):
        return pltpu.make_async_remote_copy(
            src_ref=soft.at[samples],
            dst_ref=soft_far,
            send_sem=soft_sem.at[0],
            recv_sem=soft_sem.at[1],
            device_id={"patch": device},
            device_id_type=MESH,
        )

    at_end = (z == 0) | (z == length - 1)
    helps = (z == 1) | (z == length - 2)
    outward = jnp.where(z == 1, me - 2, me + 2)

    def step(i, carry):
        code = steps(i)
        s = code & 1
        sz = lax.shift_right_logical(code, 1) & 255
        first_slot = jnp.where(sz == z, n, 2 * sz + y)
        second_slot = 2 * sz + 1 - y
        low = bounds(i)
        span = bounds(i + 1) - low
        marks = [low, low + lax.shift_right_logical(span, 1), low + span]
        rows = jnp.concatenate(
            [
                blocks[pl.ds(slot * 4 + 2 * s, 2)].reshape(cols, channels)
                for slot in (first_slot, second_slot)
            ],
            0,
        )
        both_kv = balanced_dot(rows, w_qkv[:, channels:]).astype(BF16)
        keys[...] = both_kv[:, :channels]
        values[...] = both_kv[:, channels:]
        pumps(marks[0], marks[1])
        attend(s)
        pumps(marks[1], marks[2])
        if MOVED:
            flag = lax.shift_right_logical(code, 9)

            @pl.when((flag & 1) != 0)
            def _():
                @pl.when((flag & 2) != 0)
                def _():
                    far = blocks[q_far : q_far + 2].reshape(cols, channels)
                    spread_queries(samples, far.astype(F32).T.astype(BF16))

                attend(samples)

            @pl.when((flag & 4) != 0)
            def _():
                part = normalised(samples).astype(BF16)
                blocks[o_own : o_own + 2] = part.reshape(2, cols // 2, channels)
                soft_copy(outward).start()
                for k in range(2):
                    pltpu.make_async_remote_copy(
                        src_ref=blocks.at[o_own + k],
                        dst_ref=blocks.at[o_far + k],
                        send_sem=soft_sem.at[2 + k],
                        recv_sem=recv_sem.at[4 * n + 10 + k],
                        device_id={"patch": outward},
                        device_id_type=MESH,
                    ).start()

        return carry

    lax.fori_loop(0, n_steps, step, 0)
    if MOVED:
        pumps(in_loop, to_merge)

        @pl.when(at_end)
        def _():
            soft_copy(z * 2 + 1 - y).wait_recv()
            far = blocks[o_far : o_far + 2].reshape(cols, channels).astype(F32).T
            for head in range(2 * pairs):
                row = head * HEAD_DIM
                at = (slice(head // 2, head // 2 + 1), slice((head % 2) * cols, (head % 2 + 1) * cols))
                near_max, far_max = soft[(0, 0, *at)], soft_far[(0, *at)]
                top = jnp.maximum(near_max, far_max)
                near_scale = jnp.exp(near_max - top)
                far_sum = soft_far[(1, *at)] * jnp.exp(far_max - top)
                accum[0, row : row + HEAD_DIM] = (
                    accum[0, row : row + HEAD_DIM] * near_scale + far[row : row + HEAD_DIM] * far_sum
                )
                soft[(0, 1, *at)] = soft[(0, 1, *at)] * near_scale + far_sum

    attended = jnp.concatenate([normalised(s) for s in range(samples)], 0).astype(BF16)
    load_out.wait()
    residual = hidden[...].astype(F32) + balanced_dot(attended, w_out[...])
    residual = residual.astype(BF16).astype(F32).reshape(samples, cols, channels)

    sum_rows = jnp.concatenate([jnp.sum(residual[s], 0, keepdims=True) for s in range(samples)], 0)
    cells = cols * group_size
    local_mean = split_dot(sum_rows, same_group[...]) / cells
    centred = residual - local_mean[:, None, :]
    square_rows = jnp.concatenate(
        [jnp.sum(centred[s] * centred[s], 0, keepdims=True) for s in range(samples)], 0
    )
    stats[me] = split_dot(jnp.concatenate([sum_rows / cells, square_rows], 0), to_group[...])

    def stat_copy(distance):
        return pltpu.make_async_remote_copy(
            src_ref=stats.at[me],
            dst_ref=stats.at[me],
            send_sem=stat_sem.at[0],
            recv_sem=stat_sem.at[1],
            device_id={"patch": lax.rem(me + distance, n)},
            device_id_type=MESH,
        )

    for distance in range(1, n):
        stat_copy(distance).start()

    pumps(to_merge, crossed)
    pltpu.make_async_copy(conv_w, conv_w, load_sem.at[5]).wait()
    cross_row = jnp.where(y == 0, 2, 0)
    conv_acc[...] = dot(blocks[cross : cross + 4].reshape(tokens, channels), conv_w[cross_row])
    pumps(crossed, n_ops)
    conv_acc[...] += dot(blocks[handed : handed + 4].reshape(tokens, channels), conv_w[2 - cross_row])
    for load in vectors[2:]:
        load.wait()
    load_shift.wait()

    others = stats.at[pl.ds(0, n - 1)]
    pltpu.make_async_remote_copy(
        src_ref=others,
        dst_ref=others,
        send_sem=stat_sem.at[0],
        recv_sem=stat_sem.at[1],
        device_id={"patch": z * 2 + 1 - y},
        device_id_type=MESH,
    ).wait_recv()
    every = stats[...]
    group_mean = jnp.mean(every[:, :samples], 0)
    shift = every[:, :samples] - group_mean[None]
    group_var = (jnp.sum(every[:, samples:], 0) + cells * jnp.sum(shift * shift, 0)) / (cells * n)
    wide = split_dot(jnp.concatenate([group_mean, lax.rsqrt(group_var + EPSILON)], 0), from_group[...])
    scale = wide[samples:] * gn_gain[...]
    pre = (residual - wide[:samples, None, :]) * scale[:, None, :] + gn_bias[...]
    activated = (pre / (1.0 + jnp.exp(-pre))).astype(BF16).reshape(tokens, channels)

    column = lax.broadcasted_iota(jnp.int32, (tokens, 1), 0) % cols
    taps = conv_acc[...] + dot(activated, conv_w[1])
    left, total, right = (taps[:, tap * channels : (tap + 1) * channels] for tap in range(3))
    total = total + jnp.where(column == 0, 0.0, pltpu.roll(left, 1, 0))
    total = total + jnp.where(column == cols - 1, 0.0, pltpu.roll(right, tokens - 1, 0))
    total = total.reshape(samples, cols, channels) + conv_bias[...]
    for sample in range(samples):
        out[sample, 0] = (
            total[sample] + time_shift[sample : sample + 1] + residual[sample]
        ).astype(BF16)

    def sent(source, semaphore):
        pltpu.make_async_remote_copy(
            src_ref=source,
            dst_ref=source,
            send_sem=semaphore,
            recv_sem=stat_sem.at[1],
            device_id={"patch": z * 2 + 1 - y},
            device_id_type=MESH,
        ).wait_send()

    sent(others, stat_sem.at[0])
    for k in range(3):
        for count in sorted(set(plan["sent"][k]) - {0}):
            those = [d for d in range(n) if plan["sent"][k][d] == count]
            match = functools.reduce(jnp.logical_or, [me == d for d in those])
            pl.when(match)(lambda: sent(blocks.at[pl.ds(0, count)], send_sem.at[k]))
    if MOVED:

        @pl.when(helps)
        def _():
            sent(soft.at[samples], soft_sem.at[0])
            for k in range(2):
                sent(blocks.at[o_own + k], soft_sem.at[2 + k])


def shards(n, *arrays):
    (hidden, stale_attn, stale_conv, ln_gain, ln_bias, w_qkv, w_out) = arrays[:7]
    (gn_gain, gn_bias, conv_w, conv_bias, time_shift) = arrays[7:]
    samples, rows_dev, cols, channels = hidden.shape
    assert rows_dev == 1 and samples == 2 and n % 2 == 0 and n >= 8, "unsupported split"
    tokens = samples * cols
    pairs = channels // (2 * HEAD_DIM)
    hbm = pl.BlockSpec(memory_space=pl.ANY)
    vmem = pl.BlockSpec(memory_space=pltpu.VMEM)
    dma = pltpu.SemaphoreType.DMA
    plan = device_plan(n // 2)
    parts = 4 * (n + 8)
    slots = samples + 1 if MOVED else samples
    return pl.pallas_call(
        functools.partial(kernel, n, plan),
        out_shape=pltpu.VMEM(hidden.shape, BF16),
        in_specs=[hbm] * 12,
        out_specs=vmem,
        scratch_shapes=[
            pltpu.VMEM((tokens, channels), BF16),
            pltpu.VMEM((4, tokens // 4, channels), BF16),
        ]
        + [pltpu.VMEM((channels,), F32)] * 5
        + [
            pltpu.VMEM(time_shift.shape, F32),
            pltpu.VMEM(w_qkv.shape, BF16),
            pltpu.VMEM(w_out.shape, BF16),
            pltpu.VMEM((3, channels, 3 * channels), BF16),
            pltpu.VMEM((parts, tokens // 4, channels), BF16),
            pltpu.VMEM((2 * cols, channels), BF16),
            pltpu.VMEM((2 * cols, channels), BF16),
            pltpu.VMEM((samples + 1, pairs, 2 * HEAD_DIM, 2 * cols), BF16),
            pltpu.VMEM((samples + 1, 2, pairs, 2 * cols), F32),
            pltpu.VMEM((2, pairs, 2 * cols), F32),
            pltpu.VMEM((samples + 1, channels, cols), F32),
            pltpu.VMEM((channels, channels), BF16),
            pltpu.VMEM((channels, LANES), BF16),
            pltpu.VMEM((LANES, channels), BF16),
            pltpu.VMEM((tokens, 3 * channels), F32),
            pltpu.VMEM((n, 2 * samples, LANES), F32),
            dma((7,)),
            dma((5,)),
            dma((3,)),
            dma((4 * n + 12,)),
            dma((4,)),
            dma((2,)),
        ],
        compiler_params=pltpu.CompilerParams(
            collective_id=0, has_side_effects=True, vmem_limit_bytes=56 * 2**20
        ),
        name="section",
    )(
        hidden.reshape(tokens, channels),
        stale_attn.reshape(4, tokens // 4, channels),
        stale_conv.reshape(4, tokens // 4, channels),
        ln_gain,
        ln_bias,
        w_qkv,
        w_out,
        gn_gain,
        gn_bias,
        conv_w,
        conv_bias,
        time_shift,
    )


def solution(mesh):
    wide = P("img", "patch", None, None)
    in_specs = (wide, wide, wide) + (P(),) * 8 + (P("img", None),)
    body = functools.partial(shards, mesh.shape["patch"])
    return jax.shard_map(body, mesh=mesh, in_specs=in_specs, out_specs=wide, check_vma=False)
```

```python
import functools
import heapq
import itertools

import jax
import jax.numpy as jnp
from jax import lax
from jax.experimental import pallas as pl
from jax.experimental.pallas import tpu as pltpu
from jax.sharding import PartitionSpec as P

GROUPS = 32
HEAD_DIM = 64
LANES = 128
EPSILON = 1e-05
MESH = pl.DeviceIdType.MESH
F32 = jnp.float32
BF16 = jnp.bfloat16

DOWN, UP, ACROSS = 0, 1, 2
MOVED = True
TUNED = {
    4: [
        (
            [6, 22, 54, 786, 580, 38, 770, 188, 152, 122, 106, 90, 200, 172, 140, 74, 300, 216, 698, 682, 428, 316, 444, 628, 360, 248, 232, 612, 376, 596, 504, 968, 488, 666, 984, 650],
            33,
            35,
            [(1, 0, 0), (0, 0, 0), (0, 1, 0), (1, 1, 0), (1, 2, 0), (1, 3, 0)],
            [11, 16, 18, 27, 29, 33],
        ),
        (
            [135, 151, 183, 268, 10, 26, 201, 167, 58, 284, 297, 328, 412, 217, 396, 42, 596, 580, 429, 840, 250, 234, 856, 313, 344, 120, 456, 612, 445, 472, 104, 504, 682, 72, 488, 760, 376, 744, 628, 88, 650, 666, 360, 698, 728, 712],
            43,
            43,
            [(0, 1, 0), (1, 1, 0), (0, 2, 3), (0, 3, 5), (1, 0, 0), (1, 3, 0), (0, 0, 0), (1, 2, 0)],
            [14, 22, 25, 30, 31, 35, 40, 43],
        ),
        (
            [263, 279, 295, 140, 409, 328, 156, 393, 186, 425, 311, 441, 377, 346, 12, 28, 170, 361, 856, 612, 840, 62, 216, 200, 456, 88, 46, 580, 72, 666, 472, 596, 488, 232, 628, 504, 248, 650, 104, 682, 120, 698, 728, 712, 744, 760],
            41,
            41,
            [(0, 2, 0), (1, 2, 0), (0, 1, 3), (0, 0, 5), (0, 3, 0), (1, 3, 0), (1, 1, 0), (1, 0, 0)],
            [14, 18, 24, 29, 31, 36, 37, 41],
        ),
        (
            [389, 405, 421, 437, 280, 628, 612, 769, 785, 457, 300, 316, 264, 473, 188, 360, 172, 489, 505, 60, 648, 376, 328, 44, 596, 104, 344, 728, 232, 580, 248, 120, 968, 984, 680, 744, 696, 664, 712, 760],
            32,
            34,
            [(0, 3, 0), (1, 3, 0), (1, 2, 0), (0, 2, 0), (1, 1, 0), (1, 0, 0)],
            [14, 19, 22, 27, 31, 32],
        ),
    ]
}


def special_parts(length):
    return tuple(8 * length + 4 * k for k in range(1, 8))


def mirrored_part(length, y, part):
    return part if y == 0 or part >= 8 * length else 4 * (2 * length - 1 - part // 4) + part % 4


def transfers(length):
    own_edge, cross, handed, q_own, q_far, o_own, o_far = special_parts(length)
    ends = (0, length - 1)

    def turned(zd, sz, half):
        return abs(sz - zd) == 1 and (half == 1 or (zd not in ends and sz in ends))

    result = {}
    for z, y in itertools.product(range(length), range(2)):
        sends = {}
        sides = [(k, zd) for k, zd in ((DOWN, z - 1), (UP, z + 1)) if 0 <= zd < length]
        for sz, sy, sp in itertools.product(range(length), range(2), range(4)):
            part = (2 * sz + sy) * 4 + sp
            sends[part] = [
                (k, part)
                for k, zd in sides
                if needs(length, zd, sz, sp // 2)
                and ((sz <= z if k == UP else sz >= z) if sy == y else sz == z and turned(zd, sz, sp % 2))
            ]
            if sy == y and needs(length, z, sz, sp // 2) and not turned(z, sz, sp % 2):
                sends[part].append((ACROSS, part))
        on = UP if y == 0 else DOWN
        for k in range(4):
            sends[own_edge + k] = [(ACROSS, cross + k)]
            sends[cross + k] = [(on, handed + k)] if on in dict(sides) else []
        for k in range(2):
            sends[q_own + k] = [(UP if z == 0 else DOWN, q_far + k)] if z in ends else []
            sends[o_own + k] = [(DOWN if z == 1 else UP, o_far + k)] if z in (1, length - 2) else []
        result[z, y] = sends
    return result


def needs(length, z, sz, sample):
    return not (sample == 0 and z in (0, length - 1) and abs(sz - z) > 1)


def programs_by_time(length):
    own_edge, cross, handed, q_own, q_far, o_own, o_far = special_parts(length)
    ends = (0, length - 1)
    sends = transfers(length)
    queues, busy, events, count = {}, {}, [], itertools.count()
    landed = {d: {} for d in sends}
    left, answered = {}, set()
    rank = {own_edge: 5, cross: 4, handed: 4, q_own: 0, q_far: 0, o_own: -1, o_far: -1}

    def push(t, kind, *rest):
        heapq.heappush(events, (t, next(count), kind, rest))

    def offer(t, d, part):
        for k, there in sends[d].get(part, []):
            push(t, "queue", d, k, part, there)

    def launch(t, d, k):
        busy[d, k] = bool(queues[d, k])
        if busy[d, k]:
            _, there, part = heapq.heappop(queues[d, k])
            left.setdefault((d, part), t)
            push(t + 1.76, "sent", d, k, there)

    for d in sends:
        for k in range(4):
            offer(0.0, d, (2 * d[0] + d[1]) * 4 + k)
            offer(0.0, d, own_edge + k)
        for k in range(2):
            if d[0] in ends:
                offer(2.0, d, q_own + k)
    while events:
        t, _, kind, (d, *rest) = heapq.heappop(events)
        z, y = d
        if kind == "queue":
            k, part, there = rest
            u = z if y == 0 else length - 1 - z
            c = mirrored_part(length, y, part)
            if c < 8 * length:
                order = c % 4 // 2 - abs(c // 8 - u) * (0.5 if k == ACROSS else 1.0)
            else:
                order = rank[c // 4 * 4]
            heapq.heappush(queues.setdefault((d, k), []), ((order, c), there, part))
            if not busy.get((d, k)):
                busy[d, k] = True
                push(t, "launch", d, k)
        elif kind == "launch":
            launch(t, d, rest[0])
        elif kind == "sent":
            k, there = rest
            push(t + 1.75, "landed", ((z - 1, y), (z + 1, y), (z, 1 - y))[k], there)
            launch(t, d, k)
        else:
            landed[d][rest[0]] = t
            offer(t + 0.3, d, rest[0])
            if z in (1, length - 2) and d not in answered:
                far = [
                    (2 * sz + sy) * 4 + sp
                    for sz, sy, sp in itertools.product(range(length), range(2), range(2))
                    if not needs(length, 0 if z == 1 else length - 1, sz, 0) and sz != z
                ]
                if all(p in landed[d] for p in (q_far, q_far + 1, *far)):
                    answered.add(d)
                    for k in range(2):
                        offer(t + 2.5, d, o_own + k)
    programs = []
    for z in range(length):
        d = (z, 0)
        timed = [(t, 1, p) for p, t in landed[d].items()]
        timed += [(-2.0, 0, 8 * z + k) for k in range(2)]
        if z in ends:
            timed += [(-1.0, 0, q_own + k) for k in range(2)]
        for p in (8 * z + 2, 8 * z + 3, *range(own_edge, own_edge + 4)):
            timed.append((max(0.0, left[d, p] - 1.0), 0, p))
        timed.sort()
        codes = [p * 16 + 8 * waits + sum(2**k for k, _ in sends[d].get(p, [])) for _, waits, p in timed]
        in_loop = 1 + max(i for i, (_, _, p) in enumerate(timed) if p < 8 * length)
        results = [i + 1 for i, (_, _, p) in enumerate(timed) if p >= o_far]
        complete, queries = {}, 0
        for i, (_, _, p) in enumerate(timed):
            if p < 8 * length and needs(length, z, p // 8, p % 4 // 2):
                complete[p % 4 // 2, p // 8] = i + 1
            if q_far <= p < q_far + 2:
                queries = i + 1
        steps, bounds, top, helped = [], [], 0, False
        chosen = sorted(complete, key=lambda k: (complete[k], k))
        for i, (sample, sz) in enumerate(chosen):
            top = max(top, complete[sample, sz])
            flags = 0
            if z in (1, length - 2) and sample == 0:
                if not needs(length, 0 if z == 1 else length - 1, sz, 0):
                    flags, helped, top = 1 if helped else 3, True, max(top, queries)
                    last_far = i
            steps.append([sample, sz, flags])
            bounds.append(top)
        if z in (1, length - 2):
            steps[last_far][2] += 4
        programs.append((codes, in_loop, max([in_loop, *results]), steps, bounds))
    return programs


def device_plan(length):
    n = 2 * length
    cross, handed = special_parts(length)[1:3]
    programs = TUNED.get(length) or programs_by_time(length)
    plan = {name: [] for name in ("ops", "bounds", "steps", "n_steps", "in_loop", "to_merge", "crossed", "half_handed", "n_ops")}
    plan["sent"] = [[0] * n for _ in range(3)]
    for d in range(n):
        z, y = divmod(d, 2)
        codes, in_loop, to_merge, steps, bounds = programs[z if y == 0 else length - 1 - z]
        ops = []
        for code in codes:
            where = code % 8
            if y == 1:
                where = where // 4 * 4 + where // 2 % 2 + where % 2 * 2
            ops.append(mirrored_part(length, y, code // 16) * 16 + code // 8 % 2 * 8 + where)
            for k in range(3):
                plan["sent"][k][d] += where // 2**k % 2
        plan["ops"].append(ops)
        plan["bounds"].append([*bounds, in_loop])
        plan["steps"].append(
            [s + 2 * (sz if y == 0 else length - 1 - sz) + 512 * flags for s, sz, flags in steps]
        )
        across = [i + 1 for i, code in enumerate(codes) if cross <= code // 16 < cross + 4]
        plan["n_steps"].append(len(steps))
        plan["in_loop"].append(in_loop)
        plan["to_merge"].append(to_merge)
        plan["crossed"].append(max(to_merge, *across))
        above = [i + 1 for i, code in enumerate(codes) if handed <= code // 16 < handed + 2]
        plan["half_handed"].append(max(plan["crossed"][-1], *above, 0))
        plan["n_ops"].append(len(ops))
    for name in ("ops", "bounds", "steps"):
        width = max(len(row) for row in plan[name])
        plan[name] = [row + [0] * (width - len(row)) for row in plan[name]]
    return plan


def layer_norm(values, gain, bias):
    values = values.astype(F32)
    centre = jnp.mean(values, -1, keepdims=True)
    centred = values - centre
    spread = jnp.mean(centred * centred, -1, keepdims=True)
    return (centred * lax.rsqrt(spread + EPSILON) * gain + bias).astype(BF16)


def dot(a, b):
    return jnp.dot(a, b, preferred_element_type=F32)


def balanced_dot(a, b):
    wide = b.shape[1] // 512 * 512
    half = a.shape[0] // 2
    rest = b[:, wide:]
    tail = jnp.concatenate([dot(a[:half], rest), dot(a[half:], rest)], 0)
    return jnp.concatenate([dot(a, b[:, :wide]), tail], 1)


def split_dot(a, b):
    high = a.astype(BF16)
    rest = a - high.astype(F32)
    mid = rest.astype(BF16)
    low = (rest - mid.astype(F32)).astype(BF16)
    rows = a.shape[0]
    thirds = dot(jnp.concatenate([high, mid, low], 0), b)
    return thirds[:rows] + thirds[rows : 2 * rows] + thirds[2 * rows :]


def kernel(
    n,
    plan,
    hidden_hbm,
    stale_attn_hbm,
    stale_conv_hbm,
    ln_gain_hbm,
    ln_bias_hbm,
    w_qkv_hbm,
    w_out_hbm,
    gn_gain_hbm,
    gn_bias_hbm,
    conv_w_hbm,
    conv_bias_hbm,
    time_shift_hbm,
    out,
    hidden,
    stale_attn,
    ln_gain,
    ln_bias,
    gn_gain,
    gn_bias,
    conv_bias,
    time_shift,
    w_qkv,
    w_out,
    conv_w,
    blocks,
    keys,
    values,
    q_diag,
    soft,
    soft_far,
    accum,
    same_group,
    to_group,
    from_group,
    conv_acc,
    stats,
    load_sem,
    vector_sem,
    send_sem,
    recv_sem,
    soft_sem,
    stat_sem,
):
    samples, _, cols, channels = out.shape
    tokens = samples * cols
    pairs = channels // (2 * HEAD_DIM)
    group_size = channels // GROUPS
    length = n // 2
    own_edge, cross, handed, q_own, q_far, o_own, o_far = special_parts(length)
    fresh_part = 4 * n
    me = lax.axis_index("patch")
    z = me // 2
    y = me % 2
    above_exists = z > 0
    below_exists = z < length - 1
    neighbours = ((above_exists, me - 2), (below_exists, me + 2), (True, z * 2 + 1 - y))

    barrier = pltpu.get_barrier_semaphore()
    for there, device in neighbours:
        def announce(device=device):
            pl.semaphore_signal(barrier, inc=1, device_id={"patch": device}, device_id_type=MESH)
        if there is True:
            announce()
        else:
            pl.when(there)(announce)

    load_stale = pltpu.make_async_copy(stale_attn_hbm, stale_attn, load_sem.at[0])
    load_hidden = pltpu.make_async_copy(hidden_hbm, hidden, load_sem.at[1])
    load_qkv = pltpu.make_async_copy(w_qkv_hbm, w_qkv, load_sem.at[2])
    load_edge = pltpu.make_async_copy(stale_conv_hbm, blocks.at[pl.ds(own_edge, 4)], load_sem.at[3])
    load_out = pltpu.make_async_copy(w_out_hbm, w_out, load_sem.at[4])
    load_conv = [
        pltpu.make_async_copy(
            conv_w_hbm.at[row, tap],
            conv_w.at[row, :, pl.ds(tap * channels, channels)],
            load_sem.at[5],
        )
        for row in range(3)
        for tap in range(3)
    ]
    load_shift = pltpu.make_async_copy(time_shift_hbm, time_shift, load_sem.at[6])
    vectors = [
        pltpu.make_async_copy(source, target, vector_sem.at[i])
        for i, (source, target) in enumerate(
            (
                (ln_gain_hbm, ln_gain),
                (ln_bias_hbm, ln_bias),
                (gn_gain_hbm, gn_gain),
                (gn_bias_hbm, gn_bias),
                (conv_bias_hbm, conv_bias),
            )
        )
    ]
    load_stale.start()
    for load in vectors[:2]:
        load.start()
    load_hidden.start()

    def pick(choices):
        if len(set(choices)) == 1:
            return jnp.int32(choices[0])
        value = jnp.int32(choices[0])
        for k in range(1, n):
            value = jnp.where(me == k, jnp.int32(choices[k]), value)
        return value

    def table(name):
        rows = plan[name]
        bits = max(v for row in rows for v in row).bit_length()
        per = 31 // bits
        words = [
            pick([sum(v << (bits * k) for k, v in enumerate(row[at : at + per])) for row in rows])
            for at in range(0, len(rows[0]), per)
        ]

        scale = 2**16 // per + 1
        assert all(i * scale >> 16 == i // per for i in range(len(rows[0])))

        def look(i):
            at = lax.shift_right_logical(i * scale, 16)
            level, bit = words, 1
            while len(level) > 1:
                odd = (at & bit) != 0
                pairs_of = [level[k : k + 2] for k in range(0, len(level), 2)]
                level = [jnp.where(odd, p[1], p[0]) if len(p) == 2 else p[0] for p in pairs_of]
                bit *= 2
            return lax.shift_right_logical(level[0], (i - at * per) * bits) & (2**bits - 1)

        return look

    ops, bounds, steps = table("ops"), table("bounds"), table("steps")
    n_steps = pick(plan["n_steps"])
    in_loop = pick(plan["in_loop"])
    to_merge = pick(plan["to_merge"])
    crossed = pick(plan["crossed"])
    half_handed = pick(plan["half_handed"])
    n_ops = pick(plan["n_ops"])
    soft[...] = jnp.zeros_like(soft)
    for slot in range(samples + 1):
        soft[slot, 0] = jnp.full(soft.shape[2:], -jnp.inf, F32)
    accum[...] = jnp.zeros_like(accum)
    q_diag[...] = jnp.zeros_like(q_diag)

    @pl.when(jnp.where(y == 0, z == 0, z == length - 1))
    def _():
        blocks[handed : handed + 4] = jnp.zeros_like(blocks[handed : handed + 4])

    mine = me * 4
    per_sample = 2
    for load in vectors[:2]:
        load.wait()
    load_stale.wait()
    load_qkv.start()
    load_edge.start()
    for load in vectors[2:]:
        load.start()
    load_shift.start()
    load_out.start()
    for load in load_conv:
        load.start()

    def landing_of(part):
        late = jnp.where(part < q_far, part - 8, jnp.where(part < o_far, part - 12, part - 18))
        return jnp.where(part < 4 * n, part, late)

    def pump(i, carry):
        op = ops(i)
        part = lax.shift_right_logical(op, 4)
        stale = part < 4 * n
        landed = landing_of(part)

        @pl.when((op & 8) != 0)
        def _():
            pltpu.make_async_remote_copy(
                src_ref=blocks.at[part],
                dst_ref=blocks.at[part],
                send_sem=send_sem.at[0],
                recv_sem=recv_sem.at[landed],
                device_id={"patch": z * 2 + 1 - y},
                device_id_type=MESH,
            ).wait_recv()

        there = jnp.where(stale, part, part + 4)
        landing = landing_of(there)
        for k, (_, device) in enumerate(neighbours):

            @pl.when((op & 2**k) != 0)
            def _(k=k, device=device):
                pltpu.make_async_remote_copy(
                    src_ref=blocks.at[part],
                    dst_ref=blocks.at[there],
                    send_sem=send_sem.at[k],
                    recv_sem=recv_sem.at[landing],
                    device_id={"patch": device},
                    device_id_type=MESH,
                ).start()

        return carry

    def pumps(first, last):
        lax.fori_loop(first, last, pump, 0)

    def norm_stale(s):
        part = layer_norm(stale_attn[2 * s : 2 * s + 2], ln_gain[...], ln_bias[...])
        blocks[pl.ds(mine + 2 * s, 2)] = part

    norm_stale(0)
    pl.semaphore_wait(barrier, 1 + above_exists.astype(jnp.int32) + below_exists.astype(jnp.int32))
    pumps(0, 2)
    for s in range(1, samples):
        norm_stale(s)

    load_hidden.wait()
    fresh = layer_norm(hidden[...], ln_gain[...], ln_bias[...])
    blocks[fresh_part : fresh_part + 4] = fresh.reshape(4, tokens // 4, channels)
    load_qkv.wait()
    queries = dot(fresh, w_qkv[:, :channels]).astype(BF16).astype(F32) * HEAD_DIM ** (-0.5)
    if MOVED:
        blocks[q_own : q_own + 2] = queries[:cols].astype(BF16).reshape(2, cols // 2, channels)

    def spread_queries(slot, q_t):
        for pair in range(pairs):
            for half in range(2):
                row = (2 * pair + half) * HEAD_DIM
                q_diag[
                    slot, pair, half * HEAD_DIM : (half + 1) * HEAD_DIM, half * cols : (half + 1) * cols
                ] = q_t[row : row + HEAD_DIM]

    q_t = queries.T.astype(BF16)
    for s in range(samples):
        spread_queries(s, q_t[:, s * cols : (s + 1) * cols])
    load_edge.wait()
    pumps(2, bounds(0))
    channel_row = lax.broadcasted_iota(jnp.int32, (channels, channels), 0) // group_size
    channel_col = lax.broadcasted_iota(jnp.int32, (channels, channels), 1) // group_size
    same_group[...] = jnp.where(channel_row == channel_col, 1.0, 0.0).astype(BF16)
    narrow = to_group.shape[1]
    channel = lax.broadcasted_iota(jnp.int32, (channels, narrow), 0) // group_size
    group = lax.broadcasted_iota(jnp.int32, (channels, narrow), 1)
    to_group[...] = jnp.where(channel == group, 1.0, 0.0).astype(BF16)
    channel = lax.broadcasted_iota(jnp.int32, (narrow, channels), 1) // group_size
    group = lax.broadcasted_iota(jnp.int32, (narrow, channels), 0)
    from_group[...] = jnp.where(channel == group, 1.0, 0.0).astype(BF16)

    def attend(slot):
        lanes = [slice(pair * 2 * HEAD_DIM, (pair + 1) * 2 * HEAD_DIM) for pair in range(pairs)]
        old_max, old_sum = soft[slot, 0], soft[slot, 1]
        scores = [dot(keys[:, lanes[pair]], q_diag[slot, pair]) for pair in range(pairs)]
        new_max = [
            jnp.maximum(old_max[pair : pair + 1], jnp.max(scores[pair], 0, keepdims=True))
            for pair in range(pairs)
        ]
        weights = [jnp.exp(scores[pair] - new_max[pair]) for pair in range(pairs)]
        both = [lax.dot_general(
                values[:, lanes[pair]],
                weights[pair].astype(BF16),
                (((0,), (0,)), ((), ())),
                preferred_element_type=F32,
            )
            for pair in range(pairs)]
        rescale = [jnp.exp(old_max[pair : pair + 1] - new_max[pair]) for pair in range(pairs)]
        soft[slot, 0] = jnp.concatenate(new_max, 0)
        soft[slot, 1] = jnp.concatenate(
            [
                jnp.sum(weights[pair], 0, keepdims=True) + old_sum[pair : pair + 1] * rescale[pair]
                for pair in range(pairs)
            ],
            0,
        )
        for pair in range(pairs):
            for half in range(2):
                row = (2 * pair + half) * HEAD_DIM
                own = slice(half * cols, (half + 1) * cols)
                accum[slot, row : row + HEAD_DIM] = (
                    both[pair][half * HEAD_DIM : (half + 1) * HEAD_DIM, own]
                    + accum[slot, row : row + HEAD_DIM] * rescale[pair][:, own]
                )

    def normalised(slot):
        for head in range(2 * pairs):
            row = head * HEAD_DIM
            total = soft[slot, 1, head // 2 : head // 2 + 1, (head % 2) * cols : (head % 2 + 1) * cols]
            accum[slot, row : row + HEAD_DIM] = accum[slot, row : row + HEAD_DIM] * (1.0 / total)
        return accum[slot]

    def soft_copy(device):
        return pltpu.make_async_remote_copy(
            src_ref=soft.at[samples],
            dst_ref=soft_far,
            send_sem=soft_sem.at[0],
            recv_sem=soft_sem.at[1],
            device_id={"patch": device},
            device_id_type=MESH,
        )

    at_end = (z == 0) | (z == length - 1)
    helps = (z == 1) | (z == length - 2)
    outward = jnp.where(z == 1, me - 2, me + 2)

    def step(i, carry):
        code = steps(i)
        s = code & 1
        sz = lax.shift_right_logical(code, 1) & 255
        first_slot = jnp.where(sz == z, n, 2 * sz + y)
        second_slot = 2 * sz + 1 - y
        low = bounds(i)
        span = bounds(i + 1) - low
        marks = [low, low + lax.shift_right_logical(span, 1), low + span]
        rows = jnp.concatenate(
            [
                blocks[pl.ds(slot * 4 + 2 * s, 2)].reshape(cols, channels)
                for slot in (first_slot, second_slot)
            ],
            0,
        )
        both_kv = balanced_dot(rows, w_qkv[:, channels:]).astype(BF16)
        keys[...] = both_kv[:, :channels]
        values[...] = both_kv[:, channels:]
        pumps(marks[0], marks[1])
        attend(s)
        pumps(marks[1], marks[2])
        if MOVED:
            flag = lax.shift_right_logical(code, 9)

            @pl.when((flag & 1) != 0)
            def _():
                @pl.when((flag & 2) != 0)
                def _():
                    far = blocks[q_far : q_far + 2].reshape(cols, channels)
                    spread_queries(samples, far.astype(F32).T.astype(BF16))

                attend(samples)

            @pl.when((flag & 4) != 0)
            def _():
                part = normalised(samples).T.astype(BF16)
                blocks[o_own : o_own + 2] = part.reshape(2, cols // 2, channels)
                soft_copy(outward).start()
                for k in range(2):
                    pltpu.make_async_remote_copy(
                        src_ref=blocks.at[o_own + k],
                        dst_ref=blocks.at[o_far + k],
                        send_sem=soft_sem.at[2 + k],
                        recv_sem=recv_sem.at[4 * n + 10 + k],
                        device_id={"patch": outward},
                        device_id_type=MESH,
                    ).start()

        return carry

    lax.fori_loop(0, n_steps, step, 0)
    if MOVED:
        pumps(in_loop, to_merge)

        @pl.when(at_end)
        def _():
            soft_copy(z * 2 + 1 - y).wait_recv()
            far = blocks[o_far : o_far + 2].reshape(cols, channels).astype(F32).T
            for head in range(2 * pairs):
                row = head * HEAD_DIM
                at = (slice(head // 2, head // 2 + 1), slice((head % 2) * cols, (head % 2 + 1) * cols))
                near_max, far_max = soft[(0, 0, *at)], soft_far[(0, *at)]
                top = jnp.maximum(near_max, far_max)
                near_scale = jnp.exp(near_max - top)
                far_sum = soft_far[(1, *at)] * jnp.exp(far_max - top)
                accum[0, row : row + HEAD_DIM] = (
                    accum[0, row : row + HEAD_DIM] * near_scale + far[row : row + HEAD_DIM] * far_sum
                )
                soft[(0, 1, *at)] = soft[(0, 1, *at)] * near_scale + far_sum

    attended = [normalised(s).astype(BF16) for s in range(samples)]
    load_out.wait()
    residual = hidden[...].astype(F32) + jnp.concatenate(
        [
            lax.dot_general(a, w_out[...], (((0,), (0,)), ((), ())), preferred_element_type=F32)
            for a in attended
        ],
        0,
    )
    residual = residual.astype(BF16).astype(F32).reshape(samples, cols, channels)

    sum_rows = jnp.concatenate([jnp.sum(residual[s], 0, keepdims=True) for s in range(samples)], 0)
    cells = cols * group_size
    local_mean = split_dot(sum_rows, same_group[...]) / cells
    centred = residual - local_mean[:, None, :]
    square_rows = jnp.concatenate(
        [jnp.sum(centred[s] * centred[s], 0, keepdims=True) for s in range(samples)], 0
    )
    stats[me] = split_dot(jnp.concatenate([sum_rows / cells, square_rows], 0), to_group[...])

    def stat_copy(distance):
        return pltpu.make_async_remote_copy(
            src_ref=stats.at[me],
            dst_ref=stats.at[me],
            send_sem=stat_sem.at[0],
            recv_sem=stat_sem.at[1],
            device_id={"patch": lax.rem(me + distance, n)},
            device_id_type=MESH,
        )

    for distance in range(1, n):
        stat_copy(distance).start()

    pumps(to_merge, crossed)
    pltpu.make_async_copy(conv_w, conv_w, load_sem.at[5]).wait()
    cross_row = jnp.where(y == 0, 2, 0)
    conv_acc[...] = dot(blocks[cross : cross + 4].reshape(tokens, channels), conv_w[cross_row])
    half = tokens // 2
    for first, last, at in ((crossed, half_handed, 0), (half_handed, n_ops, half)):
        pumps(first, last)
        part = blocks[handed + 2 * (at > 0) : handed + 2 * (at > 0) + 2].reshape(half, channels)
        conv_acc[at : at + half] += dot(part, conv_w[2 - cross_row])
    for load in vectors[2:]:
        load.wait()
    load_shift.wait()

    others = stats.at[pl.ds(0, n - 1)]
    pltpu.make_async_remote_copy(
        src_ref=others,
        dst_ref=others,
        send_sem=stat_sem.at[0],
        recv_sem=stat_sem.at[1],
        device_id={"patch": z * 2 + 1 - y},
        device_id_type=MESH,
    ).wait_recv()
    every = stats[...]
    group_mean = jnp.mean(every[:, :samples], 0)
    shift = every[:, :samples] - group_mean[None]
    group_var = (jnp.sum(every[:, samples:], 0) + cells * jnp.sum(shift * shift, 0)) / (cells * n)
    wide = split_dot(jnp.concatenate([group_mean, lax.rsqrt(group_var + EPSILON)], 0), from_group[...])
    scale = wide[samples:] * gn_gain[...]
    pre = (residual - wide[:samples, None, :]) * scale[:, None, :] + gn_bias[...]
    activated = (pre / (1.0 + jnp.exp(-pre))).astype(BF16).reshape(tokens, channels)

    column = lax.broadcasted_iota(jnp.int32, (tokens, 1), 0) % cols
    taps = conv_acc[...] + dot(activated, conv_w[1])
    left, total, right = (taps[:, tap * channels : (tap + 1) * channels] for tap in range(3))
    total = total + jnp.where(column == 0, 0.0, pltpu.roll(left, 1, 0))
    total = total + jnp.where(column == cols - 1, 0.0, pltpu.roll(right, tokens - 1, 0))
    total = total.reshape(samples, cols, channels) + conv_bias[...]
    for sample in range(samples):
        out[sample, 0] = (
            total[sample] + time_shift[sample : sample + 1] + residual[sample]
        ).astype(BF16)

    def sent(source, semaphore):
        pltpu.make_async_remote_copy(
            src_ref=source,
            dst_ref=source,
            send_sem=semaphore,
            recv_sem=stat_sem.at[1],
            device_id={"patch": z * 2 + 1 - y},
            device_id_type=MESH,
        ).wait_send()

    sent(others, stat_sem.at[0])
    for k in range(3):
        for count in sorted(set(plan["sent"][k]) - {0}):
            those = [d for d in range(n) if plan["sent"][k][d] == count]
            match = functools.reduce(jnp.logical_or, [me == d for d in those])
            pl.when(match)(lambda: sent(blocks.at[pl.ds(0, count)], send_sem.at[k]))
    if MOVED:

        @pl.when(helps)
        def _():
            sent(soft.at[samples], soft_sem.at[0])
            for k in range(2):
                sent(blocks.at[o_own + k], soft_sem.at[2 + k])


def shards(n, *arrays):
    (hidden, stale_attn, stale_conv, ln_gain, ln_bias, w_qkv, w_out) = arrays[:7]
    (gn_gain, gn_bias, conv_w, conv_bias, time_shift) = arrays[7:]
    samples, rows_dev, cols, channels = hidden.shape
    assert rows_dev == 1 and samples == 2 and n % 2 == 0 and n >= 8, "unsupported split"
    tokens = samples * cols
    pairs = channels // (2 * HEAD_DIM)
    hbm = pl.BlockSpec(memory_space=pl.ANY)
    vmem = pl.BlockSpec(memory_space=pltpu.VMEM)
    dma = pltpu.SemaphoreType.DMA
    plan = device_plan(n // 2)
    parts = 4 * (n + 8)
    slots = samples + 1 if MOVED else samples
    return pl.pallas_call(
        functools.partial(kernel, n, plan),
        out_shape=pltpu.VMEM(hidden.shape, BF16),
        in_specs=[hbm] * 12,
        out_specs=vmem,
        scratch_shapes=[
            pltpu.VMEM((tokens, channels), BF16),
            pltpu.VMEM((4, tokens // 4, channels), BF16),
        ]
        + [pltpu.VMEM((channels,), F32)] * 5
        + [
            pltpu.VMEM(time_shift.shape, F32),
            pltpu.VMEM(w_qkv.shape, BF16),
            pltpu.VMEM(w_out.shape, BF16),
            pltpu.VMEM((3, channels, 3 * channels), BF16),
            pltpu.VMEM((parts, tokens // 4, channels), BF16),
            pltpu.VMEM((2 * cols, channels), BF16),
            pltpu.VMEM((2 * cols, channels), BF16),
            pltpu.VMEM((samples + 1, pairs, 2 * HEAD_DIM, 2 * cols), BF16),
            pltpu.VMEM((samples + 1, 2, pairs, 2 * cols), F32),
            pltpu.VMEM((2, pairs, 2 * cols), F32),
            pltpu.VMEM((samples + 1, channels, cols), F32),
            pltpu.VMEM((channels, channels), BF16),
            pltpu.VMEM((channels, LANES), BF16),
            pltpu.VMEM((LANES, channels), BF16),
            pltpu.VMEM((tokens, 3 * channels), F32),
            pltpu.VMEM((n, 2 * samples, LANES), F32),
            dma((7,)),
            dma((5,)),
            dma((3,)),
            dma((4 * n + 12,)),
            dma((4,)),
            dma((2,)),
        ],
        compiler_params=pltpu.CompilerParams(
            collective_id=0, has_side_effects=True, vmem_limit_bytes=56 * 2**20
        ),
        name="section",
    )(
        hidden.reshape(tokens, channels),
        stale_attn.reshape(4, tokens // 4, channels),
        stale_conv.reshape(4, tokens // 4, channels),
        ln_gain,
        ln_bias,
        w_qkv,
        w_out,
        gn_gain,
        gn_bias,
        conv_w,
        conv_bias,
        time_shift,
    )


def solution(mesh):
    wide = P("img", "patch", None, None)
    in_specs = (wide, wide, wide) + (P(),) * 8 + (P("img", None),)
    body = functools.partial(shards, mesh.shape["patch"])
    return jax.shard_map(body, mesh=mesh, in_specs=in_specs, out_specs=wide, check_vma=False)
```

```python
import functools
import heapq
import itertools

import jax
import jax.numpy as jnp
from jax import lax
from jax.experimental import pallas as pl
from jax.experimental.pallas import tpu as pltpu
from jax.sharding import PartitionSpec as P

GROUPS = 32
HEAD_DIM = 64
LANES = 128
EPSILON = 1e-05
MESH = pl.DeviceIdType.MESH
F32 = jnp.float32
BF16 = jnp.bfloat16

DOWN, UP, ACROSS = 0, 1, 2
MOVED = True
TUNED = {
    4: [
        (
            [6, 22, 54, 786, 580, 38, 770, 188, 152, 122, 106, 90, 200, 172, 140, 74, 300, 216, 698, 682, 428, 316, 444, 628, 360, 248, 232, 612, 376, 596, 504, 968, 488, 666, 984, 650],
            33,
            35,
            [(1, 0, 0), (0, 0, 0), (0, 1, 0), (1, 1, 0), (1, 2, 0), (1, 3, 0)],
            [11, 16, 18, 27, 29, 33],
        ),
        (
            [135, 151, 183, 268, 10, 26, 201, 167, 58, 284, 297, 328, 412, 217, 396, 42, 596, 580, 429, 840, 250, 234, 856, 313, 344, 120, 456, 612, 445, 472, 104, 504, 682, 72, 488, 760, 376, 744, 628, 88, 650, 666, 360, 698, 728, 712],
            43,
            43,
            [(0, 1, 0), (1, 1, 0), (0, 2, 3), (0, 3, 5), (1, 0, 0), (1, 3, 0), (0, 0, 0), (1, 2, 0)],
            [14, 22, 25, 30, 31, 35, 40, 43],
        ),
        (
            [263, 279, 295, 140, 409, 328, 156, 393, 186, 425, 311, 441, 377, 346, 12, 28, 170, 361, 856, 612, 840, 62, 216, 200, 456, 88, 46, 580, 72, 666, 472, 596, 488, 232, 628, 504, 248, 650, 104, 682, 120, 698, 728, 712, 744, 760],
            41,
            41,
            [(0, 2, 0), (1, 2, 0), (0, 1, 3), (0, 0, 5), (0, 3, 0), (1, 3, 0), (1, 1, 0), (1, 0, 0)],
            [14, 18, 24, 29, 31, 36, 37, 41],
        ),
        (
            [389, 405, 421, 437, 280, 628, 612, 769, 785, 457, 300, 316, 264, 473, 188, 360, 172, 489, 505, 60, 648, 376, 328, 44, 596, 104, 344, 728, 232, 580, 248, 120, 968, 984, 680, 744, 696, 664, 712, 760],
            32,
            34,
            [(0, 3, 0), (1, 3, 0), (1, 2, 0), (0, 2, 0), (1, 1, 0), (1, 0, 0)],
            [14, 19, 22, 27, 31, 32],
        ),
    ]
}


def special_parts(length):
    return tuple(8 * length + 4 * k for k in range(1, 8))


def mirrored_part(length, y, part):
    return part if y == 0 or part >= 8 * length else 4 * (2 * length - 1 - part // 4) + part % 4


def transfers(length):
    own_edge, cross, handed, q_own, q_far, o_own, o_far = special_parts(length)
    ends = (0, length - 1)

    def turned(zd, sz, half):
        return abs(sz - zd) == 1 and (half == 1 or (zd not in ends and sz in ends))

    result = {}
    for z, y in itertools.product(range(length), range(2)):
        sends = {}
        sides = [(k, zd) for k, zd in ((DOWN, z - 1), (UP, z + 1)) if 0 <= zd < length]
        for sz, sy, sp in itertools.product(range(length), range(2), range(4)):
            part = (2 * sz + sy) * 4 + sp
            sends[part] = [
                (k, part)
                for k, zd in sides
                if needs(length, zd, sz, sp // 2)
                and ((sz <= z if k == UP else sz >= z) if sy == y else sz == z and turned(zd, sz, sp % 2))
            ]
            if sy == y and needs(length, z, sz, sp // 2) and not turned(z, sz, sp % 2):
                sends[part].append((ACROSS, part))
        on = UP if y == 0 else DOWN
        for k in range(4):
            sends[own_edge + k] = [(ACROSS, cross + k)]
            sends[cross + k] = [(on, handed + k)] if on in dict(sides) else []
        for k in range(2):
            sends[q_own + k] = [(UP if z == 0 else DOWN, q_far + k)] if z in ends else []
            sends[o_own + k] = [(DOWN if z == 1 else UP, o_far + k)] if z in (1, length - 2) else []
        result[z, y] = sends
    return result


def needs(length, z, sz, sample):
    return not (sample == 0 and z in (0, length - 1) and abs(sz - z) > 1)


def programs_by_time(length):
    own_edge, cross, handed, q_own, q_far, o_own, o_far = special_parts(length)
    ends = (0, length - 1)
    sends = transfers(length)
    queues, busy, events, count = {}, {}, [], itertools.count()
    landed = {d: {} for d in sends}
    left, answered = {}, set()
    rank = {own_edge: 5, cross: 4, handed: 4, q_own: 0, q_far: 0, o_own: -1, o_far: -1}

    def push(t, kind, *rest):
        heapq.heappush(events, (t, next(count), kind, rest))

    def offer(t, d, part):
        for k, there in sends[d].get(part, []):
            push(t, "queue", d, k, part, there)

    def launch(t, d, k):
        busy[d, k] = bool(queues[d, k])
        if busy[d, k]:
            _, there, part = heapq.heappop(queues[d, k])
            left.setdefault((d, part), t)
            push(t + 1.76, "sent", d, k, there)

    for d in sends:
        for k in range(4):
            offer(0.0, d, (2 * d[0] + d[1]) * 4 + k)
            offer(0.0, d, own_edge + k)
        for k in range(2):
            if d[0] in ends:
                offer(2.0, d, q_own + k)
    while events:
        t, _, kind, (d, *rest) = heapq.heappop(events)
        z, y = d
        if kind == "queue":
            k, part, there = rest
            u = z if y == 0 else length - 1 - z
            c = mirrored_part(length, y, part)
            if c < 8 * length:
                order = c % 4 // 2 - abs(c // 8 - u) * (0.5 if k == ACROSS else 1.0)
            else:
                order = rank[c // 4 * 4]
            heapq.heappush(queues.setdefault((d, k), []), ((order, c), there, part))
            if not busy.get((d, k)):
                busy[d, k] = True
                push(t, "launch", d, k)
        elif kind == "launch":
            launch(t, d, rest[0])
        elif kind == "sent":
            k, there = rest
            push(t + 1.75, "landed", ((z - 1, y), (z + 1, y), (z, 1 - y))[k], there)
            launch(t, d, k)
        else:
            landed[d][rest[0]] = t
            offer(t + 0.3, d, rest[0])
            if z in (1, length - 2) and d not in answered:
                far = [
                    (2 * sz + sy) * 4 + sp
                    for sz, sy, sp in itertools.product(range(length), range(2), range(2))
                    if not needs(length, 0 if z == 1 else length - 1, sz, 0) and sz != z
                ]
                if all(p in landed[d] for p in (q_far, q_far + 1, *far)):
                    answered.add(d)
                    for k in range(2):
                        offer(t + 2.5, d, o_own + k)
    programs = []
    for z in range(length):
        d = (z, 0)
        timed = [(t, 1, p) for p, t in landed[d].items()]
        timed += [(-2.0, 0, 8 * z + k) for k in range(2)]
        if z in ends:
            timed += [(-1.0, 0, q_own + k) for k in range(2)]
        for p in (8 * z + 2, 8 * z + 3, *range(own_edge, own_edge + 4)):
            timed.append((max(0.0, left[d, p] - 1.0), 0, p))
        timed.sort()
        codes = [p * 16 + 8 * waits + sum(2**k for k, _ in sends[d].get(p, [])) for _, waits, p in timed]
        in_loop = 1 + max(i for i, (_, _, p) in enumerate(timed) if p < 8 * length)
        results = [i + 1 for i, (_, _, p) in enumerate(timed) if p >= o_far]
        complete, queries = {}, 0
        for i, (_, _, p) in enumerate(timed):
            if p < 8 * length and needs(length, z, p // 8, p % 4 // 2):
                complete[p % 4 // 2, p // 8] = i + 1
            if q_far <= p < q_far + 2:
                queries = i + 1
        steps, bounds, top, helped = [], [], 0, False
        chosen = sorted(complete, key=lambda k: (complete[k], k))
        for i, (sample, sz) in enumerate(chosen):
            top = max(top, complete[sample, sz])
            flags = 0
            if z in (1, length - 2) and sample == 0:
                if not needs(length, 0 if z == 1 else length - 1, sz, 0):
                    flags, helped, top = 1 if helped else 3, True, max(top, queries)
                    last_far = i
            steps.append([sample, sz, flags])
            bounds.append(top)
        if z in (1, length - 2):
            steps[last_far][2] += 4
        programs.append((codes, in_loop, max([in_loop, *results]), steps, bounds))
    return programs


def device_plan(length):
    n = 2 * length
    cross, handed = special_parts(length)[1:3]
    programs = TUNED.get(length) or programs_by_time(length)
    plan = {name: [] for name in ("ops", "bounds", "steps", "n_steps", "in_loop", "to_merge", "crossed", "half_handed", "n_ops")}
    plan["sent"] = [[0] * n for _ in range(3)]
    for d in range(n):
        z, y = divmod(d, 2)
        codes, in_loop, to_merge, steps, bounds = programs[z if y == 0 else length - 1 - z]
        ops = []
        for code in codes:
            where = code % 8
            if y == 1:
                where = where // 4 * 4 + where // 2 % 2 + where % 2 * 2
            ops.append(mirrored_part(length, y, code // 16) * 16 + code // 8 % 2 * 8 + where)
            for k in range(3):
                plan["sent"][k][d] += where // 2**k % 2
        plan["ops"].append(ops)
        plan["bounds"].append([*bounds, in_loop])
        plan["steps"].append(
            [s + 2 * (sz if y == 0 else length - 1 - sz) + 512 * flags for s, sz, flags in steps]
        )
        across = [i + 1 for i, code in enumerate(codes) if cross <= code // 16 < cross + 4]
        plan["n_steps"].append(len(steps))
        plan["in_loop"].append(in_loop)
        plan["to_merge"].append(to_merge)
        plan["crossed"].append(max(to_merge, *across))
        above = [i + 1 for i, code in enumerate(codes) if handed <= code // 16 < handed + 2]
        plan["half_handed"].append(max(plan["crossed"][-1], *above, 0))
        plan["n_ops"].append(len(ops))
    for name in ("ops", "bounds", "steps"):
        width = max(len(row) for row in plan[name])
        plan[name] = [row + [0] * (width - len(row)) for row in plan[name]]
    return plan


def layer_norm(values, gain, bias):
    values = values.astype(F32)
    centre = jnp.mean(values, -1, keepdims=True)
    centred = values - centre
    spread = jnp.mean(centred * centred, -1, keepdims=True)
    return (centred * lax.rsqrt(spread + EPSILON) * gain + bias).astype(BF16)


def dot(a, b):
    return jnp.dot(a, b, preferred_element_type=F32)


def balanced_dot(a, b):
    wide = b.shape[1] // 512 * 512
    half = a.shape[0] // 2
    rest = b[:, wide:]
    tail = jnp.concatenate([dot(a[:half], rest), dot(a[half:], rest)], 0)
    return jnp.concatenate([dot(a, b[:, :wide]), tail], 1)


def split_dot(a, b):
    high = a.astype(BF16)
    rest = a - high.astype(F32)
    mid = rest.astype(BF16)
    low = (rest - mid.astype(F32)).astype(BF16)
    rows = a.shape[0]
    thirds = dot(jnp.concatenate([high, mid, low], 0), b)
    return thirds[:rows] + thirds[rows : 2 * rows] + thirds[2 * rows :]


def kernel(
    n,
    plan,
    hidden_hbm,
    stale_attn_hbm,
    stale_conv_hbm,
    ln_gain_hbm,
    ln_bias_hbm,
    w_qkv_hbm,
    w_out_hbm,
    gn_gain_hbm,
    gn_bias_hbm,
    conv_w_hbm,
    conv_bias_hbm,
    time_shift_hbm,
    out,
    hidden,
    stale_attn,
    ln_gain,
    ln_bias,
    gn_gain,
    gn_bias,
    conv_bias,
    time_shift,
    w_qkv,
    w_out,
    conv_w,
    blocks,
    keys,
    values,
    q_diag,
    soft,
    soft_far,
    accum,
    same_group,
    to_group,
    from_group,
    conv_acc,
    stats,
    load_sem,
    vector_sem,
    send_sem,
    recv_sem,
    soft_sem,
    stat_sem,
):
    samples, _, cols, channels = out.shape
    tokens = samples * cols
    pairs = channels // (2 * HEAD_DIM)
    group_size = channels // GROUPS
    length = n // 2
    own_edge, cross, handed, q_own, q_far, o_own, o_far = special_parts(length)
    fresh_part = 4 * n
    me = lax.axis_index("patch")
    z = me // 2
    y = me % 2
    above_exists = z > 0
    below_exists = z < length - 1
    load_stale = pltpu.make_async_copy(stale_attn_hbm, stale_attn, load_sem.at[0])
    load_hidden = pltpu.make_async_copy(hidden_hbm, hidden, load_sem.at[1])
    load_qkv = pltpu.make_async_copy(w_qkv_hbm, w_qkv, load_sem.at[2])
    load_edge = pltpu.make_async_copy(stale_conv_hbm, blocks.at[pl.ds(own_edge, 4)], load_sem.at[3])
    load_out = pltpu.make_async_copy(w_out_hbm, w_out, load_sem.at[4])
    load_conv = [
        pltpu.make_async_copy(
            conv_w_hbm.at[row, tap],
            conv_w.at[row, :, pl.ds(tap * channels, channels)],
            load_sem.at[5],
        )
        for row in range(3)
        for tap in range(3)
    ]
    load_shift = pltpu.make_async_copy(time_shift_hbm, time_shift, load_sem.at[6])
    vectors = [
        pltpu.make_async_copy(source, target, vector_sem.at[i])
        for i, (source, target) in enumerate(
            (
                (ln_gain_hbm, ln_gain),
                (ln_bias_hbm, ln_bias),
                (gn_gain_hbm, gn_gain),
                (gn_bias_hbm, gn_bias),
                (conv_bias_hbm, conv_bias),
            )
        )
    ]
    load_stale.start()
    for load in vectors[:2]:
        load.start()

    neighbours = ((above_exists, me - 2), (below_exists, me + 2), (True, z * 2 + 1 - y))

    barrier = pltpu.get_barrier_semaphore()
    for there, device in neighbours:
        def announce(device=device):
            pl.semaphore_signal(barrier, inc=1, device_id={"patch": device}, device_id_type=MESH)
        if there is True:
            announce()
        else:
            pl.when(there)(announce)

    load_hidden.start()

    def pick(choices):
        if len(set(choices)) == 1:
            return jnp.int32(choices[0])
        value = jnp.int32(choices[0])
        for k in range(1, n):
            value = jnp.where(me == k, jnp.int32(choices[k]), value)
        return value

    def table(name):
        rows = plan[name]
        bits = max(v for row in rows for v in row).bit_length()
        per = 31 // bits
        words = [
            pick([sum(v << (bits * k) for k, v in enumerate(row[at : at + per])) for row in rows])
            for at in range(0, len(rows[0]), per)
        ]

        scale = 2**16 // per + 1
        assert all(i * scale >> 16 == i // per for i in range(len(rows[0])))

        def look(i):
            at = lax.shift_right_logical(i * scale, 16)
            level, bit = words, 1
            while len(level) > 1:
                odd = (at & bit) != 0
                pairs_of = [level[k : k + 2] for k in range(0, len(level), 2)]
                level = [jnp.where(odd, p[1], p[0]) if len(p) == 2 else p[0] for p in pairs_of]
                bit *= 2
            return lax.shift_right_logical(level[0], (i - at * per) * bits) & (2**bits - 1)

        return look

    ops, bounds, steps = table("ops"), table("bounds"), table("steps")
    n_steps = pick(plan["n_steps"])
    in_loop = pick(plan["in_loop"])
    to_merge = pick(plan["to_merge"])
    crossed = pick(plan["crossed"])
    half_handed = pick(plan["half_handed"])
    n_ops = pick(plan["n_ops"])
    soft[...] = jnp.zeros_like(soft)
    for slot in range(samples + 1):
        soft[slot, 0] = jnp.full(soft.shape[2:], -jnp.inf, F32)
    accum[...] = jnp.zeros_like(accum)
    q_diag[...] = jnp.zeros_like(q_diag)

    @pl.when(jnp.where(y == 0, z == 0, z == length - 1))
    def _():
        blocks[handed : handed + 4] = jnp.zeros_like(blocks[handed : handed + 4])

    mine = me * 4
    per_sample = 2
    for load in vectors[:2]:
        load.wait()
    load_stale.wait()
    load_qkv.start()
    load_edge.start()
    for load in vectors[2:]:
        load.start()
    load_shift.start()
    load_out.start()
    for load in load_conv:
        load.start()

    def landing_of(part):
        late = jnp.where(part < q_far, part - 8, jnp.where(part < o_far, part - 12, part - 18))
        return jnp.where(part < 4 * n, part, late)

    def pump(i, carry):
        op = ops(i)
        part = lax.shift_right_logical(op, 4)
        stale = part < 4 * n
        landed = landing_of(part)

        @pl.when((op & 8) != 0)
        def _():
            pltpu.make_async_remote_copy(
                src_ref=blocks.at[part],
                dst_ref=blocks.at[part],
                send_sem=send_sem.at[0],
                recv_sem=recv_sem.at[landed],
                device_id={"patch": z * 2 + 1 - y},
                device_id_type=MESH,
            ).wait_recv()

        there = jnp.where(stale, part, part + 4)
        landing = landing_of(there)
        for k, (_, device) in enumerate(neighbours):

            @pl.when((op & 2**k) != 0)
            def _(k=k, device=device):
                pltpu.make_async_remote_copy(
                    src_ref=blocks.at[part],
                    dst_ref=blocks.at[there],
                    send_sem=send_sem.at[k],
                    recv_sem=recv_sem.at[landing],
                    device_id={"patch": device},
                    device_id_type=MESH,
                ).start()

        return carry

    def pumps(first, last):
        lax.fori_loop(first, last, pump, 0)

    def norm_stale(s):
        part = layer_norm(stale_attn[2 * s : 2 * s + 2], ln_gain[...], ln_bias[...])
        blocks[pl.ds(mine + 2 * s, 2)] = part

    norm_stale(0)
    pl.semaphore_wait(barrier, 1 + above_exists.astype(jnp.int32) + below_exists.astype(jnp.int32))
    pumps(0, 2)
    for s in range(1, samples):
        norm_stale(s)

    load_hidden.wait()
    fresh = layer_norm(hidden[...], ln_gain[...], ln_bias[...])
    blocks[fresh_part : fresh_part + 4] = fresh.reshape(4, tokens // 4, channels)
    load_qkv.wait()
    queries = dot(fresh, w_qkv[:, :channels]).astype(BF16).astype(F32) * HEAD_DIM ** (-0.5)
    if MOVED:
        blocks[q_own : q_own + 2] = queries[:cols].astype(BF16).reshape(2, cols // 2, channels)

    def spread_queries(slot, q_t):
        for pair in range(pairs):
            for half in range(2):
                row = (2 * pair + half) * HEAD_DIM
                q_diag[
                    slot, pair, half * HEAD_DIM : (half + 1) * HEAD_DIM, half * cols : (half + 1) * cols
                ] = q_t[row : row + HEAD_DIM]

    q_t = queries.T.astype(BF16)
    for s in range(samples):
        spread_queries(s, q_t[:, s * cols : (s + 1) * cols])
    load_edge.wait()
    pumps(2, bounds(0))
    channel_row = lax.broadcasted_iota(jnp.int32, (channels, channels), 0) // group_size
    channel_col = lax.broadcasted_iota(jnp.int32, (channels, channels), 1) // group_size
    same_group[...] = jnp.where(channel_row == channel_col, 1.0, 0.0).astype(BF16)
    narrow = to_group.shape[1]
    channel = lax.broadcasted_iota(jnp.int32, (channels, narrow), 0) // group_size
    group = lax.broadcasted_iota(jnp.int32, (channels, narrow), 1)
    to_group[...] = jnp.where(channel == group, 1.0, 0.0).astype(BF16)
    channel = lax.broadcasted_iota(jnp.int32, (narrow, channels), 1) // group_size
    group = lax.broadcasted_iota(jnp.int32, (narrow, channels), 0)
    from_group[...] = jnp.where(channel == group, 1.0, 0.0).astype(BF16)

    def attend(slot):
        lanes = [slice(pair * 2 * HEAD_DIM, (pair + 1) * 2 * HEAD_DIM) for pair in range(pairs)]
        old_max, old_sum = soft[slot, 0], soft[slot, 1]
        scores = [dot(keys[:, lanes[pair]], q_diag[slot, pair]) for pair in range(pairs)]
        new_max = [
            jnp.maximum(old_max[pair : pair + 1], jnp.max(scores[pair], 0, keepdims=True))
            for pair in range(pairs)
        ]
        weights = [jnp.exp(scores[pair] - new_max[pair]) for pair in range(pairs)]
        both = [lax.dot_general(
                values[:, lanes[pair]],
                weights[pair].astype(BF16),
                (((0,), (0,)), ((), ())),
                preferred_element_type=F32,
            )
            for pair in range(pairs)]
        rescale = [jnp.exp(old_max[pair : pair + 1] - new_max[pair]) for pair in range(pairs)]
        soft[slot, 0] = jnp.concatenate(new_max, 0)
        soft[slot, 1] = jnp.concatenate(
            [
                jnp.sum(weights[pair], 0, keepdims=True) + old_sum[pair : pair + 1] * rescale[pair]
                for pair in range(pairs)
            ],
            0,
        )
        for pair in range(pairs):
            for half in range(2):
                row = (2 * pair + half) * HEAD_DIM
                own = slice(half * cols, (half + 1) * cols)
                accum[slot, row : row + HEAD_DIM] = (
                    both[pair][half * HEAD_DIM : (half + 1) * HEAD_DIM, own]
                    + accum[slot, row : row + HEAD_DIM] * rescale[pair][:, own]
                )

    def normalised(slot):
        for head in range(2 * pairs):
            row = head * HEAD_DIM
            total = soft[slot, 1, head // 2 : head // 2 + 1, (head % 2) * cols : (head % 2 + 1) * cols]
            accum[slot, row : row + HEAD_DIM] = accum[slot, row : row + HEAD_DIM] * (1.0 / total)
        return accum[slot]

    def soft_copy(device):
        return pltpu.make_async_remote_copy(
            src_ref=soft.at[samples],
            dst_ref=soft_far,
            send_sem=soft_sem.at[0],
            recv_sem=soft_sem.at[1],
            device_id={"patch": device},
            device_id_type=MESH,
        )

    at_end = (z == 0) | (z == length - 1)
    helps = (z == 1) | (z == length - 2)
    outward = jnp.where(z == 1, me - 2, me + 2)

    def step(i, carry):
        code = steps(i)
        s = code & 1
        sz = lax.shift_right_logical(code, 1) & 255
        first_slot = jnp.where(sz == z, n, 2 * sz + y)
        second_slot = 2 * sz + 1 - y
        low = bounds(i)
        span = bounds(i + 1) - low
        marks = [low, low + lax.shift_right_logical(span, 1), low + span]
        rows = jnp.concatenate(
            [
                blocks[pl.ds(slot * 4 + 2 * s, 2)].reshape(cols, channels)
                for slot in (first_slot, second_slot)
            ],
            0,
        )
        both_kv = balanced_dot(rows, w_qkv[:, channels:]).astype(BF16)
        keys[...] = both_kv[:, :channels]
        values[...] = both_kv[:, channels:]
        pumps(marks[0], marks[1])
        attend(s)
        pumps(marks[1], marks[2])
        if MOVED:
            flag = lax.shift_right_logical(code, 9)

            @pl.when((flag & 1) != 0)
            def _():
                @pl.when((flag & 2) != 0)
                def _():
                    far = blocks[q_far : q_far + 2].reshape(cols, channels)
                    spread_queries(samples, far.astype(F32).T.astype(BF16))

                attend(samples)

            @pl.when((flag & 4) != 0)
            def _():
                part = normalised(samples).T.astype(BF16)
                blocks[o_own : o_own + 2] = part.reshape(2, cols // 2, channels)
                soft_copy(outward).start()
                for k in range(2):
                    pltpu.make_async_remote_copy(
                        src_ref=blocks.at[o_own + k],
                        dst_ref=blocks.at[o_far + k],
                        send_sem=soft_sem.at[2 + k],
                        recv_sem=recv_sem.at[4 * n + 10 + k],
                        device_id={"patch": outward},
                        device_id_type=MESH,
                    ).start()

        return carry

    lax.fori_loop(0, n_steps, step, 0)
    if MOVED:
        pumps(in_loop, to_merge)

        @pl.when(at_end)
        def _():
            soft_copy(z * 2 + 1 - y).wait_recv()
            far = blocks[o_far : o_far + 2].reshape(cols, channels).astype(F32).T
            for head in range(2 * pairs):
                row = head * HEAD_DIM
                at = (slice(head // 2, head // 2 + 1), slice((head % 2) * cols, (head % 2 + 1) * cols))
                near_max, far_max = soft[(0, 0, *at)], soft_far[(0, *at)]
                top = jnp.maximum(near_max, far_max)
                near_scale = jnp.exp(near_max - top)
                far_sum = soft_far[(1, *at)] * jnp.exp(far_max - top)
                accum[0, row : row + HEAD_DIM] = (
                    accum[0, row : row + HEAD_DIM] * near_scale + far[row : row + HEAD_DIM] * far_sum
                )
                soft[(0, 1, *at)] = soft[(0, 1, *at)] * near_scale + far_sum

    attended = [normalised(s).astype(BF16) for s in range(samples)]
    load_out.wait()
    residual = hidden[...].astype(F32) + jnp.concatenate(
        [
            lax.dot_general(a, w_out[...], (((0,), (0,)), ((), ())), preferred_element_type=F32)
            for a in attended
        ],
        0,
    )
    residual = residual.astype(BF16).astype(F32).reshape(samples, cols, channels)

    sum_rows = jnp.concatenate([jnp.sum(residual[s], 0, keepdims=True) for s in range(samples)], 0)
    cells = cols * group_size
    local_mean = split_dot(sum_rows, same_group[...]) / cells
    centred = residual - local_mean[:, None, :]
    square_rows = jnp.concatenate(
        [jnp.sum(centred[s] * centred[s], 0, keepdims=True) for s in range(samples)], 0
    )
    stats[me] = split_dot(jnp.concatenate([sum_rows / cells, square_rows], 0), to_group[...])

    def stat_copy(distance):
        return pltpu.make_async_remote_copy(
            src_ref=stats.at[me],
            dst_ref=stats.at[me],
            send_sem=stat_sem.at[0],
            recv_sem=stat_sem.at[1],
            device_id={"patch": lax.rem(me + distance, n)},
            device_id_type=MESH,
        )

    for distance in range(1, n):
        stat_copy(distance).start()

    pumps(to_merge, crossed)
    pltpu.make_async_copy(conv_w, conv_w, load_sem.at[5]).wait()
    cross_row = jnp.where(y == 0, 2, 0)
    conv_acc[...] = dot(blocks[cross : cross + 4].reshape(tokens, channels), conv_w[cross_row])
    half = tokens // 2
    for first, last, at in ((crossed, half_handed, 0), (half_handed, n_ops, half)):
        pumps(first, last)

        @pl.when(jnp.where(y == 0, above_exists, below_exists))
        def _(at=at):
            first_part = handed + at // (half // 2)
            part = blocks[first_part : first_part + 2].reshape(half, channels)
            conv_acc[at : at + half] += dot(part, conv_w[2 - cross_row])

    for load in vectors[2:]:
        load.wait()
    load_shift.wait()

    others = stats.at[pl.ds(0, n - 1)]
    pltpu.make_async_remote_copy(
        src_ref=others,
        dst_ref=others,
        send_sem=stat_sem.at[0],
        recv_sem=stat_sem.at[1],
        device_id={"patch": z * 2 + 1 - y},
        device_id_type=MESH,
    ).wait_recv()
    every = stats[...]
    group_mean = jnp.mean(every[:, :samples], 0)
    shift = every[:, :samples] - group_mean[None]
    group_var = (jnp.sum(every[:, samples:], 0) + cells * jnp.sum(shift * shift, 0)) / (cells * n)
    wide = split_dot(jnp.concatenate([group_mean, lax.rsqrt(group_var + EPSILON)], 0), from_group[...])
    scale = wide[samples:] * gn_gain[...]
    pre = (residual - wide[:samples, None, :]) * scale[:, None, :] + gn_bias[...]
    activated = (pre / (1.0 + jnp.exp(-pre))).astype(BF16).reshape(tokens, channels)

    column = lax.broadcasted_iota(jnp.int32, (tokens, 1), 0) % cols
    taps = conv_acc[...] + dot(activated, conv_w[1])
    left, total, right = (taps[:, tap * channels : (tap + 1) * channels] for tap in range(3))
    total = total + jnp.where(column == 0, 0.0, pltpu.roll(left, 1, 0))
    total = total + jnp.where(column == cols - 1, 0.0, pltpu.roll(right, tokens - 1, 0))
    total = total.reshape(samples, cols, channels) + conv_bias[...]
    for sample in range(samples):
        out[sample, 0] = (
            total[sample] + time_shift[sample : sample + 1] + residual[sample]
        ).astype(BF16)

    def sent(source, semaphore):
        pltpu.make_async_remote_copy(
            src_ref=source,
            dst_ref=source,
            send_sem=semaphore,
            recv_sem=stat_sem.at[1],
            device_id={"patch": z * 2 + 1 - y},
            device_id_type=MESH,
        ).wait_send()

    sent(others, stat_sem.at[0])
    for k in range(3):
        for count in sorted(set(plan["sent"][k]) - {0}):
            those = [d for d in range(n) if plan["sent"][k][d] == count]
            match = functools.reduce(jnp.logical_or, [me == d for d in those])
            pl.when(match)(lambda: sent(blocks.at[pl.ds(0, count)], send_sem.at[k]))
    if MOVED:

        @pl.when(helps)
        def _():
            sent(soft.at[samples], soft_sem.at[0])
            for k in range(2):
                sent(blocks.at[o_own + k], soft_sem.at[2 + k])


def shards(n, *arrays):
    (hidden, stale_attn, stale_conv, ln_gain, ln_bias, w_qkv, w_out) = arrays[:7]
    (gn_gain, gn_bias, conv_w, conv_bias, time_shift) = arrays[7:]
    samples, rows_dev, cols, channels = hidden.shape
    assert rows_dev == 1 and samples == 2 and n % 2 == 0 and n >= 8, "unsupported split"
    tokens = samples * cols
    pairs = channels // (2 * HEAD_DIM)
    hbm = pl.BlockSpec(memory_space=pl.ANY)
    vmem = pl.BlockSpec(memory_space=pltpu.VMEM)
    dma = pltpu.SemaphoreType.DMA
    plan = device_plan(n // 2)
    parts = 4 * (n + 8)
    slots = samples + 1 if MOVED else samples
    return pl.pallas_call(
        functools.partial(kernel, n, plan),
        out_shape=pltpu.VMEM(hidden.shape, BF16),
        in_specs=[hbm] * 12,
        out_specs=vmem,
        scratch_shapes=[
            pltpu.VMEM((tokens, channels), BF16),
            pltpu.VMEM((4, tokens // 4, channels), BF16),
        ]
        + [pltpu.VMEM((channels,), F32)] * 5
        + [
            pltpu.VMEM(time_shift.shape, F32),
            pltpu.VMEM(w_qkv.shape, BF16),
            pltpu.VMEM(w_out.shape, BF16),
            pltpu.VMEM((3, channels, 3 * channels), BF16),
            pltpu.VMEM((parts, tokens // 4, channels), BF16),
            pltpu.VMEM((2 * cols, channels), BF16),
            pltpu.VMEM((2 * cols, channels), BF16),
            pltpu.VMEM((samples + 1, pairs, 2 * HEAD_DIM, 2 * cols), BF16),
            pltpu.VMEM((samples + 1, 2, pairs, 2 * cols), F32),
            pltpu.VMEM((2, pairs, 2 * cols), F32),
            pltpu.VMEM((samples + 1, channels, cols), F32),
            pltpu.VMEM((channels, channels), BF16),
            pltpu.VMEM((channels, LANES), BF16),
            pltpu.VMEM((LANES, channels), BF16),
            pltpu.VMEM((tokens, 3 * channels), F32),
            pltpu.VMEM((n, 2 * samples, LANES), F32),
            dma((7,)),
            dma((5,)),
            dma((3,)),
            dma((4 * n + 12,)),
            dma((4,)),
            dma((2,)),
        ],
        compiler_params=pltpu.CompilerParams(
            collective_id=0, has_side_effects=True, vmem_limit_bytes=56 * 2**20
        ),
        name="section",
    )(
        hidden.reshape(tokens, channels),
        stale_attn.reshape(4, tokens // 4, channels),
        stale_conv.reshape(4, tokens // 4, channels),
        ln_gain,
        ln_bias,
        w_qkv,
        w_out,
        gn_gain,
        gn_bias,
        conv_w,
        conv_bias,
        time_shift,
    )


def solution(mesh):
    wide = P("img", "patch", None, None)
    in_specs = (wide, wide, wide) + (P(),) * 8 + (P("img", None),)
    body = functools.partial(shards, mesh.shape["patch"])
    return jax.shard_map(body, mesh=mesh, in_specs=in_specs, out_specs=wide, check_vma=False)
```

```python
import functools
import heapq
import itertools

import jax
import jax.numpy as jnp
from jax import lax
from jax.experimental import pallas as pl
from jax.experimental.pallas import tpu as pltpu
from jax.sharding import PartitionSpec as P

GROUPS = 32
HEAD_DIM = 64
LANES = 128
EPSILON = 1e-05
MESH = pl.DeviceIdType.MESH
F32 = jnp.float32
BF16 = jnp.bfloat16

DOWN, UP, ACROSS = 0, 1, 2
MOVED = True
TUNED = {
    4: [
        (
            [6, 22, 54, 786, 580, 38, 770, 188, 152, 122, 106, 90, 200, 172, 140, 74, 300, 216, 698, 682, 428, 316, 444, 628, 360, 248, 232, 612, 376, 596, 504, 968, 488, 666, 984, 650],
            33,
            35,
            [(1, 0, 0), (0, 0, 0), (0, 1, 0), (1, 1, 0), (1, 2, 0), (1, 3, 0)],
            [11, 16, 18, 27, 29, 33],
        ),
        (
            [135, 151, 183, 268, 10, 26, 201, 167, 58, 284, 297, 328, 412, 217, 396, 42, 596, 580, 429, 840, 250, 234, 856, 313, 344, 120, 456, 612, 445, 472, 104, 504, 682, 72, 488, 760, 376, 744, 628, 88, 650, 666, 360, 698, 728, 712],
            43,
            43,
            [(0, 1, 0), (1, 1, 0), (0, 2, 3), (0, 3, 5), (1, 0, 0), (1, 3, 0), (0, 0, 0), (1, 2, 0)],
            [14, 22, 25, 30, 31, 35, 40, 43],
        ),
        (
            [263, 279, 295, 140, 409, 328, 156, 393, 186, 425, 311, 441, 377, 346, 12, 28, 170, 361, 856, 612, 840, 62, 216, 200, 456, 88, 46, 580, 72, 666, 472, 596, 488, 232, 628, 504, 248, 650, 104, 682, 120, 698, 728, 712, 744, 760],
            41,
            41,
            [(0, 2, 0), (1, 2, 0), (0, 1, 3), (0, 0, 5), (0, 3, 0), (1, 3, 0), (1, 1, 0), (1, 0, 0)],
            [14, 18, 24, 29, 31, 36, 37, 41],
        ),
        (
            [389, 405, 421, 437, 280, 628, 612, 769, 785, 457, 300, 316, 264, 473, 188, 360, 172, 489, 505, 60, 648, 376, 328, 44, 596, 104, 344, 728, 232, 580, 248, 120, 968, 984, 680, 744, 696, 664, 712, 760],
            32,
            34,
            [(0, 3, 0), (1, 3, 0), (1, 2, 0), (0, 2, 0), (1, 1, 0), (1, 0, 0)],
            [14, 19, 22, 27, 31, 32],
        ),
    ]
}


def special_parts(length):
    return tuple(8 * length + 4 * k for k in range(1, 8))


def mirrored_part(length, y, part):
    return part if y == 0 or part >= 8 * length else 4 * (2 * length - 1 - part // 4) + part % 4


def transfers(length):
    own_edge, cross, handed, q_own, q_far, o_own, o_far = special_parts(length)
    ends = (0, length - 1)

    def turned(zd, sz, half):
        return abs(sz - zd) == 1 and (half == 1 or (zd not in ends and sz in ends))

    result = {}
    for z, y in itertools.product(range(length), range(2)):
        sends = {}
        sides = [(k, zd) for k, zd in ((DOWN, z - 1), (UP, z + 1)) if 0 <= zd < length]
        for sz, sy, sp in itertools.product(range(length), range(2), range(4)):
            part = (2 * sz + sy) * 4 + sp
            sends[part] = [
                (k, part)
                for k, zd in sides
                if needs(length, zd, sz, sp // 2)
                and ((sz <= z if k == UP else sz >= z) if sy == y else sz == z and turned(zd, sz, sp % 2))
            ]
            if sy == y and needs(length, z, sz, sp // 2) and not turned(z, sz, sp % 2):
                sends[part].append((ACROSS, part))
        on = UP if y == 0 else DOWN
        for k in range(4):
            sends[own_edge + k] = [(ACROSS, cross + k)]
            sends[cross + k] = [(on, handed + k)] if on in dict(sides) else []
        for k in range(2):
            sends[q_own + k] = [(UP if z == 0 else DOWN, q_far + k)] if z in ends else []
            sends[o_own + k] = [(DOWN if z == 1 else UP, o_far + k)] if z in (1, length - 2) else []
        result[z, y] = sends
    return result


def needs(length, z, sz, sample):
    return not (sample == 0 and z in (0, length - 1) and abs(sz - z) > 1)


def programs_by_time(length):
    own_edge, cross, handed, q_own, q_far, o_own, o_far = special_parts(length)
    ends = (0, length - 1)
    sends = transfers(length)
    queues, busy, events, count = {}, {}, [], itertools.count()
    landed = {d: {} for d in sends}
    left, answered = {}, set()
    rank = {own_edge: 5, cross: 4, handed: 4, q_own: 0, q_far: 0, o_own: -1, o_far: -1}

    def push(t, kind, *rest):
        heapq.heappush(events, (t, next(count), kind, rest))

    def offer(t, d, part):
        for k, there in sends[d].get(part, []):
            push(t, "queue", d, k, part, there)

    def launch(t, d, k):
        busy[d, k] = bool(queues[d, k])
        if busy[d, k]:
            _, there, part = heapq.heappop(queues[d, k])
            left.setdefault((d, part), t)
            push(t + 1.76, "sent", d, k, there)

    for d in sends:
        for k in range(4):
            offer(0.0, d, (2 * d[0] + d[1]) * 4 + k)
            offer(0.0, d, own_edge + k)
        for k in range(2):
            if d[0] in ends:
                offer(2.0, d, q_own + k)
    while events:
        t, _, kind, (d, *rest) = heapq.heappop(events)
        z, y = d
        if kind == "queue":
            k, part, there = rest
            u = z if y == 0 else length - 1 - z
            c = mirrored_part(length, y, part)
            if c < 8 * length:
                order = c % 4 // 2 - abs(c // 8 - u) * (0.5 if k == ACROSS else 1.0)
            else:
                order = rank[c // 4 * 4]
            heapq.heappush(queues.setdefault((d, k), []), ((order, c), there, part))
            if not busy.get((d, k)):
                busy[d, k] = True
                push(t, "launch", d, k)
        elif kind == "launch":
            launch(t, d, rest[0])
        elif kind == "sent":
            k, there = rest
            push(t + 1.75, "landed", ((z - 1, y), (z + 1, y), (z, 1 - y))[k], there)
            launch(t, d, k)
        else:
            landed[d][rest[0]] = t
            offer(t + 0.3, d, rest[0])
            if z in (1, length - 2) and d not in answered:
                far = [
                    (2 * sz + sy) * 4 + sp
                    for sz, sy, sp in itertools.product(range(length), range(2), range(2))
                    if not needs(length, 0 if z == 1 else length - 1, sz, 0) and sz != z
                ]
                if all(p in landed[d] for p in (q_far, q_far + 1, *far)):
                    answered.add(d)
                    for k in range(2):
                        offer(t + 2.5, d, o_own + k)
    programs = []
    for z in range(length):
        d = (z, 0)
        timed = [(t, 1, p) for p, t in landed[d].items()]
        timed += [(-2.0, 0, 8 * z + k) for k in range(2)]
        if z in ends:
            timed += [(-1.0, 0, q_own + k) for k in range(2)]
        for p in (8 * z + 2, 8 * z + 3, *range(own_edge, own_edge + 4)):
            timed.append((max(0.0, left[d, p] - 1.0), 0, p))
        timed.sort()
        codes = [p * 16 + 8 * waits + sum(2**k for k, _ in sends[d].get(p, [])) for _, waits, p in timed]
        in_loop = 1 + max(i for i, (_, _, p) in enumerate(timed) if p < 8 * length)
        results = [i + 1 for i, (_, _, p) in enumerate(timed) if p >= o_far]
        complete, queries = {}, 0
        for i, (_, _, p) in enumerate(timed):
            if p < 8 * length and needs(length, z, p // 8, p % 4 // 2):
                complete[p % 4 // 2, p // 8] = i + 1
            if q_far <= p < q_far + 2:
                queries = i + 1
        steps, bounds, top, helped = [], [], 0, False
        chosen = sorted(complete, key=lambda k: (complete[k], k))
        for i, (sample, sz) in enumerate(chosen):
            top = max(top, complete[sample, sz])
            flags = 0
            if z in (1, length - 2) and sample == 0:
                if not needs(length, 0 if z == 1 else length - 1, sz, 0):
                    flags, helped, top = 1 if helped else 3, True, max(top, queries)
                    last_far = i
            steps.append([sample, sz, flags])
            bounds.append(top)
        if z in (1, length - 2):
            steps[last_far][2] += 4
        programs.append((codes, in_loop, max([in_loop, *results]), steps, bounds))
    return programs


def device_plan(length):
    n = 2 * length
    cross, handed = special_parts(length)[1:3]
    programs = TUNED.get(length) or programs_by_time(length)
    plan = {name: [] for name in ("ops", "bounds", "steps", "n_steps", "in_loop", "to_merge", "crossed", "half_handed", "n_ops")}
    plan["sent"] = [[0] * n for _ in range(3)]
    for d in range(n):
        z, y = divmod(d, 2)
        codes, in_loop, to_merge, steps, bounds = programs[z if y == 0 else length - 1 - z]
        ops = []
        for code in codes:
            where = code % 8
            if y == 1:
                where = where // 4 * 4 + where // 2 % 2 + where % 2 * 2
            ops.append(mirrored_part(length, y, code // 16) * 16 + code // 8 % 2 * 8 + where)
            for k in range(3):
                plan["sent"][k][d] += where // 2**k % 2
        plan["ops"].append(ops)
        plan["bounds"].append([*bounds, in_loop])
        plan["steps"].append(
            [s + 2 * (sz if y == 0 else length - 1 - sz) + 512 * flags for s, sz, flags in steps]
        )
        across = [i + 1 for i, code in enumerate(codes) if cross <= code // 16 < cross + 4]
        plan["n_steps"].append(len(steps))
        plan["in_loop"].append(in_loop)
        plan["to_merge"].append(to_merge)
        plan["crossed"].append(max(to_merge, *across))
        above = [i + 1 for i, code in enumerate(codes) if handed <= code // 16 < handed + 2]
        plan["half_handed"].append(max(plan["crossed"][-1], *above, 0))
        plan["n_ops"].append(len(ops))
    for name in ("ops", "bounds", "steps"):
        width = max(len(row) for row in plan[name])
        plan[name] = [row + [0] * (width - len(row)) for row in plan[name]]
    return plan


def layer_norm(values, gain, bias):
    values = values.astype(F32)
    centre = jnp.mean(values, -1, keepdims=True)
    centred = values - centre
    spread = jnp.mean(centred * centred, -1, keepdims=True)
    return (centred * lax.rsqrt(spread + EPSILON) * gain + bias).astype(BF16)


def dot(a, b):
    return jnp.dot(a, b, preferred_element_type=F32)


def balanced_dot(a, b):
    wide = b.shape[1] // 512 * 512
    half = a.shape[0] // 2
    rest = b[:, wide:]
    tail = jnp.concatenate([dot(a[:half], rest), dot(a[half:], rest)], 0)
    return jnp.concatenate([dot(a, b[:, :wide]), tail], 1)


def split_dot(a, b):
    high = a.astype(BF16)
    rest = a - high.astype(F32)
    mid = rest.astype(BF16)
    low = (rest - mid.astype(F32)).astype(BF16)
    rows = a.shape[0]
    thirds = dot(jnp.concatenate([high, mid, low], 0), b)
    return thirds[:rows] + thirds[rows : 2 * rows] + thirds[2 * rows :]


def kernel(
    n,
    plan,
    hidden_hbm,
    stale_attn_hbm,
    stale_conv_hbm,
    ln_gain_hbm,
    ln_bias_hbm,
    w_qkv_hbm,
    w_out_hbm,
    gn_gain_hbm,
    gn_bias_hbm,
    conv_w_hbm,
    conv_bias_hbm,
    time_shift_hbm,
    out,
    hidden,
    stale_attn,
    ln_gain,
    ln_bias,
    gn_gain,
    gn_bias,
    conv_bias,
    time_shift,
    w_qkv,
    w_out,
    conv_w,
    blocks,
    keys,
    values,
    q_diag,
    soft,
    soft_far,
    accum,
    same_group,
    to_group,
    from_group,
    conv_acc,
    base,
    stats,
    load_sem,
    vector_sem,
    send_sem,
    recv_sem,
    soft_sem,
    stat_sem,
):
    samples, _, cols, channels = out.shape
    tokens = samples * cols
    pairs = channels // (2 * HEAD_DIM)
    group_size = channels // GROUPS
    length = n // 2
    own_edge, cross, handed, q_own, q_far, o_own, o_far = special_parts(length)
    fresh_part = 4 * n
    me = lax.axis_index("patch")
    z = me // 2
    y = me % 2
    above_exists = z > 0
    below_exists = z < length - 1
    neighbours = ((above_exists, me - 2), (below_exists, me + 2), (True, z * 2 + 1 - y))

    barrier = pltpu.get_barrier_semaphore()
    for there, device in neighbours:
        def announce(device=device):
            pl.semaphore_signal(barrier, inc=1, device_id={"patch": device}, device_id_type=MESH)
        if there is True:
            announce()
        else:
            pl.when(there)(announce)

    load_stale = pltpu.make_async_copy(stale_attn_hbm, stale_attn, load_sem.at[0])
    load_hidden = pltpu.make_async_copy(hidden_hbm, hidden, load_sem.at[1])
    load_qkv = pltpu.make_async_copy(w_qkv_hbm, w_qkv, load_sem.at[2])
    load_edge = pltpu.make_async_copy(stale_conv_hbm, blocks.at[pl.ds(own_edge, 4)], load_sem.at[3])
    load_out = pltpu.make_async_copy(w_out_hbm, w_out, load_sem.at[4])
    load_conv = [
        pltpu.make_async_copy(
            conv_w_hbm.at[row, tap],
            conv_w.at[row, :, pl.ds(tap * channels, channels)],
            load_sem.at[5],
        )
        for row in range(3)
        for tap in range(3)
    ]
    load_shift = pltpu.make_async_copy(time_shift_hbm, time_shift, load_sem.at[6])
    vectors = [
        pltpu.make_async_copy(source, target, vector_sem.at[i])
        for i, (source, target) in enumerate(
            (
                (ln_gain_hbm, ln_gain),
                (ln_bias_hbm, ln_bias),
                (gn_gain_hbm, gn_gain),
                (gn_bias_hbm, gn_bias),
                (conv_bias_hbm, conv_bias),
            )
        )
    ]
    load_stale.start()
    for load in vectors[:2]:
        load.start()
    load_hidden.start()

    def pick(choices):
        if len(set(choices)) == 1:
            return jnp.int32(choices[0])
        value = jnp.int32(choices[0])
        for k in range(1, n):
            value = jnp.where(me == k, jnp.int32(choices[k]), value)
        return value

    def table(name):
        rows = plan[name]
        bits = max(v for row in rows for v in row).bit_length()
        per = 31 // bits
        words = [
            pick([sum(v << (bits * k) for k, v in enumerate(row[at : at + per])) for row in rows])
            for at in range(0, len(rows[0]), per)
        ]

        scale = 2**16 // per + 1
        assert all(i * scale >> 16 == i // per for i in range(len(rows[0])))

        def look(i):
            at = lax.shift_right_logical(i * scale, 16)
            level, bit = words, 1
            while len(level) > 1:
                odd = (at & bit) != 0
                pairs_of = [level[k : k + 2] for k in range(0, len(level), 2)]
                level = [jnp.where(odd, p[1], p[0]) if len(p) == 2 else p[0] for p in pairs_of]
                bit *= 2
            return lax.shift_right_logical(level[0], (i - at * per) * bits) & (2**bits - 1)

        return look

    ops, bounds, steps = table("ops"), table("bounds"), table("steps")
    n_steps = pick(plan["n_steps"])
    in_loop = pick(plan["in_loop"])
    to_merge = pick(plan["to_merge"])
    crossed = pick(plan["crossed"])
    half_handed = pick(plan["half_handed"])
    n_ops = pick(plan["n_ops"])
    soft[...] = jnp.zeros_like(soft)
    for slot in range(samples + 1):
        soft[slot, 0] = jnp.full(soft.shape[2:], -jnp.inf, F32)
    accum[...] = jnp.zeros_like(accum)
    q_diag[...] = jnp.zeros_like(q_diag)

    @pl.when(jnp.where(y == 0, z == 0, z == length - 1))
    def _():
        blocks[handed : handed + 4] = jnp.zeros_like(blocks[handed : handed + 4])

    mine = me * 4
    for load in vectors[:2]:
        load.wait()
    load_stale.wait()
    load_qkv.start()
    load_edge.start()
    for load in vectors[2:]:
        load.start()
    load_shift.start()
    load_out.start()
    for load in load_conv:
        load.start()

    def landing_of(part):
        late = jnp.where(part < q_far, part - 8, jnp.where(part < o_far, part - 12, part - 18))
        return jnp.where(part < 4 * n, part, late)

    def pump(i, carry):
        op = ops(i)
        part = lax.shift_right_logical(op, 4)
        stale = part < 4 * n
        landed = landing_of(part)

        @pl.when((op & 8) != 0)
        def _():
            pltpu.make_async_remote_copy(
                src_ref=blocks.at[part],
                dst_ref=blocks.at[part],
                send_sem=send_sem.at[0],
                recv_sem=recv_sem.at[landed],
                device_id={"patch": z * 2 + 1 - y},
                device_id_type=MESH,
            ).wait_recv()

        there = jnp.where(stale, part, part + 4)
        landing = landing_of(there)
        for k, (_, device) in enumerate(neighbours):

            @pl.when((op & 2**k) != 0)
            def _(k=k, device=device):
                pltpu.make_async_remote_copy(
                    src_ref=blocks.at[part],
                    dst_ref=blocks.at[there],
                    send_sem=send_sem.at[k],
                    recv_sem=recv_sem.at[landing],
                    device_id={"patch": device},
                    device_id_type=MESH,
                ).start()

        return carry

    def pumps(first, last):
        lax.fori_loop(first, last, pump, 0)

    def norm_stale(s):
        part = layer_norm(stale_attn[2 * s : 2 * s + 2], ln_gain[...], ln_bias[...])
        blocks[pl.ds(mine + 2 * s, 2)] = part

    for half in range(2):
        blocks[mine + half] = layer_norm(stale_attn[half], ln_gain[...], ln_bias[...])
        if half == 0:
            pl.semaphore_wait(barrier, 1 + above_exists.astype(jnp.int32) + below_exists.astype(jnp.int32))
        pumps(half, half + 1)
    for s in range(1, samples):
        norm_stale(s)

    load_hidden.wait()
    fresh = layer_norm(hidden[...], ln_gain[...], ln_bias[...])
    blocks[fresh_part : fresh_part + 4] = fresh.reshape(4, tokens // 4, channels)
    load_qkv.wait()
    queries = dot(fresh, w_qkv[:, :channels]).astype(BF16).astype(F32) * HEAD_DIM ** (-0.5)
    if MOVED:
        blocks[q_own : q_own + 2] = queries[:cols].astype(BF16).reshape(2, cols // 2, channels)

    def spread_queries(slot, q_t):
        for pair in range(pairs):
            for half in range(2):
                row = (2 * pair + half) * HEAD_DIM
                q_diag[
                    slot, pair, half * HEAD_DIM : (half + 1) * HEAD_DIM, half * cols : (half + 1) * cols
                ] = q_t[row : row + HEAD_DIM]

    q_t = queries.T.astype(BF16)
    for s in range(samples):
        spread_queries(s, q_t[:, s * cols : (s + 1) * cols])
    load_edge.wait()
    pumps(2, bounds(0))
    channel_row = lax.broadcasted_iota(jnp.int32, (channels, channels), 0) // group_size
    channel_col = lax.broadcasted_iota(jnp.int32, (channels, channels), 1) // group_size
    same_group[...] = jnp.where(channel_row == channel_col, 1.0, 0.0).astype(BF16)
    narrow = to_group.shape[1]
    channel = lax.broadcasted_iota(jnp.int32, (channels, narrow), 0) // group_size
    group = lax.broadcasted_iota(jnp.int32, (channels, narrow), 1)
    to_group[...] = jnp.where(channel == group, 1.0, 0.0).astype(BF16)
    channel = lax.broadcasted_iota(jnp.int32, (narrow, channels), 1) // group_size
    group = lax.broadcasted_iota(jnp.int32, (narrow, channels), 0)
    from_group[...] = jnp.where(channel == group, 1.0, 0.0).astype(BF16)

    def attend(slot):
        lanes = [slice(pair * 2 * HEAD_DIM, (pair + 1) * 2 * HEAD_DIM) for pair in range(pairs)]
        old_max, old_sum = soft[slot, 0], soft[slot, 1]
        scores = [dot(keys[:, lanes[pair]], q_diag[slot, pair]) for pair in range(pairs)]
        new_max = [
            jnp.maximum(old_max[pair : pair + 1], jnp.max(scores[pair], 0, keepdims=True))
            for pair in range(pairs)
        ]
        weights = [jnp.exp(scores[pair] - new_max[pair]) for pair in range(pairs)]
        both = [lax.dot_general(
                values[:, lanes[pair]],
                weights[pair].astype(BF16),
                (((0,), (0,)), ((), ())),
                preferred_element_type=F32,
            )
            for pair in range(pairs)]
        rescale = [jnp.exp(old_max[pair : pair + 1] - new_max[pair]) for pair in range(pairs)]
        soft[slot, 0] = jnp.concatenate(new_max, 0)
        soft[slot, 1] = jnp.concatenate(
            [
                jnp.sum(weights[pair], 0, keepdims=True) + old_sum[pair : pair + 1] * rescale[pair]
                for pair in range(pairs)
            ],
            0,
        )
        for pair in range(pairs):
            for half in range(2):
                row = (2 * pair + half) * HEAD_DIM
                own = slice(half * cols, (half + 1) * cols)
                accum[slot, row : row + HEAD_DIM] = (
                    both[pair][half * HEAD_DIM : (half + 1) * HEAD_DIM, own]
                    + accum[slot, row : row + HEAD_DIM] * rescale[pair][:, own]
                )

    def normalised(slot):
        for head in range(2 * pairs):
            row = head * HEAD_DIM
            total = soft[slot, 1, head // 2 : head // 2 + 1, (head % 2) * cols : (head % 2 + 1) * cols]
            accum[slot, row : row + HEAD_DIM] = accum[slot, row : row + HEAD_DIM] * (1.0 / total)
        return accum[slot]

    def soft_copy(device):
        return pltpu.make_async_remote_copy(
            src_ref=soft.at[samples],
            dst_ref=soft_far,
            send_sem=soft_sem.at[0],
            recv_sem=soft_sem.at[1],
            device_id={"patch": device},
            device_id_type=MESH,
        )

    at_end = (z == 0) | (z == length - 1)
    helps = (z == 1) | (z == length - 2)
    outward = jnp.where(z == 1, me - 2, me + 2)

    def step(i, carry):
        code = steps(i)
        s = code & 1
        sz = lax.shift_right_logical(code, 1) & 255
        first_slot = jnp.where(sz == z, n, 2 * sz + y)
        second_slot = 2 * sz + 1 - y
        low = bounds(i)
        span = bounds(i + 1) - low
        marks = [low, low + lax.shift_right_logical(span, 1), low + span]
        rows = jnp.concatenate(
            [
                blocks[pl.ds(slot * 4 + 2 * s, 2)].reshape(cols, channels)
                for slot in (first_slot, second_slot)
            ],
            0,
        )
        both_kv = balanced_dot(rows, w_qkv[:, channels:]).astype(BF16)
        keys[...] = both_kv[:, :channels]
        values[...] = both_kv[:, channels:]
        pumps(marks[0], marks[1])
        attend(s)
        pumps(marks[1], marks[2])
        if MOVED:
            flag = lax.shift_right_logical(code, 9)

            @pl.when((flag & 1) != 0)
            def _():
                @pl.when((flag & 2) != 0)
                def _():
                    far = blocks[q_far : q_far + 2].reshape(cols, channels)
                    spread_queries(samples, far.astype(F32).T.astype(BF16))

                attend(samples)

            @pl.when((flag & 4) != 0)
            def _():
                part = normalised(samples).T.astype(BF16)
                blocks[o_own : o_own + 2] = part.reshape(2, cols // 2, channels)
                soft_copy(outward).start()
                for k in range(2):
                    pltpu.make_async_remote_copy(
                        src_ref=blocks.at[o_own + k],
                        dst_ref=blocks.at[o_far + k],
                        send_sem=soft_sem.at[2 + k],
                        recv_sem=recv_sem.at[4 * n + 10 + k],
                        device_id={"patch": outward},
                        device_id_type=MESH,
                    ).start()

        return carry

    lax.fori_loop(0, n_steps, step, 0)
    if MOVED:
        pumps(in_loop, to_merge)

        @pl.when(at_end)
        def _():
            soft_copy(z * 2 + 1 - y).wait_recv()
            far = blocks[o_far : o_far + 2].reshape(cols, channels).astype(F32).T
            for head in range(2 * pairs):
                row = head * HEAD_DIM
                at = (slice(head // 2, head // 2 + 1), slice((head % 2) * cols, (head % 2 + 1) * cols))
                near_max, far_max = soft[(0, 0, *at)], soft_far[(0, *at)]
                top = jnp.maximum(near_max, far_max)
                near_scale = jnp.exp(near_max - top)
                far_sum = soft_far[(1, *at)] * jnp.exp(far_max - top)
                accum[0, row : row + HEAD_DIM] = (
                    accum[0, row : row + HEAD_DIM] * near_scale + far[row : row + HEAD_DIM] * far_sum
                )
                soft[(0, 1, *at)] = soft[(0, 1, *at)] * near_scale + far_sum

    attended = [normalised(s).astype(BF16) for s in range(samples)]
    load_out.wait()
    residual = hidden[...].astype(F32) + jnp.concatenate(
        [
            lax.dot_general(a, w_out[...], (((0,), (0,)), ((), ())), preferred_element_type=F32)
            for a in attended
        ],
        0,
    )
    residual = residual.astype(BF16).astype(F32).reshape(samples, cols, channels)

    sum_rows = jnp.concatenate([jnp.sum(residual[s], 0, keepdims=True) for s in range(samples)], 0)
    cells = cols * group_size
    local_mean = split_dot(sum_rows, same_group[...]) / cells
    centred = residual - local_mean[:, None, :]
    square_rows = jnp.concatenate(
        [jnp.sum(centred[s] * centred[s], 0, keepdims=True) for s in range(samples)], 0
    )
    stats[me] = split_dot(jnp.concatenate([sum_rows / cells, square_rows], 0), to_group[...])

    def stat_copy(distance):
        return pltpu.make_async_remote_copy(
            src_ref=stats.at[me],
            dst_ref=stats.at[me],
            send_sem=stat_sem.at[0],
            recv_sem=stat_sem.at[1],
            device_id={"patch": lax.rem(me + distance, n)},
            device_id_type=MESH,
        )

    for distance in range(1, n):
        stat_copy(distance).start()

    pumps(to_merge, crossed)
    pltpu.make_async_copy(conv_w, conv_w, load_sem.at[5]).wait()
    cross_row = jnp.where(y == 0, 2, 0)
    conv_acc[...] = dot(blocks[cross : cross + 4].reshape(tokens, channels), conv_w[cross_row])
    half = tokens // 2
    for first, last, at in ((crossed, half_handed, 0), (half_handed, n_ops, half)):
        pumps(first, last)
        part = blocks[handed + 2 * (at > 0) : handed + 2 * (at > 0) + 2].reshape(half, channels)
        conv_acc[at : at + half] += dot(part, conv_w[2 - cross_row])
    for load in vectors[2:]:
        load.wait()
    load_shift.wait()

    column = lax.broadcasted_iota(jnp.int32, (tokens, 1), 0) % cols

    def shifted(taps):
        left, middle, right = (taps[:, tap * channels : (tap + 1) * channels] for tap in range(3))
        middle = middle + jnp.where(column == 0, 0.0, pltpu.roll(left, 1, 0))
        return middle + jnp.where(column == cols - 1, 0.0, pltpu.roll(right, tokens - 1, 0))

    added = residual + (conv_bias[...] + time_shift[...])[:, None, :]
    base[...] = shifted(conv_acc[...]) + added.reshape(tokens, channels)

    others = stats.at[pl.ds(0, n - 1)]
    pltpu.make_async_remote_copy(
        src_ref=others,
        dst_ref=others,
        send_sem=stat_sem.at[0],
        recv_sem=stat_sem.at[1],
        device_id={"patch": z * 2 + 1 - y},
        device_id_type=MESH,
    ).wait_recv()
    every = stats[...]
    group_mean = jnp.mean(every[:, :samples], 0)
    shift = every[:, :samples] - group_mean[None]
    group_var = (jnp.sum(every[:, samples:], 0) + cells * jnp.sum(shift * shift, 0)) / (cells * n)
    wide = split_dot(jnp.concatenate([group_mean, lax.rsqrt(group_var + EPSILON)], 0), from_group[...])
    scale = wide[samples:] * gn_gain[...]
    pre = (residual - wide[:samples, None, :]) * scale[:, None, :] + gn_bias[...]
    activated = (pre / (1.0 + jnp.exp(-pre))).astype(BF16).reshape(tokens, channels)

    total = base[...] + shifted(dot(activated, conv_w[1]))
    out[:, 0] = total.astype(BF16).reshape(samples, cols, channels)

    def sent(source, semaphore):
        pltpu.make_async_remote_copy(
            src_ref=source,
            dst_ref=source,
            send_sem=semaphore,
            recv_sem=stat_sem.at[1],
            device_id={"patch": z * 2 + 1 - y},
            device_id_type=MESH,
        ).wait_send()

    sent(others, stat_sem.at[0])
    for k in range(3):
        for count in sorted(set(plan["sent"][k]) - {0}):
            those = [d for d in range(n) if plan["sent"][k][d] == count]
            match = functools.reduce(jnp.logical_or, [me == d for d in those])
            pl.when(match)(lambda: sent(blocks.at[pl.ds(0, count)], send_sem.at[k]))
    if MOVED:

        @pl.when(helps)
        def _():
            sent(soft.at[samples], soft_sem.at[0])
            for k in range(2):
                sent(blocks.at[o_own + k], soft_sem.at[2 + k])


def shards(n, *arrays):
    (hidden, stale_attn, stale_conv, ln_gain, ln_bias, w_qkv, w_out) = arrays[:7]
    (gn_gain, gn_bias, conv_w, conv_bias, time_shift) = arrays[7:]
    samples, rows_dev, cols, channels = hidden.shape
    assert rows_dev == 1 and samples == 2 and n % 2 == 0 and n >= 8, "unsupported split"
    tokens = samples * cols
    pairs = channels // (2 * HEAD_DIM)
    hbm = pl.BlockSpec(memory_space=pl.ANY)
    vmem = pl.BlockSpec(memory_space=pltpu.VMEM)
    dma = pltpu.SemaphoreType.DMA
    plan = device_plan(n // 2)
    parts = 4 * (n + 8)
    slots = samples + 1 if MOVED else samples
    return pl.pallas_call(
        functools.partial(kernel, n, plan),
        out_shape=pltpu.VMEM(hidden.shape, BF16),
        in_specs=[hbm] * 12,
        out_specs=vmem,
        scratch_shapes=[
            pltpu.VMEM((tokens, channels), BF16),
            pltpu.VMEM((4, tokens // 4, channels), BF16),
        ]
        + [pltpu.VMEM((channels,), F32)] * 5
        + [
            pltpu.VMEM(time_shift.shape, F32),
            pltpu.VMEM(w_qkv.shape, BF16),
            pltpu.VMEM(w_out.shape, BF16),
            pltpu.VMEM((3, channels, 3 * channels), BF16),
            pltpu.VMEM((parts, tokens // 4, channels), BF16),
            pltpu.VMEM((2 * cols, channels), BF16),
            pltpu.VMEM((2 * cols, channels), BF16),
            pltpu.VMEM((samples + 1, pairs, 2 * HEAD_DIM, 2 * cols), BF16),
            pltpu.VMEM((samples + 1, 2, pairs, 2 * cols), F32),
            pltpu.VMEM((2, pairs, 2 * cols), F32),
            pltpu.VMEM((samples + 1, channels, cols), F32),
            pltpu.VMEM((channels, channels), BF16),
            pltpu.VMEM((channels, LANES), BF16),
            pltpu.VMEM((LANES, channels), BF16),
            pltpu.VMEM((tokens, 3 * channels), F32),
            pltpu.VMEM((tokens, channels), F32),
            pltpu.VMEM((n, 2 * samples, LANES), F32),
            dma((7,)),
            dma((5,)),
            dma((3,)),
            dma((4 * n + 12,)),
            dma((4,)),
            dma((2,)),
        ],
        compiler_params=pltpu.CompilerParams(
            collective_id=0, has_side_effects=True, vmem_limit_bytes=56 * 2**20
        ),
        name="section",
    )(
        hidden.reshape(tokens, channels),
        stale_attn.reshape(4, tokens // 4, channels),
        stale_conv.reshape(4, tokens // 4, channels),
        ln_gain,
        ln_bias,
        w_qkv,
        w_out,
        gn_gain,
        gn_bias,
        conv_w,
        conv_bias,
        time_shift,
    )


def solution(mesh):
    wide = P("img", "patch", None, None)
    in_specs = (wide, wide, wide) + (P(),) * 8 + (P("img", None),)
    body = functools.partial(shards, mesh.shape["patch"])
    return jax.shard_map(body, mesh=mesh, in_specs=in_specs, out_specs=wide, check_vma=False)
```
